32 devices in a mesh: tm: 4 (over x, core), space: 8 (over z, y).
Axes of the slice: x: 2, y: 2, z: 4, core: 2. Of those that a mesh axis runs over, the one named last changes fastest.
Arguments:
- start_value: float32 [4, 8, 512, 256], P('tm', 'space'), may hold values from -6 to 6
- old_nodes: float32 [4, 3, 8, 512, 256], P('tm', None, 'space'), may hold values from -6 to 6
- diffusivity: float32 [8, 512, 256], P('space'), may hold values from 0.2 to 2
Outputs:
- fine_nodes: float32 [4, 3, 8, 512, 256], P('tm', None, 'space')
- next_start: float32 [4, 8, 512, 256], P('tm', 'space')
- next_coarse: float32 [4, 8, 512, 256], P('tm', 'space')
The draws below stay inside these ranges and needn't reach their ends.
All inputs are finite; a program needn't handle non-finite values.
Results may differ from the reference program's by a relative error of at most 0.0001.
Values sent between devices are 32-bit elements; how exact they have to be, the bound alone decides.
A program may use at most 64 MiB of HBM per device.

```python
import math
import jax
import jax.numpy as jnp
from jax import lax

NY = 512
NZ = 256
NODES = 3
CG_ITERS = 2
NX = 8
SLICES = 4


def shard_levels(key, extent, split, low, largest):
    factor_of = 1.0
    for dim, parts in split:
        heights = jax.random.uniform(jax.random.fold_in(jax.random.fold_in(key, 6), dim), (parts,), jnp.float32, low / len(split), largest / len(split))
        factor_of = factor_of * jnp.repeat(jnp.exp(heights), extent[dim] // parts).reshape((-1,) + (1,) * (len(extent) - 1 - dim))
    return factor_of


def bell_draw(own_key, shape, scale, most, cuts=(), kind=jnp.bfloat16):
    array = scale * jax.random.normal(own_key, shape, jnp.float32)
    if cuts:
        array = array * shard_levels(own_key, shape, cuts, -0.22, 0.18)
    return jnp.clip(array, -most, most).astype(kind)


def setup_inputs(seed: int = 0) -> dict:
    streams_of = jax.random.split(jax.random.key(seed), 4)
    start_value = bell_draw(streams_of[0], (SLICES, NX, NY, NZ), 1.0, 6.0, ((0, 4), (1, 8)), jnp.float32)
    old_nodes = bell_draw(streams_of[1], (SLICES, NODES, NX, NY, NZ), 1.0, 6.0, ((0, 4), (2, 8)), jnp.float32)
    diffusivity = jnp.clip(jnp.exp(math.log(2.0) - 2.3025851 * jax.random.uniform(streams_of[2], (NX, NY, NZ), jnp.float32) ** shard_levels(streams_of[2], (NX, NY, NZ), ((0, 8),), -0.2, 0.2)), 0.2, 2.0)
    return dict(start_value=start_value, old_nodes=old_nodes, diffusivity=diffusivity)


STEP = 2.0
ROOT_SIX = math.sqrt(6.0)
NODE_TIMES = [(4.0 - ROOT_SIX) / 10.0, (4.0 + ROOT_SIX) / 10.0, 1.0]
COLLOC = [[(88.0 - 7.0 * ROOT_SIX) / 360.0, (296.0 - 169.0 * ROOT_SIX) / 1800.0, (-2.0 + 3.0 * ROOT_SIX) / 225.0], [(296.0 + 169.0 * ROOT_SIX) / 1800.0, (88.0 + 7.0 * ROOT_SIX) / 360.0, (-2.0 - 3.0 * ROOT_SIX) / 225.0], [(16.0 - ROOT_SIX) / 36.0, (16.0 + ROOT_SIX) / 36.0, 1.0 / 9.0]]

def sweep_weight(row, column):
    below = COLLOC[row - 1][column] if row > 0 else 0.0
    return COLLOC[row][column] - below

def node_width(row):
    below = NODE_TIMES[row - 1] if row > 0 else 0.0
    return NODE_TIMES[row] - below

def neighbour(field, dim, forward):
    length = field.shape[dim]
    edge = jnp.zeros_like(lax.slice_in_dim(field, 0, 1, axis=dim))
    if forward:
        return jnp.concatenate([lax.slice_in_dim(field, 1, length, axis=dim), edge], axis=dim)
    return jnp.concatenate([edge, lax.slice_in_dim(field, 0, length - 1, axis=dim)], axis=dim)

def face_table(kappa):
    faces = []
    for dim in range(3):
        for forward in (True, False):
            faces.append(0.5 * (kappa + neighbour(kappa, dim, forward)))
    total = faces[0] + faces[1] + faces[2] + faces[3] + faces[4] + faces[5]
    return (faces, total)

def apply_heat(field, faces, total):
    result = faces[0] * neighbour(field, 0, True) + faces[1] * neighbour(field, 0, False)
    result = result + faces[2] * neighbour(field, 1, True) + faces[3] * neighbour(field, 1, False)
    result = result + faces[4] * neighbour(field, 2, True) + faces[5] * neighbour(field, 2, False)
    return result - total * field

def combine(weights, images):
    summed = weights[0] * images[0]
    for column in range(1, 3):
        summed = summed + weights[column] * images[column]
    return summed

def solve(guess, residual, width, faces, total):
    iterate = guess
    direction = residual
    norm_now = jnp.sum(residual * residual)
    for sweep in range(CG_ITERS):
        product = direction - width * apply_heat(direction, faces, total)
        step_size = norm_now / jnp.sum(direction * product)
        iterate = iterate + step_size * direction
        if sweep + 1 < CG_ITERS:
            residual = residual - step_size * product
            norm_next = jnp.sum(residual * residual)
            direction = residual + norm_next / norm_now * direction
            norm_now = norm_next
    return iterate

def reference(start_value, old_nodes, diffusivity):
    faces, total = face_table(diffusivity)

    def one_slice(pair):
        begin, previous_nodes = pair
        images = [apply_heat(previous_nodes[column], faces, total) for column in range(3)]
        previous = begin
        fresh = []
        for row in range(3):
            weights = [sweep_weight(row, column) for column in range(3)]
            residual = previous - previous_nodes[row] + STEP * combine(weights, images)
            result = solve(previous_nodes[row], residual, STEP * node_width(row), faces, total)
            fresh.append(result)
            previous = result
        coarse_res = begin - previous_nodes[2] + STEP * combine(COLLOC[2], images)
        coarse_end = solve(previous_nodes[2], coarse_res, STEP, faces, total)
        return (jnp.stack(fresh), coarse_end)
    fine_nodes, coarse_ends = lax.map(one_slice, (start_value, old_nodes))
    next_start = jnp.concatenate([start_value[:1], fine_nodes[:-1, 2]], axis=0)
    next_coarse = jnp.concatenate([start_value[:1], coarse_ends[:-1]], axis=0)
    return (fine_nodes, next_start, next_coarse)
```

```python
import math

import jax
import jax.numpy as jnp
from jax import lax
from jax.experimental import pallas as pl
from jax.experimental.pallas import tpu as pltpu
from jax.sharding import PartitionSpec as P

STEP = 2.0
ROOT_SIX = math.sqrt(6.0)
NODE_TIMES = [(4.0 - ROOT_SIX) / 10.0, (4.0 + ROOT_SIX) / 10.0, 1.0]
COLLOC = [
    [
        (88.0 - 7.0 * ROOT_SIX) / 360.0,
        (296.0 - 169.0 * ROOT_SIX) / 1800.0,
        (-2.0 + 3.0 * ROOT_SIX) / 225.0,
    ],
    [
        (296.0 + 169.0 * ROOT_SIX) / 1800.0,
        (88.0 + 7.0 * ROOT_SIX) / 360.0,
        (-2.0 - 3.0 * ROOT_SIX) / 225.0,
    ],
    [(16.0 - ROOT_SIX) / 36.0, (16.0 + ROOT_SIX) / 36.0, 1.0 / 9.0],
]
MESH = pl.DeviceIdType.MESH
PAD = 8

KAPPA, NODE, START, RES, IMG, GAIN = 0, 1, 4, 5, 9, 13
FIELDS = 15
H_KAPPA, H_NODE, H_RES, H_IMG, H_GAIN = 0, 1, 4, 8, 12
HALOS = 14


def sweep_weight(row, column):
    below = COLLOC[row - 1][column] if row > 0 else 0.0
    return COLLOC[row][column] - below


def node_width(row):
    below = NODE_TIMES[row - 1] if row > 0 else 0.0
    return NODE_TIMES[row] - below


WIDTHS = [STEP * node_width(0), STEP * node_width(1), STEP * node_width(2), STEP]


def chunk_bounds(rows, tile):
    tiles = rows // tile
    parts = min(5, tiles)
    counts = [tiles // parts + (c < tiles % parts) for c in range(parts)]
    if counts[-1] > 1:
        counts[-1] -= 1
        counts[1 if parts > 2 else 0] += 1
    cuts = [tile * sum(counts[:c]) for c in range(parts + 1)]
    return [(cuts[c], cuts[c + 1] - cuts[c]) for c in range(parts)]


def tile_of(rows, most):
    best = 8
    for size in range(8, most + 1, 8):
        if rows % size == 0:
            best = size
    return best


def kernel(
    slices, slabs, ny, nz,
    start_in, nodes_in, kappa_in,
    fine_out, start_out, coarse_out,
    field, lower, upper, faces, across, result, sums,
    swap_s, swap_r, own_s, halo_s, halo_r, sum_s, sum_r, out_s, out_r, end_s, end_r, copy_s,
):
    f32 = jnp.float32
    t = lax.axis_index("tm")
    s = lax.axis_index("space")
    h = lax.rem(s, 2)
    p = lax.div(s, 2)
    pairs = slabs // 2
    half = ny // 2
    win = half + PAD
    other = 1 - h
    partner = s + 1 - 2 * h
    first_row = pl.multiple_of(h * (half - PAD), 8)
    partner_row = pl.multiple_of(other * (half - PAD), 8)
    own = pl.multiple_of(PAD * h, 8)
    mine = pl.multiple_of(h * half, 8)
    has_next = t < slices - 1
    has_prev = t > 0
    has_lower = p > 0
    has_upper = p < pairs - 1
    pending = []

    def start(copy, cond=None):
        if cond is None:
            copy.start()
        else:
            pl.when(cond)(copy.start)
        return copy

    def later(copy, cond=None):
        pending.append((copy, cond))

    def remote(src, dst, send, recv, tm, space):
        return pltpu.make_async_remote_copy(
            src_ref=src, dst_ref=dst, send_sem=send, recv_sem=recv,
            device_id=(tm, space), device_id_type=MESH,
        )

    barrier = pltpu.get_barrier_semaphore()

    def greet(d, carry):
        pl.semaphore_signal(
            barrier, inc=1, device_id=(t, lax.rem(s + d, slabs)), device_id_type=MESH
        )
        return carry

    lax.fori_loop(1, slabs, greet, 0)
    for cond, tm in ((has_next, t + 1), (has_prev, t - 1)):

        @pl.when(cond)
        def _(tm=tm):
            for space in (s, partner):
                pl.semaphore_signal(barrier, inc=1, device_id=(tm, space), device_id_type=MESH)

    sources = [kappa_in.at[0]] + [nodes_in.at[0, j, 0] for j in range(3)] + [start_in.at[0, 0]]
    loads = []
    for k, source in enumerate(sources):
        loads.append(
            start(
                pltpu.make_async_copy(
                    source.at[pl.ds(first_row, win)], field.at[k, h, pl.ds(PAD, win)], own_s.at[k]
                )
            )
        )

    zeros = jnp.zeros((PAD, nz), f32)
    for k in range(FIELDS):
        for slab in range(2):
            field[k, slab, 0:PAD, :] = zeros
            field[k, slab, win + PAD : win + 2 * PAD, :] = zeros

    def clear(ref):
        def body(i, carry):
            for k in range(HALOS):
                ref[k, pl.ds(pl.multiple_of(i * 8, 8), 8), :] = zeros
            return carry

        lax.fori_loop(0, win // 8, body, 0)

    @pl.when(jnp.logical_not(has_lower))
    def _():
        clear(lower)

    @pl.when(jnp.logical_not(has_upper))
    def _():
        clear(upper)

    pl.semaphore_wait(
        barrier,
        slabs - 1 + 2 * has_next.astype(jnp.int32) + 2 * has_prev.astype(jnp.int32),
    )

    tile = tile_of(win, 24)
    bounds = chunk_bounds(win, tile)
    chunks = len(bounds)

    def swap_copy(k, c):
        lo, rows = bounds[c]
        return remote(
            sources[k].at[pl.ds(partner_row + lo, rows)],
            field.at[k, h, pl.ds(PAD + lo, rows)],
            swap_s.at[k, c], swap_r.at[k, c], t, partner,
        )

    def swap_wait(k, c):
        lo, rows = bounds[c]
        dst = field.at[k, other, pl.ds(PAD + lo, rows)]
        remote(dst, dst, swap_s.at[k, c], swap_r.at[k, c], t, partner).wait_recv()

    for c in range(chunks):
        for k in range(4):
            later(start(swap_copy(k, c)))
    for c in range(chunks):
        later(start(swap_copy(4, c)))

    def down(f, k, c, lo, rows):
        return remote(
            field.at[f, 0, pl.ds(PAD + lo, rows)], upper.at[k, pl.ds(lo, rows)],
            halo_s.at[k, 0, c], halo_r.at[k, 0, c], t, s - 2,
        )

    def up(f, k, c, lo, rows):
        return remote(
            field.at[f, 1, pl.ds(PAD + lo, rows)], lower.at[k, pl.ds(lo, rows)],
            halo_s.at[k, 1, c], halo_r.at[k, 1, c], t, s + 2,
        )

    def first_hop(k, c, which):
        @pl.when(jnp.logical_and(which == 0, has_lower))
        def _():
            down(k, k, c, *bounds[c]).start()

        @pl.when(jnp.logical_and(which == 1, has_upper))
        def _():
            up(k, k, c, *bounds[c]).start()

    for copy in loads:
        copy.wait()
    for c in range(chunks):
        for k in range(4):
            first_hop(k, c, h)

    def halo_wait(k, c, lo, rows, sides=(0, 1)):
        if 0 in sides:

            @pl.when(has_upper)
            def _():
                remote(
                    upper.at[k, pl.ds(lo, rows)], upper.at[k, pl.ds(lo, rows)],
                    halo_s.at[k, 0, c], halo_r.at[k, 0, c], t, s + 2,
                ).wait_recv()

        if 1 in sides:

            @pl.when(has_lower)
            def _():
                remote(
                    lower.at[k, pl.ds(lo, rows)], lower.at[k, pl.ds(lo, rows)],
                    halo_s.at[k, 1, c], halo_r.at[k, 1, c], t, s - 2,
                ).wait_recv()

    def halo_sent(f, k, c, lo, rows):
        later(down(f, k, c, lo, rows), has_lower)
        later(up(f, k, c, lo, rows), has_upper)

    for k in range(4):
        for c in range(chunks):
            halo_sent(k, k, c, *bounds[c])

    lane = lax.broadcasted_iota(jnp.int32, (tile, nz), 1)

    def loop(rows, size, body, init=0, offset=0):
        def step(i, carry):
            return body(pl.multiple_of(offset + i * size, 8), carry)

        return lax.fori_loop(0, rows // size, step, init)

    def coefficients(b, carry):
        windows = [field[KAPPA, slab, pl.ds(b, tile + 2 * PAD), :] for slab in range(2)]
        centre = [w[PAD : PAD + tile] for w in windows]
        before = 0.5 * (centre[0] + lower[H_KAPPA, pl.ds(b, tile), :])
        between = 0.5 * (centre[0] + centre[1])
        after = 0.5 * (centre[1] + upper[H_KAPPA, pl.ds(b, tile), :])
        across[0, pl.ds(b, tile), :] = before
        across[1, pl.ds(b, tile), :] = between
        across[2, pl.ds(b, tile), :] = after
        ends = [before + between, between + after]
        for slab in range(2):
            w, k = windows[slab], centre[slab]
            above = 0.5 * (k + w[PAD - 1 : PAD - 1 + tile])
            below = 0.5 * (k + w[PAD + 1 : PAD + 1 + tile])
            right = jnp.where(lane == nz - 1, 0.0, pltpu.roll(k, nz - 1, axis=1))
            left = jnp.where(lane == 0, 0.0, pltpu.roll(k, 1, axis=1))
            right_face = 0.5 * (k + right)
            left_face = 0.5 * (k + left)
            faces[0, slab, pl.ds(b, tile), :] = above
            faces[1, slab, pl.ds(b, tile), :] = below
            faces[2, slab, pl.ds(b, tile), :] = jnp.where(lane == nz - 1, 0.0, right_face)
            faces[3, slab, pl.ds(b, tile), :] = ends[slab] + above + below + right_face + left_face
        return carry

    def heat(windows, outer, b, size):
        centre = [w[PAD : PAD + size] for w in windows]
        between = across[1, pl.ds(b, size), :]
        images = []
        for slab in range(2):
            w, v = windows[slab], centre[slab]
            fz = faces[2, slab, pl.ds(b, size), :]
            value = between * centre[1 - slab]
            if outer[slab] is not None:
                value = value + outer[slab]
            value = value + faces[0, slab, pl.ds(b, size), :] * w[PAD - 1 : PAD - 1 + size]
            value = value + faces[1, slab, pl.ds(b, size), :] * w[PAD + 1 : PAD + 1 + size]
            value = value + fz * pltpu.roll(v, nz - 1, axis=1) + pltpu.roll(fz * v, 1, axis=1)
            images.append(value - faces[3, slab, pl.ds(b, size), :] * v)
        return centre, images

    def plain_heat(f, k, b, size):
        windows = [field[f, slab, pl.ds(b, size + 2 * PAD), :] for slab in range(2)]
        outer = (
            across[0, pl.ds(b, size), :] * lower[k, pl.ds(b, size), :],
            across[2, pl.ds(b, size), :] * upper[k, pl.ds(b, size), :],
        )
        return heat(windows, outer, b, size)

    def folded(value):
        return jnp.sum(value.reshape(-1, 8, nz), axis=0)

    def each_slab(body):
        if slabs <= 16:
            for d in range(1, slabs):
                body(d)
        else:

            def step(d, carry):
                body(d)
                return carry

            lax.fori_loop(1, slabs, step, 0)

    def sum_copy(m, d):
        return remote(
            sums.at[m, s], sums.at[m, s], sum_s.at[m, d], sum_r.at[m, d],
            t, lax.rem(s + d, slabs),
        )

    def sum_start(m, parts):
        for row, part in enumerate(parts):
            flat = jnp.sum(part, axis=0, keepdims=True)
            line = flat[:, 0:128]
            for at in range(128, nz, 128):
                line = line + flat[:, at : at + 128]
            sums[m, s, row : row + 1, :] = line
        each_slab(lambda d: sum_copy(m, d).start())

    def sum_wait(m):
        def body(d):
            source = lax.rem(s - d + slabs, slabs)
            remote(
                sums.at[m, source], sums.at[m, source], sum_s.at[m, d], sum_r.at[m, d],
                t, source,
            ).wait_recv()

        each_slab(body)
        total = jnp.sum(sums[m], axis=0)
        total = jnp.sum(total, axis=1, keepdims=True)
        return [total[row : row + 1, :] for row in range(4)]

    def halo_send(f, k, c, lo, rows):
        start(down(f, k, c, lo, rows), has_lower)
        start(up(f, k, c, lo, rows), has_upper)
        halo_sent(f, k, c, lo, rows)

    quarter = half // 2
    set_up = own
    set_down = pl.multiple_of(own + quarter, 8)
    pieces_of = (
        ((quarter, quarter + PAD), (0, quarter + PAD)),
        ((0, quarter), (quarter + PAD, quarter)),
    )

    def img_send(m, piece):
        (lo_d, rows_d), (lo_u, rows_u) = pieces_of[piece]
        copies = (
            (down(IMG + m, H_IMG + m, piece, lo_d, rows_d), has_lower),
            (up(IMG + m, H_IMG + m, piece, lo_u, rows_u), has_upper),
        )
        for copy, cond in copies:
            start(copy, cond)
            later(copy, cond)

    def img_wait(m, piece):
        halo_wait(H_IMG + m, piece, *pieces_of[piece][0], (0,))
        halo_wait(H_IMG + m, piece, *pieces_of[piece][1], (1,))

    nothing = jnp.zeros((8, nz), f32)

    def product(m):
        def body(b, carry):
            centre, images = plain_heat(RES + m, H_RES + m, b, tile)
            row = lax.broadcasted_iota(jnp.int32, (tile, nz), 0) + b
            inside = jnp.logical_and(row >= own, row < own + half)
            norm, along = carry
            for slab in range(2):
                v = centre[slab]
                w = -WIDTHS[m] * images[slab]
                field[IMG + m, slab, pl.ds(PAD + b, tile), :] = w
                masked = jnp.where(inside, v, 0.0)
                norm = norm + folded(masked * v)
                along = along + folded(masked * w)
            return norm, along

        sums_here = loop(win, tile, body, (nothing, nothing))
        img_send(m, 0)
        return sums_here

    small = tile_of(quarter, 32)

    def local(m):
        def body(b, carry):
            windows = [field[IMG + m, slab, pl.ds(b, small + 2 * PAD), :] for slab in range(2)]
            centre, images = heat(windows, (None, None), b, small)
            norm, along = carry
            for slab in range(2):
                v = centre[slab]
                norm = norm + folded(v * v)
                along = along + folded(v * images[slab])
            return norm, along

        return loop(half, small, body, (nothing, nothing), own)

    def cross(m, sums_here, sums_local):
        img_wait(m, 0)

        def body_of(side):
            ref = lower if side == 0 else upper

            def body(b, carry):
                rows = pl.ds(b, small)
                edge = across[2 * side, rows, :] * ref[H_IMG + m, rows, :]
                return carry + folded(edge * field[IMG + m, side, pl.ds(PAD + b, small), :])

            return body

        outer = loop(quarter, small, body_of(0), nothing, set_up)
        outer = loop(quarter, small, body_of(1), outer, set_down)
        norm, along = sums_local
        sum_start(m, sums_here + (norm, -WIDTHS[m] * (along + 2.0 * outer)))

    def factors(m):
        rr, rw, ww, wbw = sum_wait(m)
        step_size = rr / (rr + rw)
        mean = rw / rr
        square = step_size * step_size
        norm_next = square * jnp.maximum(ww - mean * rw, 0.0)
        along = square * jnp.maximum(mean * mean * rw - 2.0 * mean * ww + wbw, 0.0)
        momentum = norm_next / rr
        below = norm_next * (1.0 + momentum)
        curve = jnp.maximum(norm_next + along - momentum * norm_next / step_size, below)
        step_next = norm_next / jnp.maximum(curve, 1e-37)
        on_image = step_size * step_next
        return step_size + step_next * (1.0 + momentum) - on_image, on_image

    def advance(m, scalars):
        on_res, on_img = scalars

        def body(b, carry):
            at = pl.ds(PAD + b, tile)
            rows = pl.ds(b, tile)
            for slab in range(2):
                field[RES + m + 1, slab, at, :] = (
                    field[GAIN + m, slab, at, :]
                    + on_res * field[RES + m, slab, at, :]
                    - on_img * field[IMG + m, slab, at, :]
                )
            for ref in (lower, upper):
                ref[H_RES + m + 1, rows, :] = (
                    ref[H_GAIN + m, rows, :]
                    + on_res * ref[H_RES + m, rows, :]
                    - on_img * ref[H_IMG + m, rows, :]
                )
            return carry

        loop(win, tile, body)

    def coarse_residual():
        def body(b, carry):
            at = pl.ds(PAD + b, tile)
            rows = pl.ds(b, tile)
            for slab in range(2):
                field[RES + 3, slab, at, :] = (
                    field[RES, slab, at, :] + field[GAIN, slab, at, :] + field[GAIN + 1, slab, at, :]
                )
            for ref in (lower, upper):
                ref[H_RES + 3, rows, :] = (
                    ref[H_RES, rows, :] + ref[H_GAIN, rows, :] + ref[H_GAIN + 1, rows, :]
                )
            return carry

        loop(win, tile, body)

    def finish(m, scalars, slab, ref, lo, rows):
        on_res, on_img = scalars
        node = NODE + min(m, 2)

        def body(b, carry):
            at = pl.ds(PAD + own + b, small)
            ref[pl.ds(b, small), :] = (
                field[node, slab, at, :]
                + on_res * field[RES + m, slab, at, :]
                - on_img * field[IMG + m, slab, at, :]
            )
            return carry

        loop(rows, small, body, 0, lo)

    def residuals(b, carry):
        images = [plain_heat(NODE + j, H_NODE + j, b, tile)[1] for j in range(3)]
        at = pl.ds(PAD + b, tile)
        for slab in range(2):
            nodes = [field[NODE + j, slab, at, :] for j in range(3)]
            for row, f in enumerate((RES, GAIN, GAIN + 1)):
                value = nodes[row - 1] - nodes[row] if row else -nodes[0]
                for j in range(3):
                    value = value + (STEP * sweep_weight(row, j)) * images[j][slab]
                field[f, slab, at, :] = value
        return carry

    spans = []
    for c, (lo, rows) in enumerate(bounds):
        begin = lo - tile if c else 0
        end = lo + rows - (tile if c < chunks - 1 else 0)
        spans.append((begin, end - begin))

    def begin_rows(c):
        for k in range(4):
            halo_wait(k, c, *bounds[c])
        lo, rows = spans[c]
        loop(rows, tile, coefficients, 0, lo)
        loop(rows, tile, residuals, 0, lo)

    def add_start(b, carry):
        at = pl.ds(PAD + b, tile)
        for slab in range(2):
            field[RES, slab, at, :] = field[RES, slab, at, :] + field[START, slab, at, :]
        return carry

    def begin_res(c):
        swap_wait(4, c)
        lo, rows = spans[c]
        loop(rows, tile, add_start, 0, lo)
        halo_send(RES, H_RES, c, lo, rows)

    for c in range(chunks):
        for k in range(4):
            swap_wait(k, c)
            first_hop(k, c, other)
        if c > 0:
            begin_rows(c - 1)
    for c in range(chunks):
        if c == chunks - 1:
            begin_rows(c)
        begin_res(c)
    theirs = pl.multiple_of(other * half, 8)

    def mine_of(m):
        return fine_out.at[0, m, 0, pl.ds(mine, half)]

    def hand_over(m, update):
        finish(m, update, other, result.at[m], 0, half)
        later(start(remote(result.at[m], mine_of(m), out_s.at[m], out_r.at[m], t, partner)))
        finish(m, update, h, mine_of(m), 0, half)

    @pl.when(jnp.logical_not(has_prev))
    def _():
        pltpu.make_async_copy(start_in.at[0, 0], start_out.at[0, 0], copy_s.at[0]).start()
        pltpu.make_async_copy(start_in.at[0, 0], coarse_out.at[0, 0], copy_s.at[1]).start()

    def gain_send(m, chunk_range):
        for c in chunk_range:
            if c < chunks:
                halo_send(GAIN + m, H_GAIN + m, c, *spans[c])

    def gain_wait(m):
        for c in range(chunks):
            halo_wait(H_GAIN + m, c, *spans[c])

    gain_send(0, range(0, 2))
    for c in range(chunks):
        halo_wait(H_RES, c, *spans[c])
    here = product(0)
    gain_send(0, range(2, 4))
    cross(0, here, local(0))
    gain_send(0, range(4, chunks))
    img_send(0, 1)
    gain_send(1, range(0, 2))
    update = factors(0)
    gain_wait(0)
    img_wait(0, 1)
    advance(0, update)
    here = product(1)
    gain_send(1, range(2, 4))
    hand_over(0, update)
    cross(1, here, local(1))
    gain_send(1, range(4, chunks))
    img_send(1, 1)
    gain_wait(1)
    coarse_residual()
    here_coarse = product(3)
    update = factors(1)
    img_wait(1, 1)
    advance(1, update)
    here = product(2)
    cross(3, here_coarse, local(3))
    hand_over(1, update)
    cross(2, here, local(2))

    update = factors(3)
    for k, slab in enumerate((other, h)):
        finish(3, update, slab, result.at[3 + k], 0, half)
        copy = remote(
            result.at[3 + k], coarse_out.at[0, 0, pl.ds(mine, half)],
            end_s.at[k], end_r.at[k], t + 1, (partner, s)[k],
        )
        start(copy, has_next)
        later(copy, has_next)

    pieces = 4 if half % (4 * small) == 0 else 1
    piece = half // pieces

    def pass_on(at, e):
        copy = remote(
            fine_out.at[0, 2, 0, pl.ds(at, piece)], start_out.at[0, 0, pl.ds(at, piece)],
            end_s.at[e], end_r.at[e], t + 1, s,
        )
        start(copy, has_next)
        later(copy, has_next)

    update = factors(2)
    for c in range(pieces):
        finish(2, update, other, result.at[2], c * piece, piece)
        later(
            start(
                remote(
                    result.at[2, pl.ds(c * piece, piece)],
                    fine_out.at[0, 2, 0, pl.ds(mine + c * piece, piece)],
                    out_s.at[2 + c], out_r.at[2 + c], t, partner,
                )
            )
        )
    for c in range(pieces):
        finish(2, update, h, mine_of(2), c * piece, piece)
        pass_on(mine + c * piece, 2 + c)
    for c in range(pieces):
        at = theirs + c * piece
        src = fine_out.at[0, 2, 0, pl.ds(at, piece)]
        remote(src, src, out_s.at[2 + c], out_r.at[2 + c], t, partner).wait_recv()
        pass_on(at, 2 + pieces + c)

    for m in range(2):
        dst = fine_out.at[0, m, 0, pl.ds(theirs, half)]
        remote(dst, dst, out_s.at[m], out_r.at[m], t, partner).wait_recv()

    @pl.when(jnp.logical_not(has_prev))
    def _():
        pltpu.make_async_copy(start_in.at[0, 0], start_out.at[0, 0], copy_s.at[0]).wait()
        pltpu.make_async_copy(start_in.at[0, 0], coarse_out.at[0, 0], copy_s.at[1]).wait()

    @pl.when(has_prev)
    def _():
        for k in range(2):
            dst = coarse_out.at[0, 0, pl.ds((theirs, mine)[k], half)]
            remote(dst, dst, end_s.at[k], end_r.at[k], t - 1, s).wait_recv()
        for k in range(2):
            for c in range(pieces):
                dst = start_out.at[0, 0, pl.ds((mine, theirs)[k] + c * piece, piece)]
                e = 2 + k * pieces + c
                remote(dst, dst, end_s.at[e], end_r.at[e], t - 1, s).wait_recv()

    for copy, cond in pending:
        if cond is None:
            copy.wait_send()
        else:
            pl.when(cond)(copy.wait_send)

    for m in range(4):
        each_slab(lambda d, m=m: sum_copy(m, d).wait_send())


def store(fine, begin, coarse, fine_out, start_out, coarse_out, sem):
    pairs = [(begin.at[0, 0], start_out.at[0, 0]), (coarse.at[0, 0], coarse_out.at[0, 0])]
    pairs += [(fine.at[0, m, 0], fine_out.at[0, m, 0]) for m in range(fine.shape[1])]
    copies = []
    for k, (src, dst) in enumerate(pairs):
        rows = src.shape[0] // 2
        for j in range(2):
            at = pl.ds(j * rows, rows)
            copies.append(pltpu.make_async_copy(src.at[at], dst.at[at], sem.at[2 * k + j]))
    for copy in copies:
        copy.start()
    for copy in copies:
        copy.wait()


def solution(mesh):
    slices, slabs = mesh.shape["tm"], mesh.shape["space"]

    def on_device(start_value, old_nodes, diffusivity):
        ny, nz = start_value.shape[2:]
        half = ny // 2
        win = half + PAD
        chunks = len(chunk_bounds(win, tile_of(win, 24)))
        vmem = lambda *shape: pltpu.VMEM(shape, jnp.float32)
        dma = lambda *shape: pltpu.SemaphoreType.DMA(shape)

        def body(*refs):
            kernel(slices, slabs, ny, nz, *refs)

        nodes, ends = pltpu.VMEM(old_nodes.shape, jnp.float32), pltpu.VMEM(start_value.shape, jnp.float32)
        results = pl.pallas_call(
            body,
            out_shape=(nodes, ends, ends),
            in_specs=[pl.BlockSpec(memory_space=pltpu.HBM)] * 3,
            out_specs=(pl.BlockSpec(memory_space=pltpu.VMEM),) * 3,
            scratch_shapes=[
                vmem(FIELDS, 2, win + 2 * PAD, nz),
                vmem(HALOS, win, nz),
                vmem(HALOS, win, nz),
                vmem(4, 2, win, nz),
                vmem(3, win, nz),
                vmem(5, half, nz),
                vmem(4, slabs, 4, 128),
                dma(5, chunks), dma(5, chunks), dma(5),
                dma(HALOS, 2, chunks), dma(HALOS, 2, chunks),
                dma(4, slabs), dma(4, slabs),
                dma(6), dma(6), dma(10), dma(10), dma(2),
            ],
            compiler_params=pltpu.CompilerParams(
                collective_id=0, has_side_effects=True, vmem_limit_bytes=61 * 1024 * 1024
            ),
            name="pfasst",
        )(start_value, old_nodes, diffusivity)
        return pl.pallas_call(
            store,
            out_shape=tuple(jax.ShapeDtypeStruct(r.shape, jnp.float32) for r in results),
            in_specs=[pl.BlockSpec(memory_space=pltpu.VMEM)] * 3,
            out_specs=(pl.BlockSpec(memory_space=pltpu.HBM),) * 3,
            scratch_shapes=[dma(4 + 2 * old_nodes.shape[1])],
            compiler_params=pltpu.CompilerParams(vmem_limit_bytes=1024 * 1024),
            name="store",
        )(*results)

    in_specs = (
        P("tm", "space", None, None),
        P("tm", None, "space", None, None),
        P("space", None, None),
    )
    out_specs = (
        P("tm", None, "space", None, None),
        P("tm", "space", None, None),
        P("tm", "space", None, None),
    )
    return jax.shard_map(
        on_device, mesh=mesh, in_specs=in_specs, out_specs=out_specs, check_vma=False
    )
```

```python
import math

import jax
import jax.numpy as jnp
from jax import lax
from jax.experimental import pallas as pl
from jax.experimental.pallas import tpu as pltpu
from jax.sharding import PartitionSpec as P

STEP = 2.0
ROOT_SIX = math.sqrt(6.0)
NODE_TIMES = [(4.0 - ROOT_SIX) / 10.0, (4.0 + ROOT_SIX) / 10.0, 1.0]
COLLOC = [
    [
        (88.0 - 7.0 * ROOT_SIX) / 360.0,
        (296.0 - 169.0 * ROOT_SIX) / 1800.0,
        (-2.0 + 3.0 * ROOT_SIX) / 225.0,
    ],
    [
        (296.0 + 169.0 * ROOT_SIX) / 1800.0,
        (88.0 + 7.0 * ROOT_SIX) / 360.0,
        (-2.0 - 3.0 * ROOT_SIX) / 225.0,
    ],
    [(16.0 - ROOT_SIX) / 36.0, (16.0 + ROOT_SIX) / 36.0, 1.0 / 9.0],
]
MESH = pl.DeviceIdType.MESH
PAD = 8

KAPPA, NODE, START, RES, IMG, GAIN = 0, 1, 4, 5, 9, 13
FIELDS = 15
H_KAPPA, H_NODE, H_RES, H_IMG, H_GAIN = 0, 1, 4, 8, 12
HALOS = 14


def sweep_weight(row, column):
    below = COLLOC[row - 1][column] if row > 0 else 0.0
    return COLLOC[row][column] - below


def node_width(row):
    below = NODE_TIMES[row - 1] if row > 0 else 0.0
    return NODE_TIMES[row] - below


WIDTHS = [STEP * node_width(0), STEP * node_width(1), STEP * node_width(2), STEP]


def chunk_bounds(rows, tile):
    tiles = rows // tile
    parts = min(5, tiles)
    counts = [tiles // parts + (c < tiles % parts) for c in range(parts)]
    if counts[-1] > 1:
        counts[-1] -= 1
        counts[1 if parts > 2 else 0] += 1
    cuts = [tile * sum(counts[:c]) for c in range(parts + 1)]
    return [(cuts[c], cuts[c + 1] - cuts[c]) for c in range(parts)]


def tile_of(rows, most):
    best = 8
    for size in range(8, most + 1, 8):
        if rows % size == 0:
            best = size
    return best


def kernel(
    slices, slabs, ny, nz,
    start_in, nodes_in, kappa_in,
    fine_out, start_out, coarse_out,
    field, lower, upper, faces, across, outgoing, result, mail, sums,
    swap_s, swap_r, own_s, kin_s, kin_r, mail_s, mail_r, halo_s, halo_r, sum_s, sum_r, out_s, out_r, end_s, end_r, copy_s,
):
    f32 = jnp.float32
    t = lax.axis_index("tm")
    s = lax.axis_index("space")
    h = lax.rem(s, 2)
    p = lax.div(s, 2)
    pairs = slabs // 2
    half = ny // 2
    win = half + PAD
    other = 1 - h
    partner = s + 1 - 2 * h
    core = lax.rem(t, 2)
    sibling = t + 1 - 2 * core
    first_row = pl.multiple_of(h * (half - PAD), 8)
    partner_row = pl.multiple_of(other * (half - PAD), 8)
    own = pl.multiple_of(PAD * h, 8)
    mine = pl.multiple_of(h * half, 8)
    has_next = t < slices - 1
    has_prev = t > 0
    has_lower = p > 0
    has_upper = p < pairs - 1
    pending = []

    def later(ref, sem, cond=None):
        pending.append((ref, sem, cond))

    def remote(src, dst, send, recv, tm, space):
        return pltpu.make_async_remote_copy(
            src_ref=src, dst_ref=dst, send_sem=send, recv_sem=recv,
            device_id=(tm, space), device_id_type=MESH,
        )

    barrier = pltpu.get_barrier_semaphore()

    def greet(d, carry):
        pl.semaphore_signal(
            barrier, inc=1, device_id=(t, lax.rem(s + d, slabs)), device_id_type=MESH
        )
        return carry

    lax.fori_loop(1, slabs, greet, 0)
    for cond, tm in ((has_next, t + 1), (has_prev, t - 1)):

        @pl.when(cond)
        def _(tm=tm):
            for space in (s, partner):
                pl.semaphore_signal(barrier, inc=1, device_id=(tm, space), device_id_type=MESH)

    sources = [kappa_in.at[0]] + [nodes_in.at[0, j, 0] for j in range(3)] + [start_in.at[0, 0]]
    for k, source in enumerate(sources):
        pltpu.make_async_copy(
            source.at[pl.ds(first_row, win)], field.at[k, h, pl.ds(PAD, win)], own_s.at[0]
        ).start()
        pltpu.make_async_copy(
            source.at[pl.ds(partner_row, win)], outgoing.at[k], own_s.at[1]
        ).start()

    zeros = jnp.zeros((PAD, nz), f32)
    for k in range(FIELDS):
        for slab in range(2):
            field[k, slab, 0:PAD, :] = zeros
            field[k, slab, win + PAD : win + 2 * PAD, :] = zeros

    def clear(ref):
        def body(i, carry):
            for k in range(HALOS):
                ref[k, pl.ds(pl.multiple_of(i * 8, 8), 8), :] = zeros
            return carry

        lax.fori_loop(0, win // 8, body, 0)

    @pl.when(jnp.logical_not(has_lower))
    def _():
        clear(lower)

    @pl.when(jnp.logical_not(has_upper))
    def _():
        clear(upper)

    pl.semaphore_wait(
        barrier,
        slabs - 1 + 2 * has_next.astype(jnp.int32) + 2 * has_prev.astype(jnp.int32),
    )

    tile = tile_of(win, 24)
    bounds = chunk_bounds(win, tile)
    chunks = len(bounds)

    cuts = [8 * (win // 8 * q // 4) for q in range(5)]
    parts = [(cuts[q], cuts[q + 1] - cuts[q]) for q in range(4)]
    share = slices % 2 == 0

    def bounds_of(k, c):
        return bounds[c] if k else parts[c]

    def each_part(body):
        for q in range(4):
            if share:
                pl.when(core == q // 2)(lambda q=q: body(q))
            else:
                body(q)

    halves = [(cuts[0], cuts[2]), (cuts[2], cuts[4] - cuts[2])] if share else [(0, win)]

    def each_half(body, mine_too=True):
        for q, (lo, rows) in enumerate(halves):
            if share:
                pl.when((core == q) == mine_too)(lambda lo=lo, rows=rows: body(lo, rows))
            else:
                body(lo, rows)

    def arrived(ref, sem):
        remote(ref, ref, sum_s.at[0], sem, t, partner).wait_recv()

    def sent(ref, sem):
        remote(ref, ref, sem, sum_r.at[0], t, partner).wait_send()

    def swap_sem(k, c):
        return swap_r.at[4 + (k - 1) * chunks + c if k else c]

    def swap_start(k, c):
        lo, rows = bounds_of(k, c)
        remote(
            outgoing.at[k, pl.ds(lo, rows)], field.at[k, h, pl.ds(PAD + lo, rows)],
            swap_s.at[min(k, 1)], swap_sem(k, c), t, partner,
        ).start()

    def swap_wait(k, c):
        lo, rows = bounds_of(k, c)
        arrived(field.at[k, other, pl.ds(PAD + lo, rows)], swap_sem(k, c))

    def kin_ref(e, lo, rows):
        if e == 0:
            return field.at[KAPPA, other, pl.ds(PAD + lo, rows)]
        return (lower, upper)[e - 1].at[H_KAPPA, pl.ds(lo, rows)]

    def kin_copy(e, lo, rows):
        ref = kin_ref(e, lo, rows)
        return remote(ref, ref, kin_s.at[e], kin_r.at[e], sibling, s)

    def kin_start(e):
        if share:
            each_half(lambda lo, rows: kin_copy(e, lo, rows).start())

    def kin_wait(e):
        if share:
            each_half(lambda lo, rows: arrived(kin_ref(e, lo, rows), kin_r.at[e]), False)

    def kin_sent(e):
        if share:
            each_half(lambda lo, rows: sent(kin_ref(e, lo, rows), kin_s.at[e]))

    pltpu.make_async_copy(outgoing, outgoing, own_s.at[1]).wait()
    each_part(lambda q: swap_start(0, q))
    for c in range(chunks):
        for k in range(1, 4):
            swap_start(k, c)
    for c in range(chunks):
        swap_start(4, c)
    later(outgoing.at[pl.ds(1, 4)], swap_s.at[1])

    def halo_sems(k, c, side):
        if k == H_KAPPA:
            slots = 0, 0
        elif k < H_RES:
            slots = 1, 1 + c
        elif k == H_RES:
            slots = 2, 1 + chunks
        elif k >= H_GAIN:
            slots = 3, 2 + chunks + k - H_GAIN
        else:
            m = k - H_IMG
            slots = 4 + m // 2, 4 + chunks + (2 * m + c if m < 2 else 2 + m)
        return halo_s.at[side, slots[0]], halo_r.at[side, slots[1]]

    def down(f, k, c, lo, rows):
        return remote(
            field.at[f, 0, pl.ds(PAD + lo, rows)], upper.at[k, pl.ds(lo, rows)],
            *halo_sems(k, c, 0), t, s - 2,
        )

    def up(f, k, c, lo, rows):
        return remote(
            field.at[f, 1, pl.ds(PAD + lo, rows)], lower.at[k, pl.ds(lo, rows)],
            *halo_sems(k, c, 1), t, s + 2,
        )

    def first_hop(k, c, which):
        @pl.when(jnp.logical_and(which == 0, has_lower))
        def _():
            down(k, k, c, *bounds_of(k, c)).start()

        @pl.when(jnp.logical_and(which == 1, has_upper))
        def _():
            up(k, k, c, *bounds_of(k, c)).start()

    own_rows = field.at[pl.ds(0, 5), h, pl.ds(PAD, win)]
    pltpu.make_async_copy(own_rows, own_rows, own_s.at[0]).wait()
    each_part(lambda q: first_hop(0, q, h))
    for c in range(chunks):
        for k in range(1, 4):
            first_hop(k, c, h)

    def halo_wait(k, c, lo, rows, sides=(0, 1), fields=None):
        which = k if fields is None else pl.ds(k, fields)
        for side, ref, cond in ((0, upper, has_upper), (1, lower, has_lower)):
            if side in sides:

                @pl.when(cond)
                def _(side=side, ref=ref):
                    arrived(ref.at[which, pl.ds(lo, rows)], halo_sems(k, c, side)[1])

    def halo_later(f, slot, lo, rows, fields=None, sides=(0, 1)):
        which = f if fields is None else pl.ds(f, fields)
        for side in sides:
            ref = field.at[which, side, pl.ds(PAD + lo, rows)]
            later(ref, halo_s.at[side, slot], (has_lower, has_upper)[side])

    lane = lax.broadcasted_iota(jnp.int32, (tile, nz), 1)

    def loop(rows, size, body, init=0, offset=0):
        def step(i, carry):
            return body(pl.multiple_of(offset + i * size, 8), carry)

        return lax.fori_loop(0, rows // size, step, init)

    def coefficients(b, carry):
        windows = [field[KAPPA, slab, pl.ds(b, tile + 2 * PAD), :] for slab in range(2)]
        centre = [w[PAD : PAD + tile] for w in windows]
        before = 0.5 * (centre[0] + lower[H_KAPPA, pl.ds(b, tile), :])
        between = 0.5 * (centre[0] + centre[1])
        after = 0.5 * (centre[1] + upper[H_KAPPA, pl.ds(b, tile), :])
        across[0, pl.ds(b, tile), :] = before
        across[1, pl.ds(b, tile), :] = between
        across[2, pl.ds(b, tile), :] = after
        ends = [before + between, between + after]
        for slab in range(2):
            w, k = windows[slab], centre[slab]
            above = 0.5 * (k + w[PAD - 1 : PAD - 1 + tile])
            below = 0.5 * (k + w[PAD + 1 : PAD + 1 + tile])
            right = jnp.where(lane == nz - 1, 0.0, pltpu.roll(k, nz - 1, axis=1))
            left = jnp.where(lane == 0, 0.0, pltpu.roll(k, 1, axis=1))
            right_face = 0.5 * (k + right)
            left_face = 0.5 * (k + left)
            faces[0, slab, pl.ds(b, tile), :] = above
            faces[1, slab, pl.ds(b, tile), :] = below
            faces[2, slab, pl.ds(b, tile), :] = jnp.where(lane == nz - 1, 0.0, right_face)
            faces[3, slab, pl.ds(b, tile), :] = ends[slab] + above + below + right_face + left_face
        return carry

    def heat(windows, outer, b, size):
        centre = [w[PAD : PAD + size] for w in windows]
        between = across[1, pl.ds(b, size), :]
        images = []
        for slab in range(2):
            w, v = windows[slab], centre[slab]
            fz = faces[2, slab, pl.ds(b, size), :]
            value = between * centre[1 - slab]
            if outer[slab] is not None:
                value = value + outer[slab]
            value = value + faces[0, slab, pl.ds(b, size), :] * w[PAD - 1 : PAD - 1 + size]
            value = value + faces[1, slab, pl.ds(b, size), :] * w[PAD + 1 : PAD + 1 + size]
            value = value + fz * pltpu.roll(v, nz - 1, axis=1) + pltpu.roll(fz * v, 1, axis=1)
            images.append(value - faces[3, slab, pl.ds(b, size), :] * v)
        return centre, images

    def plain_heat(f, k, b, size):
        windows = [field[f, slab, pl.ds(b, size + 2 * PAD), :] for slab in range(2)]
        outer = (
            across[0, pl.ds(b, size), :] * lower[k, pl.ds(b, size), :],
            across[2, pl.ds(b, size), :] * upper[k, pl.ds(b, size), :],
        )
        return heat(windows, outer, b, size)

    def folded(value):
        return jnp.sum(value.reshape(-1, 8, nz), axis=0)

    def each_slab(body):
        if slabs <= 16:
            for d in range(1, slabs):
                body(d)
        else:

            def step(d, carry):
                body(d)
                return carry

            lax.fori_loop(1, slabs, step, 0)

    def sum_copy(m, d):
        return remote(
            sums.at[m, s], sums.at[m, s], sum_s.at[0], sum_r.at[m], t, lax.rem(s + d, slabs),
        )

    def sum_start(m, parts):
        for row, part in enumerate(parts):
            flat = jnp.sum(part, axis=0, keepdims=True)
            line = flat[:, 0:128]
            for at in range(128, nz, 128):
                line = line + flat[:, at : at + 128]
            sums[m, s, row : row + 1, :] = line
        each_slab(lambda d: sum_copy(m, d).start())

    def sum_wait(m):
        arrived(sums.at[m, pl.ds(0, slabs - 1)], sum_r.at[m])
        total = jnp.sum(sums[m], axis=0)
        total = jnp.sum(total, axis=1, keepdims=True)
        return [total[row : row + 1, :] for row in range(4)]

    def halo_send(f, k, c, lo, rows):
        pl.when(has_lower)(down(f, k, c, lo, rows).start)
        pl.when(has_upper)(up(f, k, c, lo, rows).start)

    quarter = half // 2
    set_up = own
    set_down = pl.multiple_of(own + quarter, 8)
    pieces_of = (
        ((quarter, quarter + PAD), (0, quarter + PAD)),
        ((0, quarter), (quarter + PAD, quarter)),
    )

    def img_send(m, piece):
        (lo_d, rows_d), (lo_u, rows_u) = pieces_of[piece]
        pl.when(has_lower)(down(IMG + m, H_IMG + m, piece, lo_d, rows_d).start)
        pl.when(has_upper)(up(IMG + m, H_IMG + m, piece, lo_u, rows_u).start)

    def img_wait(m, piece):
        halo_wait(H_IMG + m, piece, *pieces_of[piece][0], (0,))
        halo_wait(H_IMG + m, piece, *pieces_of[piece][1], (1,))

    nothing = jnp.zeros((8, nz), f32)

    def product(m):
        def body(b, carry):
            centre, images = plain_heat(RES + m, H_RES + m, b, tile)
            row = lax.broadcasted_iota(jnp.int32, (tile, nz), 0) + b
            inside = jnp.logical_and(row >= own, row < own + half)
            norm, along = carry
            for slab in range(2):
                v = centre[slab]
                w = -WIDTHS[m] * images[slab]
                field[IMG + m, slab, pl.ds(PAD + b, tile), :] = w
                masked = jnp.where(inside, v, 0.0)
                norm = norm + folded(masked * v)
                along = along + folded(masked * w)
            return norm, along

        sums_here = loop(win, tile, body, (nothing, nothing))
        img_send(m, 0)
        return sums_here

    small = tile_of(quarter, 32)

    def local(m):
        def body(b, carry):
            windows = [field[IMG + m, slab, pl.ds(b, small + 2 * PAD), :] for slab in range(2)]
            centre, images = heat(windows, (None, None), b, small)
            norm, along = carry
            for slab in range(2):
                v = centre[slab]
                norm = norm + folded(v * v)
                along = along + folded(v * images[slab])
            return norm, along

        return loop(half, small, body, (nothing, nothing), own)

    def cross(m, sums_here, sums_local):
        img_wait(m, 0)

        def body_of(side):
            ref = lower if side == 0 else upper

            def body(b, carry):
                rows = pl.ds(b, small)
                edge = across[2 * side, rows, :] * ref[H_IMG + m, rows, :]
                return carry + folded(edge * field[IMG + m, side, pl.ds(PAD + b, small), :])

            return body

        outer = loop(quarter, small, body_of(0), nothing, set_up)
        outer = loop(quarter, small, body_of(1), outer, set_down)
        norm, along = sums_local
        sum_start(m, sums_here + (norm, -WIDTHS[m] * (along + 2.0 * outer)))

    def factors(m):
        rr, rw, ww, wbw = sum_wait(m)
        step_size = rr / (rr + rw)
        mean = rw / rr
        square = step_size * step_size
        norm_next = square * jnp.maximum(ww - mean * rw, 0.0)
        along = square * jnp.maximum(mean * mean * rw - 2.0 * mean * ww + wbw, 0.0)
        momentum = norm_next / rr
        below = norm_next * (1.0 + momentum)
        curve = jnp.maximum(norm_next + along - momentum * norm_next / step_size, below)
        step_next = norm_next / jnp.maximum(curve, 1e-37)
        on_image = step_size * step_next
        return step_size + step_next * (1.0 + momentum) - on_image, on_image

    def advance(m, scalars):
        on_res, on_img = scalars

        def body(b, carry):
            at = pl.ds(PAD + b, tile)
            rows = pl.ds(b, tile)
            for slab in range(2):
                field[RES + m + 1, slab, at, :] = (
                    field[GAIN + m, slab, at, :]
                    + on_res * field[RES + m, slab, at, :]
                    - on_img * field[IMG + m, slab, at, :]
                )
            for ref in (lower, upper):
                ref[H_RES + m + 1, rows, :] = (
                    ref[H_GAIN + m, rows, :]
                    + on_res * ref[H_RES + m, rows, :]
                    - on_img * ref[H_IMG + m, rows, :]
                )
            return carry

        loop(win, tile, body)

    def coarse_residual():
        def body(b, carry):
            at = pl.ds(PAD + b, tile)
            for slab in range(2):
                field[RES + 3, slab, at, :] = (
                    field[RES, slab, at, :] + field[GAIN, slab, at, :] + field[GAIN + 1, slab, at, :]
                )
            return carry

        loop(win, tile, body)

    def coarse_halo():
        def body(b, carry):
            rows = pl.ds(b, tile)
            for ref in (lower, upper):
                ref[H_RES + 3, rows, :] = (
                    ref[H_RES, rows, :] + ref[H_GAIN, rows, :] + ref[H_GAIN + 1, rows, :]
                )
            return carry

        loop(win, tile, body)

    def mail_copy(k):
        return remote(
            field.at[(RES + 3, IMG + 3)[k], other, pl.ds(PAD + own, half)], mail.at[k],
            mail_s.at[k], mail_r.at[k], t, partner,
        )

    def mail_send(k):
        pl.when(has_next)(mail_copy(k).start)
        later(mail.at[k], mail_s.at[k], has_next)

    def mail_wait(k):
        pl.when(has_next)(mail_copy(k).wait_recv)

    def finish(m, scalars, slab, ref, lo, rows):
        on_res, on_img = scalars
        node = NODE + min(m, 2)

        def body(b, carry):
            at = pl.ds(PAD + own + b, small)
            ref[pl.ds(b, small), :] = (
                field[node, slab, at, :]
                + on_res * field[RES + m, slab, at, :]
                - on_img * field[IMG + m, slab, at, :]
            )
            return carry

        loop(rows, small, body, 0, lo)

    def residuals(b, carry):
        images = [plain_heat(NODE + j, H_NODE + j, b, tile)[1] for j in range(3)]
        at = pl.ds(PAD + b, tile)
        for slab in range(2):
            nodes = [field[NODE + j, slab, at, :] for j in range(3)]
            for row, f in enumerate((RES, GAIN, GAIN + 1)):
                value = nodes[row - 1] - nodes[row] if row else -nodes[0]
                for j in range(3):
                    value = value + (STEP * sweep_weight(row, j)) * images[j][slab]
                field[f, slab, at, :] = value
        return carry

    spans = []
    for c, (lo, rows) in enumerate(bounds):
        begin = lo - tile if c else 0
        end = lo + rows - (tile if c < chunks - 1 else 0)
        spans.append((begin, end - begin))

    def begin_rows(c):
        halo_wait(H_NODE, c, *bounds[c], fields=3)
        lo, rows = spans[c]
        loop(rows, tile, coefficients, 0, lo)
        loop(rows, tile, residuals, 0, lo)

    def add_start(b, carry):
        at = pl.ds(PAD + b, tile)
        for slab in range(2):
            field[RES, slab, at, :] = field[RES, slab, at, :] + field[START, slab, at, :]
        return carry

    def begin_res(c):
        swap_wait(4, c)
        lo, rows = spans[c]
        loop(rows, tile, add_start, 0, lo)
        halo_send(RES, H_RES, c, lo, rows)

    def pass_kappa(q):
        swap_wait(0, q)
        if share:
            kin_copy(0, *parts[q]).start()
        first_hop(0, q, other)

    each_part(pass_kappa)
    for c in range(chunks):
        for k in range(1, 4):
            swap_wait(k, c)
            first_hop(k, c, other)
        if c == 0:
            each_half(lambda lo, rows: halo_wait(H_KAPPA, 0, lo, rows))
            pl.when(has_lower)(lambda: kin_start(1))
            pl.when(has_upper)(lambda: kin_start(2))
        if c == min(1, chunks - 1):
            kin_wait(0)
            pl.when(has_lower)(lambda: kin_wait(1))
            pl.when(has_upper)(lambda: kin_wait(2))
        if c > 0:
            begin_rows(c - 1)
    for c in range(chunks):
        if c == chunks - 1:
            begin_rows(c)
        begin_res(c)
    theirs = pl.multiple_of(other * half, 8)

    def mine_of(m):
        return fine_out.at[0, m, 0, pl.ds(mine, half)]

    def hand_over(m, update):
        finish(m, update, other, result.at[m], 0, half)
        remote(result.at[m], mine_of(m), out_s.at[m], out_r.at[m], t, partner).start()
        later(result.at[m], out_s.at[m])
        finish(m, update, h, mine_of(m), 0, half)

    @pl.when(jnp.logical_not(has_prev))
    def _():
        pltpu.make_async_copy(start_in.at[0, 0], start_out.at[0, 0], copy_s.at[0]).start()
        pltpu.make_async_copy(start_in.at[0, 0], coarse_out.at[0, 0], copy_s.at[1]).start()

    def gain_send(m, chunk_range):
        for c in chunk_range:
            if c < chunks:
                halo_send(GAIN + m, H_GAIN + m, c, *spans[c])

    def gain_wait(m):
        halo_wait(H_GAIN + m, 0, 0, win)

    gain_send(0, range(0, 2))
    halo_wait(H_RES, 0, 0, win)
    here = product(0)
    gain_send(0, range(2, 4))
    cross(0, here, local(0))
    gain_send(0, range(4, chunks))
    img_send(0, 1)
    gain_send(1, range(0, 2))
    coarse_residual()
    mail_send(0)
    update = factors(0)
    gain_wait(0)
    img_wait(0, 1)
    advance(0, update)
    here = product(1)
    gain_send(1, range(2, 4))
    cross(1, here, local(1))
    hand_over(0, update)
    gain_send(1, range(4, chunks))
    img_send(1, 1)
    gain_wait(1)
    coarse_halo()
    here_coarse = product(3)
    mail_send(1)
    update = factors(1)
    img_wait(1, 1)
    advance(1, update)
    here = product(2)
    cross(3, here_coarse, local(3))
    cross(2, here, local(2))
    hand_over(1, update)

    def coarse_send(k):
        copy = remote(
            result.at[3 + k], coarse_out.at[0, 0, pl.ds((mine, theirs)[k], half)],
            end_s.at[0], end_r.at[0], t + 1, s,
        )
        pl.when(has_next)(copy.start)

    update = factors(3)
    finish(3, update, h, result.at[3], 0, half)
    coarse_send(0)
    for k in range(2):
        mail_wait(k)

    def coarse_rest(b, carry):
        rows = pl.ds(b, small)
        result[4, rows, :] = (
            outgoing[3, pl.ds(PAD * other + b, small), :]
            + update[0] * mail[0, rows, :]
            - update[1] * mail[1, rows, :]
        )
        return carry

    loop(half, small, coarse_rest)
    coarse_send(1)

    pieces = 4 if half % (4 * small) == 0 else 1
    piece = half // pieces

    def pass_on(at):
        copy = remote(
            fine_out.at[0, 2, 0, pl.ds(at, piece)], start_out.at[0, 0, pl.ds(at, piece)],
            end_s.at[1], end_r.at[1], t + 1, s,
        )
        pl.when(has_next)(copy.start)

    update = factors(2)
    for c in range(pieces):
        finish(2, update, other, result.at[2], c * piece, piece)
        remote(
            result.at[2, pl.ds(c * piece, piece)],
            fine_out.at[0, 2, 0, pl.ds(mine + c * piece, piece)],
            out_s.at[2], out_r.at[2 + c], t, partner,
        ).start()
    for c in range(pieces):
        finish(2, update, h, mine_of(2), c * piece, piece)
        pass_on(mine + c * piece)
    for c in range(pieces):
        at = theirs + c * piece
        src = fine_out.at[0, 2, 0, pl.ds(at, piece)]
        arrived(src, out_r.at[2 + c])
        pass_on(at)

    for m in range(2):
        dst = fine_out.at[0, m, 0, pl.ds(theirs, half)]
        arrived(dst, out_r.at[m])

    @pl.when(jnp.logical_not(has_prev))
    def _():
        pltpu.make_async_copy(start_in.at[0, 0], start_out.at[0, 0], copy_s.at[0]).wait()
        pltpu.make_async_copy(start_in.at[0, 0], coarse_out.at[0, 0], copy_s.at[1]).wait()

    @pl.when(has_prev)
    def _():
        arrived(coarse_out.at[0, 0], end_r.at[0])
        arrived(start_out.at[0, 0], end_r.at[1])

    each_half(lambda lo, rows: sent(outgoing.at[0, pl.ds(lo, rows)], swap_s.at[0]))
    for side, cond in ((0, has_lower), (1, has_upper)):

        @pl.when(cond)
        def _(side=side):
            each_half(
                lambda lo, rows: sent(
                    field.at[KAPPA, side, pl.ds(PAD + lo, rows)], halo_s.at[side, 0]
                )
            )

    kin_sent(0)
    pl.when(has_lower)(lambda: kin_sent(1))
    pl.when(has_upper)(lambda: kin_sent(2))
    halo_later(NODE, 1, 0, win, 3)
    halo_later(RES, 2, 0, win)
    halo_later(GAIN, 3, 0, win, 2)
    halo_later(IMG, 4, 0, win, 2)
    for side in range(2):
        halo_later(IMG + 2, 5, *pieces_of[0][side], 2, (side,))
    later(result.at[2], out_s.at[2])
    later(result.at[pl.ds(3, 2)], end_s.at[0], has_next)
    later(fine_out.at[0, 2, 0], end_s.at[1], has_next)
    later(sums.at[pl.ds(0, 4), pl.ds(0, slabs - 1)], sum_s.at[0])
    for ref, sem, cond in pending:
        if cond is None:
            sent(ref, sem)
        else:
            pl.when(cond)(lambda ref=ref, sem=sem: sent(ref, sem))


def store(fine, begin, coarse, fine_out, start_out, coarse_out, sem):
    pairs = [(begin.at[0, 0], start_out.at[0, 0]), (coarse.at[0, 0], coarse_out.at[0, 0])]
    pairs += [(fine.at[0, m, 0], fine_out.at[0, m, 0]) for m in range(fine.shape[1])]
    copies = []
    for k, (src, dst) in enumerate(pairs):
        rows = src.shape[0] // 2
        for j in range(2):
            at = pl.ds(j * rows, rows)
            copies.append(pltpu.make_async_copy(src.at[at], dst.at[at], sem.at[2 * k + j]))
    for copy in copies:
        copy.start()
    for copy in copies:
        copy.wait()


def solution(mesh):
    slices, slabs = mesh.shape["tm"], mesh.shape["space"]

    def on_device(start_value, old_nodes, diffusivity):
        ny, nz = start_value.shape[2:]
        half = ny // 2
        win = half + PAD
        chunks = len(chunk_bounds(win, tile_of(win, 24)))
        vmem = lambda *shape: pltpu.VMEM(shape, jnp.float32)
        dma = lambda *shape: pltpu.SemaphoreType.DMA(shape)

        def body(*refs):
            kernel(slices, slabs, ny, nz, *refs)

        nodes, ends = pltpu.VMEM(old_nodes.shape, jnp.float32), pltpu.VMEM(start_value.shape, jnp.float32)
        results = pl.pallas_call(
            body,
            out_shape=(nodes, ends, ends),
            in_specs=[pl.BlockSpec(memory_space=pltpu.HBM)] * 3,
            out_specs=(pl.BlockSpec(memory_space=pltpu.VMEM),) * 3,
            scratch_shapes=[
                vmem(FIELDS, 2, win + 2 * PAD, nz),
                vmem(HALOS, win, nz),
                vmem(HALOS, win, nz),
                vmem(4, 2, win, nz),
                vmem(3, win, nz),
                vmem(5, win, nz),
                vmem(5, half, nz),
                vmem(2, half, nz),
                vmem(4, slabs, 4, 128),
                dma(2), dma(4 + 4 * chunks), dma(2), dma(3), dma(3), dma(2), dma(2),
                dma(2, 6), dma(2, 10 + chunks), dma(1), dma(4),
                dma(3), dma(6), dma(2), dma(2), dma(2),
            ],
            compiler_params=pltpu.CompilerParams(
                collective_id=0, has_side_effects=True, vmem_limit_bytes=61 * 1024 * 1024
            ),
            name="pfasst",
        )(start_value, old_nodes, diffusivity)
        return pl.pallas_call(
            store,
            out_shape=tuple(jax.ShapeDtypeStruct(r.shape, jnp.float32) for r in results),
            in_specs=[pl.BlockSpec(memory_space=pltpu.VMEM)] * 3,
            out_specs=(pl.BlockSpec(memory_space=pltpu.HBM),) * 3,
            scratch_shapes=[dma(4 + 2 * old_nodes.shape[1])],
            compiler_params=pltpu.CompilerParams(vmem_limit_bytes=1024 * 1024),
            name="store",
        )(*results)

    in_specs = (
        P("tm", "space", None, None),
        P("tm", None, "space", None, None),
        P("space", None, None),
    )
    out_specs = (
        P("tm", None, "space", None, None),
        P("tm", "space", None, None),
        P("tm", "space", None, None),
    )
    return jax.shard_map(
        on_device, mesh=mesh, in_specs=in_specs, out_specs=out_specs, check_vma=False
    )
```

```python
import math

import jax
import jax.numpy as jnp
from jax import lax
from jax.experimental import pallas as pl
from jax.experimental.pallas import tpu as pltpu
from jax.sharding import PartitionSpec as P

STEP = 2.0
ROOT_SIX = math.sqrt(6.0)
NODE_TIMES = [(4.0 - ROOT_SIX) / 10.0, (4.0 + ROOT_SIX) / 10.0, 1.0]
COLLOC = [
    [
        (88.0 - 7.0 * ROOT_SIX) / 360.0,
        (296.0 - 169.0 * ROOT_SIX) / 1800.0,
        (-2.0 + 3.0 * ROOT_SIX) / 225.0,
    ],
    [
        (296.0 + 169.0 * ROOT_SIX) / 1800.0,
        (88.0 + 7.0 * ROOT_SIX) / 360.0,
        (-2.0 - 3.0 * ROOT_SIX) / 225.0,
    ],
    [(16.0 - ROOT_SIX) / 36.0, (16.0 + ROOT_SIX) / 36.0, 1.0 / 9.0],
]
MESH = pl.DeviceIdType.MESH
PAD = 8
SOUTH_PARTS = 2

KAPPA, NODE, START, RES, IMG, GAIN = 0, 1, 4, 5, 9, 13
FIELDS = 15
H_KAPPA, H_NODE, H_RES, H_IMG, H_GAIN = 0, 1, 4, 8, 12
HALOS = 14


def sweep_weight(row, column):
    below = COLLOC[row - 1][column] if row > 0 else 0.0
    return COLLOC[row][column] - below


def node_width(row):
    below = NODE_TIMES[row - 1] if row > 0 else 0.0
    return NODE_TIMES[row] - below


WIDTHS = [STEP * node_width(0), STEP * node_width(1), STEP * node_width(2), STEP]


def chunk_bounds(rows, tile):
    tiles = rows // tile
    parts = min(5, tiles)
    counts = [tiles // parts + (c < tiles % parts) for c in range(parts)]
    if counts[-1] > 1:
        counts[-1] -= 1
        counts[1 if parts > 2 else 0] += 1
    cuts = [tile * sum(counts[:c]) for c in range(parts + 1)]
    return [(cuts[c], cuts[c + 1] - cuts[c]) for c in range(parts)]


def tile_of(rows, most):
    best = 8
    for size in range(8, most + 1, 8):
        if rows % size == 0:
            best = size
    return best


def kernel(
    slices, slabs, ny, nz,
    start_in, nodes_in, kappa_in,
    fine_out, start_out, coarse_out,
    field, lower, upper, faces, across, outgoing, result, mail, kept, marks, sums,
    swap_s, swap_r, own_s, kin_s, kin_r, mail_s, mail_r, kept_s, kept_r, halo_s, halo_r, sum_s, sum_r, out_s, out_r, end_s, end_r, copy_s,
):
    f32 = jnp.float32
    t = lax.axis_index("tm")
    s = lax.axis_index("space")
    h = lax.rem(s, 2)
    p = lax.div(s, 2)
    pairs = slabs // 2
    half = ny // 2
    win = half + PAD
    other = 1 - h
    partner = s + 1 - 2 * h
    core = lax.rem(t, 2)
    sibling = t + 1 - 2 * core
    first_row = pl.multiple_of(h * (half - PAD), 8)
    partner_row = pl.multiple_of(other * (half - PAD), 8)
    own = pl.multiple_of(PAD * h, 8)
    mine = pl.multiple_of(h * half, 8)
    has_next = t < slices - 1
    has_prev = t > 0
    has_lower = p > 0
    has_upper = p < pairs - 1
    pending = []

    def later(ref, sem, cond=None):
        pending.append((ref, sem, cond))

    def remote(src, dst, send, recv, tm, space):
        return pltpu.make_async_remote_copy(
            src_ref=src, dst_ref=dst, send_sem=send, recv_sem=recv,
            device_id=(tm, space), device_id_type=MESH,
        )

    barrier = pltpu.get_barrier_semaphore()

    def greet(d, carry):
        pl.semaphore_signal(
            barrier, inc=1, device_id=(t, lax.rem(s + d, slabs)), device_id_type=MESH
        )
        return carry

    lax.fori_loop(1, slabs, greet, 0)
    for cond, tm in ((has_next, t + 1), (has_prev, t - 1)):

        @pl.when(cond)
        def _(tm=tm):
            for space in (s, partner):
                pl.semaphore_signal(barrier, inc=1, device_id=(tm, space), device_id_type=MESH)

    sources = [kappa_in.at[0]] + [nodes_in.at[0, j, 0] for j in range(3)] + [start_in.at[0, 0]]
    for k, source in enumerate(sources):
        pltpu.make_async_copy(
            source.at[pl.ds(first_row, win)], field.at[k, h, pl.ds(PAD, win)], own_s.at[0]
        ).start()
        pltpu.make_async_copy(
            source.at[pl.ds(partner_row, win)], outgoing.at[k], own_s.at[1]
        ).start()

    zeros = jnp.zeros((PAD, nz), f32)
    for k in range(FIELDS):
        for slab in range(2):
            field[k, slab, 0:PAD, :] = zeros
            field[k, slab, win + PAD : win + 2 * PAD, :] = zeros

    def clear(ref):
        def body(i, carry):
            for k in range(HALOS):
                ref[k, pl.ds(pl.multiple_of(i * 8, 8), 8), :] = zeros
            return carry

        lax.fori_loop(0, win // 8, body, 0)

    @pl.when(jnp.logical_not(has_lower))
    def _():
        clear(lower)

    @pl.when(jnp.logical_not(has_upper))
    def _():
        clear(upper)

    pl.semaphore_wait(
        barrier,
        slabs - 1 + 2 * has_next.astype(jnp.int32) + 2 * has_prev.astype(jnp.int32),
    )

    tile = tile_of(win, 24)
    bounds = chunk_bounds(win, tile)
    chunks = len(bounds)

    cuts = [8 * (win // 8 * q // 4) for q in range(5)]
    parts = [(cuts[q], cuts[q + 1] - cuts[q]) for q in range(4)]
    share = slices % 2 == 0

    def bounds_of(k, c):
        return bounds[c] if k else parts[c]

    def each_part(body):
        for q in range(4):
            if share:
                pl.when(core == (q >= SOUTH_PARTS))(lambda q=q: body(q))
            else:
                body(q)

    first = cuts[SOUTH_PARTS]
    halves = [(0, first), (first, win - first)] if share else [(0, win)]

    def each_half(body, mine_too=True):
        for q, (lo, rows) in enumerate(halves):
            if share and rows:
                pl.when((core == q) == mine_too)(lambda lo=lo, rows=rows: body(lo, rows))
            elif not share:
                body(lo, rows)

    def arrived(ref, sem):
        remote(ref, ref, sum_s.at[0], sem, t, partner).wait_recv()

    def sent(ref, sem):
        remote(ref, ref, sem, sum_r.at[0], t, partner).wait_send()

    def swap_sem(k, c):
        return swap_r.at[4 + (k - 1) * chunks + c if k else c]

    def swap_start(k, c):
        lo, rows = bounds_of(k, c)
        remote(
            outgoing.at[k, pl.ds(lo, rows)], field.at[k, h, pl.ds(PAD + lo, rows)],
            swap_s.at[min(k, 1)], swap_sem(k, c), t, partner,
        ).start()

    def swap_wait(k, c):
        lo, rows = bounds_of(k, c)
        arrived(field.at[k, other, pl.ds(PAD + lo, rows)], swap_sem(k, c))

    def kin_ref(e, lo, rows):
        if e == 0:
            return field.at[KAPPA, other, pl.ds(PAD + lo, rows)]
        return (lower, upper)[e - 1].at[H_KAPPA, pl.ds(lo, rows)]

    def kin_copy(e, lo, rows):
        ref = kin_ref(e, lo, rows)
        return remote(ref, ref, kin_s.at[e], kin_r.at[e], sibling, s)

    def kin_start(e):
        if share:
            each_half(lambda lo, rows: kin_copy(e, lo, rows).start())

    def kin_wait(e):
        if share:
            each_half(lambda lo, rows: arrived(kin_ref(e, lo, rows), kin_r.at[e]), False)

    def kin_sent(e):
        if share:
            each_half(lambda lo, rows: sent(kin_ref(e, lo, rows), kin_s.at[e]))

    pltpu.make_async_copy(outgoing, outgoing, own_s.at[1]).wait()
    each_part(lambda q: swap_start(0, q))
    for c in range(chunks):
        for k in range(1, 4):
            swap_start(k, c)
    for c in range(chunks):
        swap_start(4, c)
    later(outgoing.at[pl.ds(1, 4)], swap_s.at[1])

    def halo_sems(k, c, side):
        if k == H_KAPPA:
            slots = 0, 0
        elif k < H_RES:
            slots = 1, 1 + c
        elif k == H_RES:
            slots = 2, 1 + chunks
        elif k >= H_GAIN:
            slots = 3, 2 + chunks + k - H_GAIN
        else:
            m = k - H_IMG
            slots = 4 + m // 2, 4 + chunks + (2 * m + c if m < 2 else 2 + m)
        return halo_s.at[side, slots[0]], halo_r.at[side, slots[1]]

    def down(f, k, c, lo, rows):
        return remote(
            field.at[f, 0, pl.ds(PAD + lo, rows)], upper.at[k, pl.ds(lo, rows)],
            *halo_sems(k, c, 0), t, s - 2,
        )

    def up(f, k, c, lo, rows):
        return remote(
            field.at[f, 1, pl.ds(PAD + lo, rows)], lower.at[k, pl.ds(lo, rows)],
            *halo_sems(k, c, 1), t, s + 2,
        )

    def first_hop(k, c, which):
        @pl.when(jnp.logical_and(which == 0, has_lower))
        def _():
            down(k, k, c, *bounds_of(k, c)).start()

        @pl.when(jnp.logical_and(which == 1, has_upper))
        def _():
            up(k, k, c, *bounds_of(k, c)).start()

    own_rows = field.at[pl.ds(0, 5), h, pl.ds(PAD, win)]
    pltpu.make_async_copy(own_rows, own_rows, own_s.at[0]).wait()
    each_part(lambda q: first_hop(0, q, h))
    for c in range(chunks):
        for k in range(1, 4):
            first_hop(k, c, h)

    def halo_wait(k, c, lo, rows, sides=(0, 1), fields=None):
        which = k if fields is None else pl.ds(k, fields)
        for side, ref, cond in ((0, upper, has_upper), (1, lower, has_lower)):
            if side in sides:

                @pl.when(cond)
                def _(side=side, ref=ref):
                    arrived(ref.at[which, pl.ds(lo, rows)], halo_sems(k, c, side)[1])

    def halo_later(f, slot, lo, rows, fields=None, sides=(0, 1)):
        which = f if fields is None else pl.ds(f, fields)
        for side in sides:
            ref = field.at[which, side, pl.ds(PAD + lo, rows)]
            later(ref, halo_s.at[side, slot], (has_lower, has_upper)[side])

    lane = lax.broadcasted_iota(jnp.int32, (tile, nz), 1)

    def loop(rows, size, body, init=0, offset=0):
        def step(i, carry):
            return body(pl.multiple_of(offset + i * size, 8), carry)

        return lax.fori_loop(0, rows // size, step, init)

    def coefficients(b, carry):
        windows = [field[KAPPA, slab, pl.ds(b, tile + 2 * PAD), :] for slab in range(2)]
        centre = [w[PAD : PAD + tile] for w in windows]
        before = 0.5 * (centre[0] + lower[H_KAPPA, pl.ds(b, tile), :])
        between = 0.5 * (centre[0] + centre[1])
        after = 0.5 * (centre[1] + upper[H_KAPPA, pl.ds(b, tile), :])
        across[0, pl.ds(b, tile), :] = before
        across[1, pl.ds(b, tile), :] = between
        across[2, pl.ds(b, tile), :] = after
        ends = [before + between, between + after]
        for slab in range(2):
            w, k = windows[slab], centre[slab]
            above = 0.5 * (k + w[PAD - 1 : PAD - 1 + tile])
            below = 0.5 * (k + w[PAD + 1 : PAD + 1 + tile])
            right = jnp.where(lane == nz - 1, 0.0, pltpu.roll(k, nz - 1, axis=1))
            left = jnp.where(lane == 0, 0.0, pltpu.roll(k, 1, axis=1))
            right_face = 0.5 * (k + right)
            left_face = 0.5 * (k + left)
            faces[0, slab, pl.ds(b, tile), :] = above
            faces[1, slab, pl.ds(b, tile), :] = below
            faces[2, slab, pl.ds(b, tile), :] = jnp.where(lane == nz - 1, 0.0, right_face)
            faces[3, slab, pl.ds(b, tile), :] = ends[slab] + above + below + right_face + left_face
        return carry

    def heat(windows, outer, b, size):
        centre = [w[PAD : PAD + size] for w in windows]
        between = across[1, pl.ds(b, size), :]
        images = []
        for slab in range(2):
            w, v = windows[slab], centre[slab]
            fz = faces[2, slab, pl.ds(b, size), :]
            value = between * centre[1 - slab]
            if outer[slab] is not None:
                value = value + outer[slab]
            value = value + faces[0, slab, pl.ds(b, size), :] * w[PAD - 1 : PAD - 1 + size]
            value = value + faces[1, slab, pl.ds(b, size), :] * w[PAD + 1 : PAD + 1 + size]
            value = value + fz * pltpu.roll(v, nz - 1, axis=1) + pltpu.roll(fz * v, 1, axis=1)
            images.append(value - faces[3, slab, pl.ds(b, size), :] * v)
        return centre, images

    def plain_heat(f, k, b, size):
        windows = [field[f, slab, pl.ds(b, size + 2 * PAD), :] for slab in range(2)]
        outer = (
            across[0, pl.ds(b, size), :] * lower[k, pl.ds(b, size), :],
            across[2, pl.ds(b, size), :] * upper[k, pl.ds(b, size), :],
        )
        return heat(windows, outer, b, size)

    def folded(value):
        return jnp.sum(value.reshape(-1, 8, nz), axis=0)

    def each_slab(body):
        if slabs <= 16:
            for d in range(1, slabs):
                body(d)
        else:

            def step(d, carry):
                body(d)
                return carry

            lax.fori_loop(1, slabs, step, 0)

    def sum_copy(m, d):
        return remote(
            sums.at[m, s], sums.at[m, s], sum_s.at[0], sum_r.at[m], t, lax.rem(s + d, slabs),
        )

    def sum_start(m, parts):
        for row, part in enumerate(parts):
            flat = jnp.sum(part, axis=0, keepdims=True)
            line = flat[:, 0:128]
            for at in range(128, nz, 128):
                line = line + flat[:, at : at + 128]
            sums[m, s, row : row + 1, :] = line
        each_slab(lambda d: sum_copy(m, d).start())

    def sum_wait(m):
        arrived(sums.at[m, pl.ds(0, slabs - 1)], sum_r.at[m])
        total = jnp.sum(sums[m], axis=0)
        total = jnp.sum(total, axis=1, keepdims=True)
        return [total[row : row + 1, :] for row in range(4)]

    def halo_send(f, k, c, lo, rows):
        pl.when(has_lower)(down(f, k, c, lo, rows).start)
        pl.when(has_upper)(up(f, k, c, lo, rows).start)

    quarter = half // 2
    set_up = own
    set_down = pl.multiple_of(own + quarter, 8)
    pieces_of = (
        ((quarter, quarter + PAD), (0, quarter + PAD)),
        ((0, quarter), (quarter + PAD, quarter)),
    )

    def img_send(m, piece):
        (lo_d, rows_d), (lo_u, rows_u) = pieces_of[piece]
        pl.when(has_lower)(down(IMG + m, H_IMG + m, piece, lo_d, rows_d).start)
        pl.when(has_upper)(up(IMG + m, H_IMG + m, piece, lo_u, rows_u).start)

    def img_wait(m, piece):
        halo_wait(H_IMG + m, piece, *pieces_of[piece][0], (0,))
        halo_wait(H_IMG + m, piece, *pieces_of[piece][1], (1,))

    nothing = jnp.zeros((8, nz), f32)

    def product(m):
        def body(b, carry):
            centre, images = plain_heat(RES + m, H_RES + m, b, tile)
            row = lax.broadcasted_iota(jnp.int32, (tile, nz), 0) + b
            inside = jnp.logical_and(row >= own, row < own + half)
            norm, along = carry
            for slab in range(2):
                v = centre[slab]
                w = -WIDTHS[m] * images[slab]
                field[IMG + m, slab, pl.ds(PAD + b, tile), :] = w
                masked = jnp.where(inside, v, 0.0)
                norm = norm + folded(masked * v)
                along = along + folded(masked * w)
            return norm, along

        sums_here = loop(win, tile, body, (nothing, nothing))
        img_send(m, 0)
        return sums_here

    small = tile_of(quarter, 32)

    def local(m):
        def body(b, carry):
            windows = [field[IMG + m, slab, pl.ds(b, small + 2 * PAD), :] for slab in range(2)]
            centre, images = heat(windows, (None, None), b, small)
            norm, along = carry
            for slab in range(2):
                v = centre[slab]
                norm = norm + folded(v * v)
                along = along + folded(v * images[slab])
            return norm, along

        return loop(half, small, body, (nothing, nothing), own)

    def cross(m, sums_here, sums_local):
        img_wait(m, 0)

        def body_of(side):
            ref = lower if side == 0 else upper

            def body(b, carry):
                rows = pl.ds(b, small)
                edge = across[2 * side, rows, :] * ref[H_IMG + m, rows, :]
                return carry + folded(edge * field[IMG + m, side, pl.ds(PAD + b, small), :])

            return body

        outer = loop(quarter, small, body_of(0), nothing, set_up)
        outer = loop(quarter, small, body_of(1), outer, set_down)
        norm, along = sums_local
        sum_start(m, sums_here + (norm, -WIDTHS[m] * (along + 2.0 * outer)))

    def factors(m):
        rr, rw, ww, wbw = sum_wait(m)
        step_size = rr / (rr + rw)
        mean = rw / rr
        square = step_size * step_size
        norm_next = square * jnp.maximum(ww - mean * rw, 0.0)
        along = square * jnp.maximum(mean * mean * rw - 2.0 * mean * ww + wbw, 0.0)
        momentum = norm_next / rr
        below = norm_next * (1.0 + momentum)
        curve = jnp.maximum(norm_next + along - momentum * norm_next / step_size, below)
        step_next = norm_next / jnp.maximum(curve, 1e-37)
        on_image = step_size * step_next
        return step_size + step_next * (1.0 + momentum) - on_image, on_image

    def advance(m, scalars):
        on_res, on_img = scalars

        def body(b, carry):
            at = pl.ds(PAD + b, tile)
            rows = pl.ds(b, tile)
            for slab in range(2):
                field[RES + m + 1, slab, at, :] = (
                    field[GAIN + m, slab, at, :]
                    + on_res * field[RES + m, slab, at, :]
                    - on_img * field[IMG + m, slab, at, :]
                )
            for ref in (lower, upper):
                ref[H_RES + m + 1, rows, :] = (
                    ref[H_GAIN + m, rows, :]
                    + on_res * ref[H_RES + m, rows, :]
                    - on_img * ref[H_IMG + m, rows, :]
                )
            return carry

        loop(win, tile, body)

    def coarse_residual():
        def body(b, carry):
            at = pl.ds(PAD + b, tile)
            for slab in range(2):
                field[RES + 3, slab, at, :] = (
                    field[RES, slab, at, :] + field[GAIN, slab, at, :] + field[GAIN + 1, slab, at, :]
                )
            return carry

        loop(win, tile, body)

    def coarse_halo():
        def body(b, carry):
            rows = pl.ds(b, tile)
            for ref in (lower, upper):
                ref[H_RES + 3, rows, :] = (
                    ref[H_RES, rows, :] + ref[H_GAIN, rows, :] + ref[H_GAIN + 1, rows, :]
                )
            return carry

        loop(win, tile, body)

    mailed = (GAIN, GAIN + 1, IMG + 1, IMG + 2)

    def mail_copy(k):
        return remote(
            field.at[mailed[k], other, pl.ds(PAD + own, half)], mail.at[k],
            mail_s.at[k], mail_r.at[k], t, partner,
        )

    def mail_send(k):
        mail_copy(k).start()
        later(mail.at[k], mail_s.at[k])

    def coarse_send(k, which=(0, 1)):
        for slab, space in [((h, s), (other, partner))[w] for w in which]:
            copy = remote(
                field.at[(RES + 3, IMG + 3)[k - 1], slab, pl.ds(PAD + own, half)],
                kept.at[k, pl.ds(mine, half)], kept_s.at[k], kept_r.at[k], t + 1, space,
            )
            pl.when(has_next)(copy.start)

    def kept_copy(k):
        if k == 0:
            src, dst = nodes_in.at[0, 2, 0], kept.at[0]
        else:
            src, dst = marks.at[0], marks.at[1]
        return remote(src, dst, kept_s.at[k], kept_r.at[k], t + 1, s)

    def finish(m, scalars, slab, ref, lo, rows):
        on_res, on_img = scalars
        node = NODE + min(m, 2)

        def body(b, carry):
            at = pl.ds(PAD + own + b, small)
            ref[pl.ds(b, small), :] = (
                field[node, slab, at, :]
                + on_res * field[RES + m, slab, at, :]
                - on_img * field[IMG + m, slab, at, :]
            )
            return carry

        loop(rows, small, body, 0, lo)

    def residuals(b, carry):
        images = [plain_heat(NODE + j, H_NODE + j, b, tile)[1] for j in range(3)]
        at = pl.ds(PAD + b, tile)
        for slab in range(2):
            nodes = [field[NODE + j, slab, at, :] for j in range(3)]
            for row, f in enumerate((RES, GAIN, GAIN + 1)):
                value = nodes[row - 1] - nodes[row] if row else -nodes[0]
                for j in range(3):
                    value = value + (STEP * sweep_weight(row, j)) * images[j][slab]
                field[f, slab, at, :] = value
        return carry

    spans = []
    for c, (lo, rows) in enumerate(bounds):
        begin = lo - tile if c else 0
        end = lo + rows - (tile if c < chunks - 1 else 0)
        spans.append((begin, end - begin))

    def begin_rows(c):
        halo_wait(H_NODE, c, *bounds[c], fields=3)
        lo, rows = spans[c]
        loop(rows, tile, coefficients, 0, lo)
        loop(rows, tile, residuals, 0, lo)

    def add_start(b, carry):
        at = pl.ds(PAD + b, tile)
        for slab in range(2):
            field[RES, slab, at, :] = field[RES, slab, at, :] + field[START, slab, at, :]
        return carry

    def begin_res(c):
        swap_wait(4, c)
        lo, rows = spans[c]
        loop(rows, tile, add_start, 0, lo)
        halo_send(RES, H_RES, c, lo, rows)

    def pass_kappa(q):
        swap_wait(0, q)
        if share:
            kin_copy(0, *parts[q]).start()
        first_hop(0, q, other)

    each_part(pass_kappa)
    for c in range(chunks):
        for k in range(1, 4):
            swap_wait(k, c)
            first_hop(k, c, other)
        if c == 0:
            each_half(lambda lo, rows: halo_wait(H_KAPPA, 0, lo, rows))
            pl.when(has_lower)(lambda: kin_start(1))
            pl.when(has_upper)(lambda: kin_start(2))
        if c == min(1, chunks - 1):
            kin_wait(0)
            pl.when(has_lower)(lambda: kin_wait(1))
            pl.when(has_upper)(lambda: kin_wait(2))
        if c > 0:
            begin_rows(c - 1)
    for c in range(chunks):
        if c == chunks - 1:
            begin_rows(c)
        begin_res(c)
    mail_send(0)
    mail_send(1)
    theirs = pl.multiple_of(other * half, 8)
    beside = pl.multiple_of(PAD * other, 8)

    def half_of(m, at):
        return fine_out.at[0, m, 0, pl.ds(at, half)]

    def finish_start(update):
        finish(0, update, other, result, 0, half)
        remote(result, half_of(0, mine), out_s.at[0], out_r.at[0], t, partner).start()
        later(result, out_s.at[0])
        finish(0, update, h, half_of(0, mine), 0, half)

    def finish_second(update):
        finish(1, update, h, half_of(1, mine), 0, half)
        arrived(half_of(0, theirs), out_r.at[0])
        for k in range(3):
            mail_copy(k).wait_recv()

        def body(b, carry):
            rows, at = pl.ds(b, small), pl.ds(beside + b, small)
            there = pl.ds(theirs + b, small)
            residual = fine_out[0, 0, 0, there, :] - outgoing[1, at, :] + mail[0, rows, :]
            step = update[0] * residual - update[1] * mail[2, rows, :]
            fine_out[0, 1, 0, there, :] = outgoing[2, at, :] + step
            mail[1, rows, :] = mail[1, rows, :] + step
            return carry

        loop(half, small, body)

    def finish_third(update, lo, rows):
        def body(b, carry):
            at = pl.ds(b, small)
            fine_out[0, 2, 0, pl.ds(theirs + b, small), :] = (
                outgoing[3, pl.ds(beside + b, small), :]
                + update[0] * mail[1, at, :]
                - update[1] * mail[3, at, :]
            )
            return carry

        loop(rows, small, body, 0, lo)

    def finish_coarse():
        on_res, on_img = marks[1, 0:1, 0:1], marks[1, 1:2, 0:1]

        def body(b, carry):
            at = pl.ds(b, small)
            coarse_out[0, 0, at, :] = (
                kept[0, at, :] + on_res * kept[1, at, :] - on_img * kept[2, at, :]
            )
            return carry

        loop(ny, small, body)

    pl.when(has_next)(kept_copy(0).start)

    @pl.when(jnp.logical_not(has_prev))
    def _():
        pltpu.make_async_copy(start_in.at[0, 0], start_out.at[0, 0], copy_s.at[0]).start()
        pltpu.make_async_copy(start_in.at[0, 0], coarse_out.at[0, 0], copy_s.at[1]).start()

    def gain_send(m, chunk_range):
        for c in chunk_range:
            if c < chunks:
                halo_send(GAIN + m, H_GAIN + m, c, *spans[c])

    def gain_wait(m):
        halo_wait(H_GAIN + m, 0, 0, win)

    gain_send(0, range(0, 2))
    halo_wait(H_RES, 0, 0, win)
    here = product(0)
    gain_send(0, range(2, 4))
    cross(0, here, local(0))
    gain_send(0, range(4, chunks))
    img_send(0, 1)
    gain_send(1, range(0, 2))
    coarse_residual()
    coarse_send(1)
    update = factors(0)
    gain_wait(0)
    img_wait(0, 1)
    advance(0, update)
    here = product(1)
    mail_send(2)
    gain_send(1, range(2, 4))
    cross(1, here, local(1))
    finish_start(update)
    gain_send(1, range(4, chunks))
    img_send(1, 1)
    gain_wait(1)
    coarse_halo()
    here_coarse = product(3)
    coarse_send(2, (0,))
    update = factors(1)
    img_wait(1, 1)
    advance(1, update)
    here = product(2)
    mail_send(3)
    cross(3, here_coarse, local(3))
    cross(2, here, local(2))
    coarse_send(2, (1,))
    finish_second(update)

    pieces = 2 if half % (2 * small) == 0 else 1
    piece = half // pieces

    def pass_on(at):
        copy = remote(
            fine_out.at[0, 2, 0, pl.ds(at, piece)], start_out.at[0, 0, pl.ds(at, piece)],
            end_s.at[0], end_r.at[0], t + 1, s,
        )
        pl.when(has_next)(copy.start)

    update = factors(3)
    for row in range(2):
        marks[0, row : row + 1, :] = jnp.broadcast_to(update[row], (1, 128))
    pl.when(has_next)(kept_copy(3).start)

    mail_copy(3).wait_recv()
    update = factors(2)
    for c in range(pieces):
        finish(2, update, h, half_of(2, mine), c * piece, piece)
        pass_on(mine + c * piece)
    for c in range(pieces):
        finish_third(update, c * piece, piece)
        pass_on(theirs + c * piece)

    @pl.when(jnp.logical_not(has_prev))
    def _():
        pltpu.make_async_copy(start_in.at[0, 0], start_out.at[0, 0], copy_s.at[0]).wait()
        pltpu.make_async_copy(start_in.at[0, 0], coarse_out.at[0, 0], copy_s.at[1]).wait()

    @pl.when(has_prev)
    def _():
        for k in range(3):
            arrived(kept.at[k], kept_r.at[k])
        arrived(marks.at[1], kept_r.at[3])
        finish_coarse()
        arrived(start_out.at[0, 0], end_r.at[0])

    each_half(lambda lo, rows: sent(outgoing.at[0, pl.ds(lo, rows)], swap_s.at[0]))
    for side, cond in ((0, has_lower), (1, has_upper)):

        @pl.when(cond)
        def _(side=side):
            each_half(
                lambda lo, rows: sent(
                    field.at[KAPPA, side, pl.ds(PAD + lo, rows)], halo_s.at[side, 0]
                )
            )

    kin_sent(0)
    pl.when(has_lower)(lambda: kin_sent(1))
    pl.when(has_upper)(lambda: kin_sent(2))
    halo_later(NODE, 1, 0, win, 3)
    halo_later(RES, 2, 0, win)
    halo_later(GAIN, 3, 0, win, 2)
    halo_later(IMG, 4, 0, win, 2)
    for side in range(2):
        halo_later(IMG + 2, 5, *pieces_of[0][side], 2, (side,))
    for k in range(3):
        later(kept.at[k], kept_s.at[k], has_next)
    later(marks.at[0], kept_s.at[3], has_next)
    later(fine_out.at[0, 2, 0], end_s.at[0], has_next)
    later(sums.at[pl.ds(0, 4), pl.ds(0, slabs - 1)], sum_s.at[0])
    for ref, sem, cond in pending:
        if cond is None:
            sent(ref, sem)
        else:
            pl.when(cond)(lambda ref=ref, sem=sem: sent(ref, sem))


def store(fine, begin, coarse, fine_out, start_out, coarse_out, sem):
    pairs = [(begin.at[0, 0], start_out.at[0, 0]), (coarse.at[0, 0], coarse_out.at[0, 0])]
    pairs += [(fine.at[0, m, 0], fine_out.at[0, m, 0]) for m in range(fine.shape[1])]
    copies = []
    for k, (src, dst) in enumerate(pairs):
        rows = src.shape[0] // 2
        for j in range(2):
            at = pl.ds(j * rows, rows)
            copies.append(pltpu.make_async_copy(src.at[at], dst.at[at], sem.at[2 * k + j]))
    for copy in copies:
        copy.start()
    for copy in copies:
        copy.wait()


def solution(mesh):
    slices, slabs = mesh.shape["tm"], mesh.shape["space"]

    def on_device(start_value, old_nodes, diffusivity):
        ny, nz = start_value.shape[2:]
        half = ny // 2
        win = half + PAD
        chunks = len(chunk_bounds(win, tile_of(win, 24)))
        vmem = lambda *shape: pltpu.VMEM(shape, jnp.float32)
        dma = lambda *shape: pltpu.SemaphoreType.DMA(shape)

        def body(*refs):
            kernel(slices, slabs, ny, nz, *refs)

        nodes, ends = pltpu.VMEM(old_nodes.shape, jnp.float32), pltpu.VMEM(start_value.shape, jnp.float32)
        results = pl.pallas_call(
            body,
            out_shape=(nodes, ends, ends),
            in_specs=[pl.BlockSpec(memory_space=pltpu.HBM)] * 3,
            out_specs=(pl.BlockSpec(memory_space=pltpu.VMEM),) * 3,
            scratch_shapes=[
                vmem(FIELDS, 2, win + 2 * PAD, nz),
                vmem(HALOS, win, nz),
                vmem(HALOS, win, nz),
                vmem(4, 2, win, nz),
                vmem(3, win, nz),
                vmem(5, win, nz),
                vmem(half, nz),
                vmem(4, half, nz),
                vmem(3, ny, nz),
                vmem(2, 8, 128),
                vmem(4, slabs, 4, 128),
                dma(2), dma(4 + 4 * chunks), dma(2), dma(3), dma(3), dma(4), dma(4), dma(4), dma(4),
                dma(2, 6), dma(2, 10 + chunks), dma(1), dma(4),
                dma(1), dma(1), dma(1), dma(1), dma(2),
            ],
            compiler_params=pltpu.CompilerParams(
                collective_id=0, has_side_effects=True, vmem_limit_bytes=61 * 1024 * 1024
            ),
            name="pfasst",
        )(start_value, old_nodes, diffusivity)
        return pl.pallas_call(
            store,
            out_shape=tuple(jax.ShapeDtypeStruct(r.shape, jnp.float32) for r in results),
            in_specs=[pl.BlockSpec(memory_space=pltpu.VMEM)] * 3,
            out_specs=(pl.BlockSpec(memory_space=pltpu.HBM),) * 3,
            scratch_shapes=[dma(4 + 2 * old_nodes.shape[1])],
            compiler_params=pltpu.CompilerParams(vmem_limit_bytes=1024 * 1024),
            name="store",
        )(*results)

    in_specs = (
        P("tm", "space", None, None),
        P("tm", None, "space", None, None),
        P("space", None, None),
    )
    out_specs = (
        P("tm", None, "space", None, None),
        P("tm", "space", None, None),
        P("tm", "space", None, None),
    )
    return jax.shard_map(
        on_device, mesh=mesh, in_specs=in_specs, out_specs=out_specs, check_vma=False
    )
```

```python
import math

import jax
import jax.numpy as jnp
from jax import lax
from jax.experimental import pallas as pl
from jax.experimental.pallas import tpu as pltpu
from jax.sharding import PartitionSpec as P

STEP = 2.0
ROOT_SIX = math.sqrt(6.0)
NODE_TIMES = [(4.0 - ROOT_SIX) / 10.0, (4.0 + ROOT_SIX) / 10.0, 1.0]
COLLOC = [
    [
        (88.0 - 7.0 * ROOT_SIX) / 360.0,
        (296.0 - 169.0 * ROOT_SIX) / 1800.0,
        (-2.0 + 3.0 * ROOT_SIX) / 225.0,
    ],
    [
        (296.0 + 169.0 * ROOT_SIX) / 1800.0,
        (88.0 + 7.0 * ROOT_SIX) / 360.0,
        (-2.0 - 3.0 * ROOT_SIX) / 225.0,
    ],
    [(16.0 - ROOT_SIX) / 36.0, (16.0 + ROOT_SIX) / 36.0, 1.0 / 9.0],
]
MESH = pl.DeviceIdType.MESH
PAD = 8
UNROLL = 16
SHARES = (1, 1)

KAPPA, NODE, START, RES, IMG, GAIN = 0, 1, 4, 5, 9, 13
FIELDS = 15
H_KAPPA, H_NODE, H_RES, H_IMG, H_GAIN = 0, 1, 4, 8, 12
HALOS = 14


def sweep_weight(row, column):
    below = COLLOC[row - 1][column] if row > 0 else 0.0
    return COLLOC[row][column] - below


def node_width(row):
    below = NODE_TIMES[row - 1] if row > 0 else 0.0
    return NODE_TIMES[row] - below


WIDTHS = [STEP * node_width(0), STEP * node_width(1), STEP * node_width(2), STEP]


def chunk_bounds(rows, tile):
    tiles = rows // tile
    parts = min(5, tiles)
    counts = [tiles // parts + (c < tiles % parts) for c in range(parts)]
    if counts[-1] > 1:
        counts[-1] -= 1
        counts[1 if parts > 2 else 0] += 1
    cuts = [tile * sum(counts[:c]) for c in range(parts + 1)]
    return [(cuts[c], cuts[c + 1] - cuts[c]) for c in range(parts)]


def tile_of(rows, most):
    best = 8
    for size in range(8, most + 1, 8):
        if rows % size == 0:
            best = size
    return best


def kernel(
    slices, slabs, ny, nz,
    start_in, nodes_in, kappa_in,
    fine_out, start_out, coarse_out,
    field, lower, upper, faces, across, outgoing, result, mail, kept, ahead, marks, sums,
    swap_s, swap_r, own_s, kin_s, kin_r, mail_s, mail_r, kept_s, kept_r, halo_s, halo_r, sum_s, sum_r, out_s, out_r, end_s, end_r, copy_s,
):
    f32 = jnp.float32
    t = lax.axis_index("tm")
    s = lax.axis_index("space")
    h = lax.rem(s, 2)
    p = lax.div(s, 2)
    pairs = slabs // 2
    half = ny // 2
    win = half + PAD
    other = 1 - h
    partner = s + 1 - 2 * h
    team = next(n for n in (4, 2, 1) if slices % n == 0)
    rank = lax.rem(t, team)
    early = lax.rem(t, 2) == 1
    first_row = pl.multiple_of(h * (half - PAD), 8)
    partner_row = pl.multiple_of(other * (half - PAD), 8)
    own = pl.multiple_of(PAD * h, 8)
    mine = pl.multiple_of(h * half, 8)
    has_next = t < slices - 1
    has_prev = t > 0
    has_lower = p > 0
    has_upper = p < pairs - 1
    pending = []

    def later(ref, sem, cond=None):
        pending.append((ref, sem, cond))

    def remote(src, dst, send, recv, tm, space):
        return pltpu.make_async_remote_copy(
            src_ref=src, dst_ref=dst, send_sem=send, recv_sem=recv,
            device_id=(tm, space), device_id_type=MESH,
        )

    barrier = pltpu.get_barrier_semaphore()

    def greet(d, carry):
        pl.semaphore_signal(
            barrier, inc=1, device_id=(t, lax.rem(s + d, slabs)), device_id_type=MESH
        )
        return carry

    lax.fori_loop(1, slabs, greet, 0)
    for cond, tm in ((has_next, t + 1), (has_prev, t - 1)):

        @pl.when(cond)
        def _(tm=tm):
            for space in (s, partner):
                pl.semaphore_signal(barrier, inc=1, device_id=(tm, space), device_id_type=MESH)

    far = [jnp.abs(rank - q) > 1 for q in range(team)]
    for q in range(team):

        @pl.when(far[q])
        def _(q=q):
            pl.semaphore_signal(
                barrier, inc=1, device_id=(t - rank + q, s), device_id_type=MESH
            )

    sources = [kappa_in.at[0]] + [nodes_in.at[0, j, 0] for j in range(3)] + [start_in.at[0, 0]]
    for k, source in enumerate(sources):
        pltpu.make_async_copy(
            source.at[pl.ds(first_row, win)], field.at[k, h, pl.ds(PAD, win)], own_s.at[0]
        ).start()
        pltpu.make_async_copy(
            source.at[pl.ds(partner_row, win)], outgoing.at[k], own_s.at[1]
        ).start()

    zeros = jnp.zeros((PAD, nz), f32)
    for k in range(FIELDS):
        for slab in range(2):
            field[k, slab, 0:PAD, :] = zeros
            field[k, slab, win + PAD : win + 2 * PAD, :] = zeros

    def clear(ref):
        def body(i, carry):
            for k in range(HALOS):
                ref[k, pl.ds(pl.multiple_of(i * 8, 8), 8), :] = zeros
            return carry

        lax.fori_loop(0, win // 8, body, 0)

    @pl.when(jnp.logical_not(has_lower))
    def _():
        clear(lower)

    @pl.when(jnp.logical_not(has_upper))
    def _():
        clear(upper)

    pl.semaphore_wait(
        barrier,
        slabs - 1 + 2 * has_next.astype(jnp.int32) + 2 * has_prev.astype(jnp.int32)
        + sum(f.astype(jnp.int32) for f in far),
    )

    tile = tile_of(win, 24)
    bounds = chunk_bounds(win, tile)
    chunks = len(bounds)

    weights = [SHARES[q % 2] for q in range(team)]
    cuts = [8 * (win // 8 * sum(weights[:q]) // sum(weights)) for q in range(team)] + [win]
    parts = [(cuts[q], cuts[q + 1] - cuts[q]) for q in range(team)]

    def bounds_of(k, c):
        return bounds[c] if k else parts[c]

    def each_part(body):
        for q in range(team):
            if parts[q][1]:
                pl.when(rank == q)(lambda q=q: body(q))

    def arrived(ref, sem):
        remote(ref, ref, sum_s.at[0], sem, t, partner).wait_recv()

    def sent(ref, sem):
        remote(ref, ref, sem, sum_r.at[0], t, partner).wait_send()

    def swap_sem(k, c):
        return swap_r.at[4 + (k - 1) * chunks + c if k else c]

    def swap_start(k, c):
        lo, rows = bounds_of(k, c)
        remote(
            outgoing.at[k, pl.ds(lo, rows)], field.at[k, h, pl.ds(PAD + lo, rows)],
            swap_s.at[min(k, 1)], swap_sem(k, c), t, partner,
        ).start()

    def swap_wait(k, c):
        lo, rows = bounds_of(k, c)
        arrived(field.at[k, other, pl.ds(PAD + lo, rows)], swap_sem(k, c))

    def kin_ref(e, lo, rows):
        if e == 0:
            return field.at[KAPPA, other, pl.ds(PAD + lo, rows)]
        return (lower, upper)[e - 1].at[H_KAPPA, pl.ds(lo, rows)]

    def kin_start(e, q):
        ref = kin_ref(e, *parts[q])
        for peer in range(team):
            if peer != q:
                remote(ref, ref, kin_s.at[e], kin_r.at[e], t - q + peer, s).start()

    def kin_wait(e):
        for q in range(team):
            rows = win - parts[q][1]
            if rows:
                pl.when(rank == q)(lambda rows=rows: arrived(kin_ref(e, 0, rows), kin_r.at[e]))

    def kin_sent(e):
        if team > 1:
            each_part(
                lambda q: sent(field.at[pl.ds(0, team - 1), 0, pl.ds(0, parts[q][1])], kin_s.at[e])
            )

    pltpu.make_async_copy(outgoing, outgoing, own_s.at[1]).wait()
    each_part(lambda q: swap_start(0, q))
    for c in range(chunks):
        for k in range(1, 4):
            swap_start(k, c)
    for c in range(chunks):
        swap_start(4, c)
    later(outgoing.at[pl.ds(1, 4)], swap_s.at[1])

    def halo_sems(k, c, side):
        if k == H_KAPPA:
            slots = 0, 0
        elif k < H_RES:
            slots = 1, 1 + c
        elif k == H_RES:
            slots = 2, 1 + chunks
        elif k >= H_GAIN:
            slots = 3, 2 + chunks + k - H_GAIN
        else:
            m = k - H_IMG
            slots = 4 + m // 2, 4 + chunks + (2 * m + c if m < 2 else 2 + m)
        return halo_s.at[side, slots[0]], halo_r.at[side, slots[1]]

    def down(f, k, c, lo, rows):
        return remote(
            field.at[f, 0, pl.ds(PAD + lo, rows)], upper.at[k, pl.ds(lo, rows)],
            *halo_sems(k, c, 0), t, s - 2,
        )

    def up(f, k, c, lo, rows):
        return remote(
            field.at[f, 1, pl.ds(PAD + lo, rows)], lower.at[k, pl.ds(lo, rows)],
            *halo_sems(k, c, 1), t, s + 2,
        )

    def first_hop(k, c, which):
        @pl.when(jnp.logical_and(which == 0, has_lower))
        def _():
            down(k, k, c, *bounds_of(k, c)).start()

        @pl.when(jnp.logical_and(which == 1, has_upper))
        def _():
            up(k, k, c, *bounds_of(k, c)).start()

    own_rows = field.at[pl.ds(0, 5), h, pl.ds(PAD, win)]
    pltpu.make_async_copy(own_rows, own_rows, own_s.at[0]).wait()
    each_part(lambda q: first_hop(0, q, h))
    for c in range(chunks):
        for k in range(1, 4):
            first_hop(k, c, h)

    def halo_wait(k, c, lo, rows, sides=(0, 1), fields=None):
        which = k if fields is None else pl.ds(k, fields)
        for side, ref, cond in ((0, upper, has_upper), (1, lower, has_lower)):
            if side in sides:

                @pl.when(cond)
                def _(side=side, ref=ref):
                    arrived(ref.at[which, pl.ds(lo, rows)], halo_sems(k, c, side)[1])

    def halo_later(f, slot, lo, rows, fields=None, sides=(0, 1)):
        which = f if fields is None else pl.ds(f, fields)
        for side in sides:
            ref = field.at[which, side, pl.ds(PAD + lo, rows)]
            later(ref, halo_s.at[side, slot], (has_lower, has_upper)[side])

    lane = lax.broadcasted_iota(jnp.int32, (tile, nz), 1)

    def loop(rows, size, body, init=0, offset=0):
        def step(i, carry):
            return body(pl.multiple_of(offset + i * size, 8), carry)

        count = rows // size
        return lax.fori_loop(0, count, step, init, unroll=max(u for u in range(1, UNROLL + 1) if count % u == 0))

    def coefficients(b, carry):
        windows = [field[KAPPA, slab, pl.ds(b, tile + 2 * PAD), :] for slab in range(2)]
        centre = [w[PAD : PAD + tile] for w in windows]
        before = 0.5 * (centre[0] + lower[H_KAPPA, pl.ds(b, tile), :])
        between = 0.5 * (centre[0] + centre[1])
        after = 0.5 * (centre[1] + upper[H_KAPPA, pl.ds(b, tile), :])
        across[0, pl.ds(b, tile), :] = before
        across[1, pl.ds(b, tile), :] = between
        across[2, pl.ds(b, tile), :] = after
        ends = [before + between, between + after]
        for slab in range(2):
            w, k = windows[slab], centre[slab]
            above = 0.5 * (k + w[PAD - 1 : PAD - 1 + tile])
            below = 0.5 * (k + w[PAD + 1 : PAD + 1 + tile])
            right = jnp.where(lane == nz - 1, 0.0, pltpu.roll(k, nz - 1, axis=1))
            left = jnp.where(lane == 0, 0.0, pltpu.roll(k, 1, axis=1))
            right_face = 0.5 * (k + right)
            left_face = 0.5 * (k + left)
            faces[0, slab, pl.ds(b, tile), :] = above
            faces[1, slab, pl.ds(b, tile), :] = below
            faces[2, slab, pl.ds(b, tile), :] = jnp.where(lane == nz - 1, 0.0, right_face)
            faces[3, slab, pl.ds(b, tile), :] = ends[slab] + above + below + right_face + left_face
        return carry

    def heat(windows, outer, b, size):
        centre = [w[PAD : PAD + size] for w in windows]
        between = across[1, pl.ds(b, size), :]
        images = []
        for slab in range(2):
            w, v = windows[slab], centre[slab]
            fz = faces[2, slab, pl.ds(b, size), :]
            value = between * centre[1 - slab]
            if outer[slab] is not None:
                value = value + outer[slab]
            value = value + faces[0, slab, pl.ds(b, size), :] * w[PAD - 1 : PAD - 1 + size]
            value = value + faces[1, slab, pl.ds(b, size), :] * w[PAD + 1 : PAD + 1 + size]
            value = value + fz * pltpu.roll(v, nz - 1, axis=1) + pltpu.roll(fz * v, 1, axis=1)
            images.append(value - faces[3, slab, pl.ds(b, size), :] * v)
        return centre, images

    def plain_heat(f, k, b, size):
        windows = [field[f, slab, pl.ds(b, size + 2 * PAD), :] for slab in range(2)]
        outer = (
            across[0, pl.ds(b, size), :] * lower[k, pl.ds(b, size), :],
            across[2, pl.ds(b, size), :] * upper[k, pl.ds(b, size), :],
        )
        return heat(windows, outer, b, size)

    def folded(value):
        return jnp.sum(value.reshape(-1, 8, nz), axis=0)

    def each_slab(body):
        if slabs <= 16:
            for d in range(1, slabs):
                body(d)
        else:

            def step(d, carry):
                body(d)
                return carry

            lax.fori_loop(1, slabs, step, 0)

    def sum_copy(m, d):
        return remote(
            sums.at[m, s], sums.at[m, s], sum_s.at[0], sum_r.at[m], t, lax.rem(s + d, slabs),
        )

    def sum_start(m, parts):
        for row, part in enumerate(parts):
            flat = jnp.sum(part, axis=0, keepdims=True)
            line = flat[:, 0:128]
            for at in range(128, nz, 128):
                line = line + flat[:, at : at + 128]
            sums[m, s, row : row + 1, :] = line
        each_slab(lambda d: sum_copy(m, d).start())

    def sum_wait(m):
        arrived(sums.at[m, pl.ds(0, slabs - 1)], sum_r.at[m])
        total = jnp.sum(sums[m], axis=0)
        total = jnp.sum(total, axis=1, keepdims=True)
        return [total[row : row + 1, :] for row in range(4)]

    def halo_send(f, k, c, lo, rows):
        pl.when(has_lower)(down(f, k, c, lo, rows).start)
        pl.when(has_upper)(up(f, k, c, lo, rows).start)

    quarter = half // 2
    set_up = own
    set_down = pl.multiple_of(own + quarter, 8)
    pieces_of = (
        ((quarter, quarter + PAD), (0, quarter + PAD)),
        ((0, quarter), (quarter + PAD, quarter)),
    )

    def img_send(m, piece):
        (lo_d, rows_d), (lo_u, rows_u) = pieces_of[piece]
        pl.when(has_lower)(down(IMG + m, H_IMG + m, piece, lo_d, rows_d).start)
        pl.when(has_upper)(up(IMG + m, H_IMG + m, piece, lo_u, rows_u).start)

    def img_wait(m, piece):
        halo_wait(H_IMG + m, piece, *pieces_of[piece][0], (0,))
        halo_wait(H_IMG + m, piece, *pieces_of[piece][1], (1,))

    nothing = jnp.zeros((8, nz), f32)

    def product(m):
        def body(b, carry):
            centre, images = plain_heat(RES + m, H_RES + m, b, tile)
            row = lax.broadcasted_iota(jnp.int32, (tile, nz), 0) + b
            inside = jnp.logical_and(row >= own, row < own + half)
            norm, along = carry
            for slab in range(2):
                v = centre[slab]
                w = -WIDTHS[m] * images[slab]
                field[IMG + m, slab, pl.ds(PAD + b, tile), :] = w
                masked = jnp.where(inside, v, 0.0)
                norm = norm + folded(masked * v)
                along = along + folded(masked * w)
            return norm, along

        sums_here = loop(win, tile, body, (nothing, nothing))
        img_send(m, 0)
        return sums_here

    small = tile_of(quarter, 32)

    def local(m):
        def body(b, carry):
            windows = [field[IMG + m, slab, pl.ds(b, small + 2 * PAD), :] for slab in range(2)]
            centre, images = heat(windows, (None, None), b, small)
            norm, along = carry
            for slab in range(2):
                v = centre[slab]
                norm = norm + folded(v * v)
                along = along + folded(v * images[slab])
            return norm, along

        return loop(half, small, body, (nothing, nothing), own)

    def cross(m, sums_here, sums_local):
        img_wait(m, 0)

        def body_of(side):
            ref = lower if side == 0 else upper

            def body(b, carry):
                rows = pl.ds(b, small)
                edge = across[2 * side, rows, :] * ref[H_IMG + m, rows, :]
                return carry + folded(edge * field[IMG + m, side, pl.ds(PAD + b, small), :])

            return body

        outer = loop(quarter, small, body_of(0), nothing, set_up)
        outer = loop(quarter, small, body_of(1), outer, set_down)
        norm, along = sums_local
        sum_start(m, sums_here + (norm, -WIDTHS[m] * (along + 2.0 * outer)))

    def factors(m):
        rr, rw, ww, wbw = sum_wait(m)
        step_size = rr / (rr + rw)
        mean = rw / rr
        square = step_size * step_size
        norm_next = square * jnp.maximum(ww - mean * rw, 0.0)
        along = square * jnp.maximum(mean * mean * rw - 2.0 * mean * ww + wbw, 0.0)
        momentum = norm_next / rr
        below = norm_next * (1.0 + momentum)
        curve = jnp.maximum(norm_next + along - momentum * norm_next / step_size, below)
        step_next = norm_next / jnp.maximum(curve, 1e-37)
        on_image = step_size * step_next
        return step_size + step_next * (1.0 + momentum) - on_image, on_image

    def advance(m, scalars):
        on_res, on_img = scalars

        def body(b, carry):
            at = pl.ds(PAD + b, tile)
            rows = pl.ds(b, tile)
            for slab in range(2):
                field[RES + m + 1, slab, at, :] = (
                    field[GAIN + m, slab, at, :]
                    + on_res * field[RES + m, slab, at, :]
                    - on_img * field[IMG + m, slab, at, :]
                )
            for ref in (lower, upper):
                ref[H_RES + m + 1, rows, :] = (
                    ref[H_GAIN + m, rows, :]
                    + on_res * ref[H_RES + m, rows, :]
                    - on_img * ref[H_IMG + m, rows, :]
                )
            return carry

        loop(win, tile, body)

    def coarse_residual():
        def body(b, carry):
            at = pl.ds(PAD + b, tile)
            for slab in range(2):
                field[RES + 3, slab, at, :] = (
                    field[RES, slab, at, :] + field[GAIN, slab, at, :] + field[GAIN + 1, slab, at, :]
                )
            return carry

        loop(win, tile, body)

    def coarse_halo():
        def body(b, carry):
            rows = pl.ds(b, tile)
            for ref in (lower, upper):
                ref[H_RES + 3, rows, :] = (
                    ref[H_RES, rows, :] + ref[H_GAIN, rows, :] + ref[H_GAIN + 1, rows, :]
                )
            return carry

        loop(win, tile, body)

    mailed = (GAIN, GAIN + 1, IMG + 1, IMG + 2, RES + 3)

    def mail_copy(k):
        return remote(
            field.at[mailed[k], other, pl.ds(PAD + own, half)], mail.at[k],
            mail_s.at[k], mail_r.at[k], t, partner,
        )

    def mail_send(k):
        mail_copy(k).start()
        later(mail.at[k], mail_s.at[k])

    def coarse_send(k, which=(0, 1), cond=True):
        for slab, space in [((h, s), (other, partner))[w] for w in which]:
            copy = remote(
                field.at[(RES + 3, IMG + 3)[k - 1], slab, pl.ds(PAD + own, half)],
                kept.at[k, pl.ds(mine, half)], kept_s.at[k], kept_r.at[k], t + 1, space,
            )
            pl.when(jnp.logical_and(has_next, cond))(copy.start)

    def kept_copy(k):
        if k == 0:
            src, dst = nodes_in.at[0, 2, 0], kept.at[0]
        else:
            src, dst = marks.at[k - 3], marks.at[k - 1]
        return remote(src, dst, kept_s.at[k], kept_r.at[k], t + 1, s)

    def marks_send(k, update):
        for row in range(2):
            marks[k - 3, row : row + 1, :] = jnp.broadcast_to(update[row], (1, 128))
        pl.when(has_next)(kept_copy(k).start)

    def marks_of(k):
        arrived(marks.at[k - 1], kept_r.at[k])
        return marks[k - 1, 0:1, 0:1], marks[k - 1, 1:2, 0:1]

    def ahead_send(e):
        copy = remote(
            field.at[(RES + 2, IMG + 2)[e], h, pl.ds(PAD + own, half)], ahead.at[e],
            kept_s.at[5], kept_r.at[5], t + 1, s,
        )
        pl.when(has_next)(copy.start)

    def finish(m, scalars, slab, ref, lo, rows):
        on_res, on_img = scalars
        node = NODE + min(m, 2)

        def body(b, carry):
            at = pl.ds(PAD + own + b, small)
            ref[pl.ds(b, small), :] = (
                field[node, slab, at, :]
                + on_res * field[RES + m, slab, at, :]
                - on_img * field[IMG + m, slab, at, :]
            )
            return carry

        loop(rows, small, body, 0, lo)

    def residuals(b, carry):
        images = [plain_heat(NODE + j, H_NODE + j, b, tile)[1] for j in range(3)]
        at = pl.ds(PAD + b, tile)
        for slab in range(2):
            nodes = [field[NODE + j, slab, at, :] for j in range(3)]
            for row, f in enumerate((RES, GAIN, GAIN + 1)):
                value = nodes[row - 1] - nodes[row] if row else -nodes[0]
                for j in range(3):
                    value = value + (STEP * sweep_weight(row, j)) * images[j][slab]
                field[f, slab, at, :] = value
        return carry

    spans = []
    for c, (lo, rows) in enumerate(bounds):
        begin = lo - tile if c else 0
        end = lo + rows - (tile if c < chunks - 1 else 0)
        spans.append((begin, end - begin))

    def begin_rows(c):
        halo_wait(H_NODE, c, *bounds[c], fields=3)
        lo, rows = spans[c]
        loop(rows, tile, coefficients, 0, lo)
        loop(rows, tile, residuals, 0, lo)

    def add_start(b, carry):
        at = pl.ds(PAD + b, tile)
        for slab in range(2):
            field[RES, slab, at, :] = field[RES, slab, at, :] + field[START, slab, at, :]
        return carry

    def begin_res(c):
        swap_wait(4, c)
        lo, rows = spans[c]
        loop(rows, tile, add_start, 0, lo)
        halo_send(RES, H_RES, c, lo, rows)

    def pass_kappa(q):
        swap_wait(0, q)
        kin_start(0, q)
        first_hop(0, q, other)

    each_part(pass_kappa)
    for c in range(chunks):
        for k in range(1, 4):
            swap_wait(k, c)
            first_hop(k, c, other)
        if c == 0:
            each_part(lambda q: halo_wait(H_KAPPA, 0, *parts[q]))
            pl.when(has_lower)(lambda: each_part(lambda q: kin_start(1, q)))
            pl.when(has_upper)(lambda: each_part(lambda q: kin_start(2, q)))
        if c == min(1, chunks - 1):
            kin_wait(0)
            pl.when(has_lower)(lambda: kin_wait(1))
            pl.when(has_upper)(lambda: kin_wait(2))
        if c > 0:
            begin_rows(c - 1)
    for c in range(chunks):
        if c == chunks - 1:
            begin_rows(c)
        begin_res(c)
    mail_send(0)
    mail_send(1)
    theirs = pl.multiple_of(other * half, 8)
    beside = pl.multiple_of(PAD * other, 8)

    def half_of(m, at):
        return fine_out.at[0, m, 0, pl.ds(at, half)]

    def finish_start(update):
        finish(0, update, other, result, 0, half)
        remote(result, half_of(0, mine), out_s.at[0], out_r.at[0], t, partner).start()
        later(result, out_s.at[0])
        finish(0, update, h, half_of(0, mine), 0, half)

    def finish_second(update):
        finish(1, update, h, half_of(1, mine), 0, half)
        arrived(half_of(0, theirs), out_r.at[0])
        for k in range(3):
            mail_copy(k).wait_recv()

        def body(b, carry):
            rows, at = pl.ds(b, small), pl.ds(beside + b, small)
            there = pl.ds(theirs + b, small)
            residual = fine_out[0, 0, 0, there, :] - outgoing[1, at, :] + mail[0, rows, :]
            step = update[0] * residual - update[1] * mail[2, rows, :]
            fine_out[0, 1, 0, there, :] = outgoing[2, at, :] + step
            mail[1, rows, :] = mail[1, rows, :] + step
            return carry

        loop(half, small, body)

    def finish_third(update, lo, rows):
        def body(b, carry):
            at = pl.ds(b, small)
            fine_out[0, 2, 0, pl.ds(theirs + b, small), :] = (
                outgoing[3, pl.ds(beside + b, small), :]
                + update[0] * mail[1, at, :]
                - update[1] * mail[3, at, :]
            )
            return carry

        loop(rows, small, body, 0, lo)

    def finish_coarse():
        on_res, on_img = marks_of(3)

        def body(b, carry):
            at = pl.ds(b, small)
            coarse_out[0, 0, at, :] = (
                kept[0, at, :] + on_res * kept[1, at, :] - on_img * kept[2, at, :]
            )
            return carry

        loop(ny, small, body)

    @pl.when(jnp.logical_not(has_prev))
    def _():
        pltpu.make_async_copy(start_in.at[0, 0], start_out.at[0, 0], copy_s.at[0]).start()
        pltpu.make_async_copy(start_in.at[0, 0], coarse_out.at[0, 0], copy_s.at[1]).start()

    def gain_send(m, chunk_range):
        for c in chunk_range:
            if c < chunks:
                halo_send(GAIN + m, H_GAIN + m, c, *spans[c])

    def gain_wait(m):
        halo_wait(H_GAIN + m, 0, 0, win)

    gain_send(0, range(0, 2))
    pl.when(has_next)(kept_copy(0).start)
    halo_wait(H_RES, 0, 0, win)
    here = product(0)
    gain_send(0, range(2, 4))
    cross(0, here, local(0))
    gain_send(0, range(4, chunks))
    img_send(0, 1)
    gain_send(1, range(0, 2))
    coarse_residual()
    coarse_send(1, (0,))
    pl.when(has_next)(mail_copy(4).start)
    later(mail.at[4], mail_s.at[4], has_next)
    update = factors(0)
    gain_wait(0)
    img_wait(0, 1)
    advance(0, update)
    here = product(1)
    mail_send(2)
    gain_send(1, range(2, 4))
    cross(1, here, local(1))

    @pl.when(has_next)
    def _():
        mail_copy(4).wait_recv()
        remote(
            mail.at[4], kept.at[1, pl.ds(theirs, half)], kept_s.at[1], kept_r.at[1], t + 1, s
        ).start()

    finish_start(update)
    gain_send(1, range(4, chunks))
    img_send(1, 1)
    gain_wait(1)
    coarse_halo()
    here_coarse = product(3)
    coarse_send(2, (0,))
    coarse_send(2, (1,), early)
    update = factors(1)
    img_wait(1, 1)
    advance(1, update)
    ahead_send(0)
    here = product(2)
    ahead_send(1)
    mail_send(3)
    cross(3, here_coarse, local(3))
    cross(2, here, local(2))
    coarse_send(2, (1,), jnp.logical_not(early))
    finish_second(update)

    def finish_next():
        on_res, on_img = marks_of(4)
        arrived(ahead, kept_r.at[5])

        def body(b, carry):
            at, rows = pl.ds(mine + b, small), pl.ds(b, small)
            start_out[0, 0, at, :] = (
                kept[0, at, :] + on_res * ahead[0, rows, :] - on_img * ahead[1, rows, :]
            )
            return carry

        loop(half, small, body)

    marks_send(3, factors(3))
    mail_copy(3).wait_recv()
    update = factors(2)
    marks_send(4, update)
    pieces = 2 if half % (2 * small) == 0 else 1
    piece = half // pieces
    for c in range(pieces):
        at = theirs + c * piece
        finish_third(update, c * piece, piece)
        copy = remote(
            fine_out.at[0, 2, 0, pl.ds(at, piece)], start_out.at[0, 0, pl.ds(at, piece)],
            end_s.at[0], end_r.at[0], t + 1, s,
        )
        pl.when(has_next)(copy.start)
    finish(2, update, h, half_of(2, mine), 0, half)

    @pl.when(jnp.logical_not(has_prev))
    def _():
        pltpu.make_async_copy(start_in.at[0, 0], start_out.at[0, 0], copy_s.at[0]).wait()
        pltpu.make_async_copy(start_in.at[0, 0], coarse_out.at[0, 0], copy_s.at[1]).wait()

    @pl.when(has_prev)
    def _():
        for k in range(3):
            arrived(kept.at[k], kept_r.at[k])
        finish_coarse()
        finish_next()
        arrived(start_out.at[0, 0, pl.ds(theirs, half)], end_r.at[0])

    each_part(lambda q: sent(outgoing.at[0, pl.ds(*parts[q])], swap_s.at[0]))
    for side, cond in ((0, has_lower), (1, has_upper)):

        @pl.when(cond)
        def _(side=side):
            each_part(
                lambda q: sent(
                    field.at[KAPPA, side, pl.ds(PAD + parts[q][0], parts[q][1])],
                    halo_s.at[side, 0],
                )
            )

    kin_sent(0)
    pl.when(has_lower)(lambda: kin_sent(1))
    pl.when(has_upper)(lambda: kin_sent(2))
    halo_later(NODE, 1, 0, win, 3)
    halo_later(RES, 2, 0, win)
    halo_later(GAIN, 3, 0, win, 2)
    halo_later(IMG, 4, 0, win, 2)
    for side in range(2):
        halo_later(IMG + 2, 5, *pieces_of[0][side], 2, (side,))
    for k in range(3):
        later(kept.at[k], kept_s.at[k], has_next)
    for k in range(2):
        later(marks.at[k], kept_s.at[3 + k], has_next)
    later(ahead, kept_s.at[5], has_next)
    later(fine_out.at[0, 2, 0, pl.ds(theirs, half)], end_s.at[0], has_next)
    later(sums.at[pl.ds(0, 4), pl.ds(0, slabs - 1)], sum_s.at[0])
    for ref, sem, cond in pending:
        if cond is None:
            sent(ref, sem)
        else:
            pl.when(cond)(lambda ref=ref, sem=sem: sent(ref, sem))


def store(fine, begin, coarse, fine_out, start_out, coarse_out, sem):
    pairs = [(begin.at[0, 0], start_out.at[0, 0]), (coarse.at[0, 0], coarse_out.at[0, 0])]
    pairs += [(fine.at[0, m, 0], fine_out.at[0, m, 0]) for m in range(fine.shape[1])]
    copies = []
    for k, (src, dst) in enumerate(pairs):
        rows = src.shape[0] // 2
        for j in range(2):
            at = pl.ds(j * rows, rows)
            copies.append(pltpu.make_async_copy(src.at[at], dst.at[at], sem.at[2 * k + j]))
    for copy in copies:
        copy.start()
    for copy in copies:
        copy.wait()


def solution(mesh):
    slices, slabs = mesh.shape["tm"], mesh.shape["space"]

    def on_device(start_value, old_nodes, diffusivity):
        ny, nz = start_value.shape[2:]
        half = ny // 2
        win = half + PAD
        chunks = len(chunk_bounds(win, tile_of(win, 24)))
        vmem = lambda *shape: pltpu.VMEM(shape, jnp.float32)
        dma = lambda *shape: pltpu.SemaphoreType.DMA(shape)

        def body(*refs):
            kernel(slices, slabs, ny, nz, *refs)

        nodes, ends = pltpu.VMEM(old_nodes.shape, jnp.float32), pltpu.VMEM(start_value.shape, jnp.float32)
        results = pl.pallas_call(
            body,
            out_shape=(nodes, ends, ends),
            in_specs=[pl.BlockSpec(memory_space=pltpu.HBM)] * 3,
            out_specs=(pl.BlockSpec(memory_space=pltpu.VMEM),) * 3,
            scratch_shapes=[
                vmem(FIELDS, 2, win + 2 * PAD, nz),
                vmem(HALOS, win, nz),
                vmem(HALOS, win, nz),
                vmem(4, 2, win, nz),
                vmem(3, win, nz),
                vmem(5, win, nz),
                vmem(half, nz),
                vmem(5, half, nz),
                vmem(3, ny, nz),
                vmem(2, half, nz),
                vmem(4, 8, 128),
                vmem(4, slabs, 4, 128),
                dma(2), dma(4 + 4 * chunks), dma(2), dma(3), dma(3), dma(5), dma(5), dma(6), dma(6),
                dma(2, 6), dma(2, 10 + chunks), dma(1), dma(4),
                dma(1), dma(1), dma(1), dma(1), dma(2),
            ],
            compiler_params=pltpu.CompilerParams(
                collective_id=0, has_side_effects=True, vmem_limit_bytes=61 * 1024 * 1024
            ),
            name="pfasst",
        )(start_value, old_nodes, diffusivity)
        return pl.pallas_call(
            store,
            out_shape=tuple(jax.ShapeDtypeStruct(r.shape, jnp.float32) for r in results),
            in_specs=[pl.BlockSpec(memory_space=pltpu.VMEM)] * 3,
            out_specs=(pl.BlockSpec(memory_space=pltpu.HBM),) * 3,
            scratch_shapes=[dma(4 + 2 * old_nodes.shape[1])],
            compiler_params=pltpu.CompilerParams(vmem_limit_bytes=1024 * 1024),
            name="store",
        )(*results)

    in_specs = (
        P("tm", "space", None, None),
        P("tm", None, "space", None, None),
        P("space", None, None),
    )
    out_specs = (
        P("tm", None, "space", None, None),
        P("tm", "space", None, None),
        P("tm", "space", None, None),
    )
    return jax.shard_map(
        on_device, mesh=mesh, in_specs=in_specs, out_specs=out_specs, check_vma=False
    )
```

```python
import math

import jax
import jax.numpy as jnp
from jax import lax
from jax.experimental import pallas as pl
from jax.experimental.pallas import tpu as pltpu
from jax.sharding import PartitionSpec as P

STEP = 2.0
ROOT_SIX = math.sqrt(6.0)
NODE_TIMES = [(4.0 - ROOT_SIX) / 10.0, (4.0 + ROOT_SIX) / 10.0, 1.0]
COLLOC = [
    [
        (88.0 - 7.0 * ROOT_SIX) / 360.0,
        (296.0 - 169.0 * ROOT_SIX) / 1800.0,
        (-2.0 + 3.0 * ROOT_SIX) / 225.0,
    ],
    [
        (296.0 + 169.0 * ROOT_SIX) / 1800.0,
        (88.0 + 7.0 * ROOT_SIX) / 360.0,
        (-2.0 - 3.0 * ROOT_SIX) / 225.0,
    ],
    [(16.0 - ROOT_SIX) / 36.0, (16.0 + ROOT_SIX) / 36.0, 1.0 / 9.0],
]
MESH = pl.DeviceIdType.MESH
PAD = 8
UNROLL = 16
SHARES = (1, 1)

KAPPA, NODE, START, RES, IMG, GAIN = 0, 1, 4, 5, 9, 13
FIELDS = 15
H_KAPPA, H_NODE, H_RES, H_IMG, H_GAIN = 0, 1, 4, 8, 12
HALOS = 14


def sweep_weight(row, column):
    below = COLLOC[row - 1][column] if row > 0 else 0.0
    return COLLOC[row][column] - below


def node_width(row):
    below = NODE_TIMES[row - 1] if row > 0 else 0.0
    return NODE_TIMES[row] - below


WIDTHS = [STEP * node_width(0), STEP * node_width(1), STEP * node_width(2), STEP]


def chunk_bounds(rows, tile):
    tiles = rows // tile
    parts = min(4, tiles)
    counts = [tiles // parts + (c < tiles % parts) for c in range(parts)]
    if counts[-1] > 1:
        counts[-1] -= 1
        counts[1 if parts > 2 else 0] += 1
    cuts = [tile * sum(counts[:c]) for c in range(parts + 1)]
    return [(cuts[c], cuts[c + 1] - cuts[c]) for c in range(parts)]


def tile_of(rows, most):
    best = 8
    for size in range(8, most + 1, 8):
        if rows % size == 0:
            best = size
    return best


def kernel(
    slices, slabs, ny, nz,
    start_in, nodes_in, kappa_in,
    fine_out, start_out, coarse_out,
    field, lower, upper, faces, across, outgoing, result, mail, kept, ahead, marks, sums,
    swap_s, swap_r, own_s, kin_s, kin_r, mail_s, mail_r, kept_s, kept_r, halo_s, halo_r, sum_s, sum_r, out_s, out_r, end_s, end_r, copy_s,
):
    f32 = jnp.float32
    t = lax.axis_index("tm")
    s = lax.axis_index("space")
    h = lax.rem(s, 2)
    p = lax.div(s, 2)
    pairs = slabs // 2
    half = ny // 2
    win = half + PAD
    other = 1 - h
    partner = s + 1 - 2 * h
    team = next(n for n in (4, 2, 1) if slices % n == 0)
    rank = lax.rem(t, team)
    early = lax.rem(t, 2) == 1
    first_row = pl.multiple_of(h * (half - PAD), 8)
    partner_row = pl.multiple_of(other * (half - PAD), 8)
    own = pl.multiple_of(PAD * h, 8)
    mine = pl.multiple_of(h * half, 8)
    has_next = t < slices - 1
    has_prev = t > 0
    has_lower = p > 0
    has_upper = p < pairs - 1
    pending = []

    def later(ref, sem, cond=None):
        pending.append((ref, sem, cond))

    def remote(src, dst, send, recv, tm, space):
        return pltpu.make_async_remote_copy(
            src_ref=src, dst_ref=dst, send_sem=send, recv_sem=recv,
            device_id=(tm, space), device_id_type=MESH,
        )

    barrier = pltpu.get_barrier_semaphore()

    def greet(d, carry):
        pl.semaphore_signal(
            barrier, inc=1, device_id=(t, lax.rem(s + d, slabs)), device_id_type=MESH
        )
        return carry

    lax.fori_loop(1, slabs, greet, 0)
    for cond, tm in ((has_next, t + 1), (has_prev, t - 1)):

        @pl.when(cond)
        def _(tm=tm):
            for space in (s, partner):
                pl.semaphore_signal(barrier, inc=1, device_id=(tm, space), device_id_type=MESH)

    far = [jnp.abs(rank - q) > 1 for q in range(team)]
    for q in range(team):

        @pl.when(far[q])
        def _(q=q):
            pl.semaphore_signal(
                barrier, inc=1, device_id=(t - rank + q, s), device_id_type=MESH
            )

    sources = [kappa_in.at[0]] + [nodes_in.at[0, j, 0] for j in range(3)] + [start_in.at[0, 0]]
    for k, source in enumerate(sources):
        pltpu.make_async_copy(
            source.at[pl.ds(first_row, win)], field.at[k, h, pl.ds(PAD, win)], own_s.at[0]
        ).start()
        pltpu.make_async_copy(
            source.at[pl.ds(partner_row, win)], outgoing.at[k], own_s.at[1]
        ).start()

    zeros = jnp.zeros((PAD, nz), f32)
    for k in range(FIELDS):
        for slab in range(2):
            field[k, slab, 0:PAD, :] = zeros
            field[k, slab, win + PAD : win + 2 * PAD, :] = zeros

    def clear(ref):
        def body(i, carry):
            for k in range(HALOS):
                ref[k, pl.ds(pl.multiple_of(i * 8, 8), 8), :] = zeros
            return carry

        lax.fori_loop(0, win // 8, body, 0)

    @pl.when(jnp.logical_not(has_lower))
    def _():
        clear(lower)

    @pl.when(jnp.logical_not(has_upper))
    def _():
        clear(upper)

    pl.semaphore_wait(
        barrier,
        slabs - 1 + 2 * has_next.astype(jnp.int32) + 2 * has_prev.astype(jnp.int32)
        + sum(f.astype(jnp.int32) for f in far),
    )

    tile = tile_of(win, 24)
    bounds = chunk_bounds(win, tile)
    chunks = len(bounds)

    weights = [SHARES[q % 2] for q in range(team)]
    cuts = [8 * (win // 8 * sum(weights[:q]) // sum(weights)) for q in range(team)] + [win]
    parts = [(cuts[q], cuts[q + 1] - cuts[q]) for q in range(team)]

    def bounds_of(k, c):
        return bounds[c] if k else parts[c]

    def each_part(body):
        for q in range(team):
            if parts[q][1]:
                pl.when(rank == q)(lambda q=q: body(q))

    def arrived(ref, sem):
        remote(ref, ref, sum_s.at[0], sem, t, partner).wait_recv()

    def sent(ref, sem):
        remote(ref, ref, sem, sum_r.at[0], t, partner).wait_send()

    def swap_sem(k, c):
        return swap_r.at[1 + (k - 1) * chunks + c if k else 0]

    def swap_start(k, c):
        lo, rows = bounds_of(k, c)
        remote(
            outgoing.at[k, pl.ds(lo, rows)], field.at[k, h, pl.ds(PAD + lo, rows)],
            swap_s.at[min(k, 1)], swap_sem(k, c), t, partner,
        ).start()

    def swap_wait(k, c):
        lo, rows = bounds_of(k, c)
        arrived(field.at[k, other, pl.ds(PAD + lo, rows)], swap_sem(k, c))

    def kin_ref(e, lo, rows):
        if e == 0:
            return field.at[KAPPA, other, pl.ds(PAD + lo, rows)]
        return (lower, upper)[e - 1].at[H_KAPPA, pl.ds(lo, rows)]

    def kin_start(e, q):
        ref = kin_ref(e, *parts[q])
        for peer in range(team):
            if peer != q:
                remote(ref, ref, kin_s.at[e], kin_r.at[e], t - q + peer, s).start()

    def kin_wait(e):
        for q in range(team):
            rows = win - parts[q][1]
            if rows:
                pl.when(rank == q)(lambda rows=rows: arrived(kin_ref(e, 0, rows), kin_r.at[e]))

    def kin_sent(e):
        if team > 1:
            each_part(
                lambda q: sent(field.at[pl.ds(0, team - 1), 0, pl.ds(0, parts[q][1])], kin_s.at[e])
            )

    pltpu.make_async_copy(outgoing, outgoing, own_s.at[1]).wait()
    each_part(lambda q: swap_start(0, q))
    for c in range(chunks):
        for k in range(1, 4):
            swap_start(k, c)
    for c in range(chunks):
        swap_start(4, c)
    later(outgoing.at[pl.ds(1, 4)], swap_s.at[1])

    def halo_sems(k, c, side):
        if k == H_KAPPA:
            slots = 0, 0
        elif k < H_RES:
            slots = 1, 1 + c
        elif k == H_RES:
            slots = 2, 1 + chunks
        elif k >= H_GAIN:
            slots = 3, 2 + chunks + k - H_GAIN
        else:
            m = k - H_IMG
            slots = 4 + m // 2, 4 + chunks + (2 * m + c if m < 2 else 2 + m)
        return halo_s.at[side, slots[0]], halo_r.at[side, slots[1]]

    def down(f, k, c, lo, rows):
        return remote(
            field.at[f, 0, pl.ds(PAD + lo, rows)], upper.at[k, pl.ds(lo, rows)],
            *halo_sems(k, c, 0), t, s - 2,
        )

    def up(f, k, c, lo, rows):
        return remote(
            field.at[f, 1, pl.ds(PAD + lo, rows)], lower.at[k, pl.ds(lo, rows)],
            *halo_sems(k, c, 1), t, s + 2,
        )

    def first_hop(k, c, which):
        @pl.when(jnp.logical_and(which == 0, has_lower))
        def _():
            down(k, k, c, *bounds_of(k, c)).start()

        @pl.when(jnp.logical_and(which == 1, has_upper))
        def _():
            up(k, k, c, *bounds_of(k, c)).start()

    own_rows = field.at[pl.ds(0, 5), h, pl.ds(PAD, win)]
    pltpu.make_async_copy(own_rows, own_rows, own_s.at[0]).wait()
    each_part(lambda q: first_hop(0, q, h))
    for c in range(chunks):
        for k in range(1, 4):
            first_hop(k, c, h)

    def halo_wait(k, c, lo, rows, sides=(0, 1), fields=None):
        which = k if fields is None else pl.ds(k, fields)
        for side, ref, cond in ((0, upper, has_upper), (1, lower, has_lower)):
            if side in sides:

                @pl.when(cond)
                def _(side=side, ref=ref):
                    arrived(ref.at[which, pl.ds(lo, rows)], halo_sems(k, c, side)[1])

    def halo_later(f, slot, lo, rows, fields=None, sides=(0, 1)):
        which = f if fields is None else pl.ds(f, fields)
        for side in sides:
            ref = field.at[which, side, pl.ds(PAD + lo, rows)]
            later(ref, halo_s.at[side, slot], (has_lower, has_upper)[side])

    lane = lax.broadcasted_iota(jnp.int32, (tile, nz), 1)

    def loop(rows, size, body, init=0, offset=0):
        def step(i, carry):
            return body(pl.multiple_of(offset + i * size, 8), carry)

        count = rows // size
        return lax.fori_loop(0, count, step, init, unroll=max(u for u in range(1, UNROLL + 1) if count % u == 0))

    def coefficients(b, carry):
        windows = [field[KAPPA, slab, pl.ds(b, tile + 2 * PAD), :] for slab in range(2)]
        centre = [w[PAD : PAD + tile] for w in windows]
        before = 0.5 * (centre[0] + lower[H_KAPPA, pl.ds(b, tile), :])
        between = 0.5 * (centre[0] + centre[1])
        after = 0.5 * (centre[1] + upper[H_KAPPA, pl.ds(b, tile), :])
        across[0, pl.ds(b, tile), :] = before
        across[1, pl.ds(b, tile), :] = between
        across[2, pl.ds(b, tile), :] = after
        ends = [before + between, between + after]
        for slab in range(2):
            w, k = windows[slab], centre[slab]
            above = 0.5 * (k + w[PAD - 1 : PAD - 1 + tile])
            below = 0.5 * (k + w[PAD + 1 : PAD + 1 + tile])
            right = jnp.where(lane == nz - 1, 0.0, pltpu.roll(k, nz - 1, axis=1))
            left = jnp.where(lane == 0, 0.0, pltpu.roll(k, 1, axis=1))
            right_face = 0.5 * (k + right)
            left_face = 0.5 * (k + left)
            faces[0, slab, pl.ds(b, tile), :] = above
            faces[1, slab, pl.ds(b, tile), :] = below
            faces[2, slab, pl.ds(b, tile), :] = jnp.where(lane == nz - 1, 0.0, right_face)
            faces[3, slab, pl.ds(b, tile), :] = ends[slab] + above + below + right_face + left_face
        return carry

    def heat(windows, outer, b, size):
        centre = [w[PAD : PAD + size] for w in windows]
        between = across[1, pl.ds(b, size), :]
        images = []
        for slab in range(2):
            w, v = windows[slab], centre[slab]
            fz = faces[2, slab, pl.ds(b, size), :]
            value = between * centre[1 - slab]
            if outer[slab] is not None:
                value = value + outer[slab]
            value = value + faces[0, slab, pl.ds(b, size), :] * w[PAD - 1 : PAD - 1 + size]
            value = value + faces[1, slab, pl.ds(b, size), :] * w[PAD + 1 : PAD + 1 + size]
            value = value + fz * pltpu.roll(v, nz - 1, axis=1) + pltpu.roll(fz * v, 1, axis=1)
            images.append(value - faces[3, slab, pl.ds(b, size), :] * v)
        return centre, images

    def plain_heat(f, k, b, size):
        windows = [field[f, slab, pl.ds(b, size + 2 * PAD), :] for slab in range(2)]
        outer = (
            across[0, pl.ds(b, size), :] * lower[k, pl.ds(b, size), :],
            across[2, pl.ds(b, size), :] * upper[k, pl.ds(b, size), :],
        )
        return heat(windows, outer, b, size)

    def folded(value):
        return jnp.sum(value.reshape(-1, 8, nz), axis=0)

    def each_slab(body):
        if slabs <= 16:
            for d in range(1, slabs):
                body(d)
        else:

            def step(d, carry):
                body(d)
                return carry

            lax.fori_loop(1, slabs, step, 0)

    def sum_copy(m, d):
        return remote(
            sums.at[m, s], sums.at[m, s], sum_s.at[0], sum_r.at[m], t, lax.rem(s + d, slabs),
        )

    def sum_start(m, parts):
        for row, part in enumerate(parts):
            flat = jnp.sum(part, axis=0, keepdims=True)
            line = flat[:, 0:128]
            for at in range(128, nz, 128):
                line = line + flat[:, at : at + 128]
            sums[m, s, row : row + 1, :] = line
        each_slab(lambda d: sum_copy(m, d).start())

    def sum_wait(m):
        arrived(sums.at[m, pl.ds(0, slabs - 1)], sum_r.at[m])
        total = jnp.sum(sums[m], axis=0)
        total = jnp.sum(total, axis=1, keepdims=True)
        return [total[row : row + 1, :] for row in range(4)]

    def halo_send(f, k, c, lo, rows):
        pl.when(has_lower)(down(f, k, c, lo, rows).start)
        pl.when(has_upper)(up(f, k, c, lo, rows).start)

    quarter = half // 2
    set_up = own
    set_down = pl.multiple_of(own + quarter, 8)
    pieces_of = (
        ((quarter, quarter + PAD), (0, quarter + PAD)),
        ((0, quarter), (quarter + PAD, quarter)),
    )

    def rows_of(m, piece):
        if m < 2:
            return pieces_of[piece]
        return (set_down, quarter), (set_up, quarter)

    def img_send(m, piece):
        (lo_d, rows_d), (lo_u, rows_u) = rows_of(m, piece)
        pl.when(has_lower)(down(IMG + m, H_IMG + m, piece, lo_d, rows_d).start)
        pl.when(has_upper)(up(IMG + m, H_IMG + m, piece, lo_u, rows_u).start)

    def img_wait(m, piece):
        for side in range(2):
            halo_wait(H_IMG + m, piece, *rows_of(m, piece)[side], (side,))

    nothing = jnp.zeros((8, nz), f32)

    def product(m):
        def body(b, carry):
            centre, images = plain_heat(RES + m, H_RES + m, b, tile)
            row = lax.broadcasted_iota(jnp.int32, (tile, nz), 0) + b
            inside = jnp.logical_and(row >= own, row < own + half)
            norm, along = carry
            for slab in range(2):
                v = centre[slab]
                w = -WIDTHS[m] * images[slab]
                field[IMG + m, slab, pl.ds(PAD + b, tile), :] = w
                masked = jnp.where(inside, v, 0.0)
                norm = norm + folded(masked * v)
                along = along + folded(masked * w)
            return norm, along

        sums_here = loop(win, tile, body, (nothing, nothing))
        img_send(m, 0)
        return sums_here

    small = tile_of(quarter, 32)

    def local(m):
        def body(b, carry):
            windows = [field[IMG + m, slab, pl.ds(b, small + 2 * PAD), :] for slab in range(2)]
            centre, images = heat(windows, (None, None), b, small)
            norm, along = carry
            for slab in range(2):
                v = centre[slab]
                norm = norm + folded(v * v)
                along = along + folded(v * images[slab])
            return norm, along

        return loop(half, small, body, (nothing, nothing), own)

    def cross(m, sums_here, sums_local):
        img_wait(m, 0)

        def body_of(side):
            ref = lower if side == 0 else upper

            def body(b, carry):
                rows = pl.ds(b, small)
                edge = across[2 * side, rows, :] * ref[H_IMG + m, rows, :]
                return carry + folded(edge * field[IMG + m, side, pl.ds(PAD + b, small), :])

            return body

        outer = loop(quarter, small, body_of(0), nothing, set_up)
        outer = loop(quarter, small, body_of(1), outer, set_down)
        norm, along = sums_local
        sum_start(m, sums_here + (norm, -WIDTHS[m] * (along + 2.0 * outer)))

    def factors(m):
        rr, rw, ww, wbw = sum_wait(m)
        step_size = rr / (rr + rw)
        mean = rw / rr
        square = step_size * step_size
        norm_next = square * jnp.maximum(ww - mean * rw, 0.0)
        along = square * jnp.maximum(mean * mean * rw - 2.0 * mean * ww + wbw, 0.0)
        momentum = norm_next / rr
        below = norm_next * (1.0 + momentum)
        curve = jnp.maximum(norm_next + along - momentum * norm_next / step_size, below)
        step_next = norm_next / jnp.maximum(curve, 1e-37)
        on_image = step_size * step_next
        return step_size + step_next * (1.0 + momentum) - on_image, on_image

    def advance(m, scalars):
        on_res, on_img = scalars

        def body(b, carry):
            at = pl.ds(PAD + b, tile)
            rows = pl.ds(b, tile)
            for slab in range(2):
                field[RES + m + 1, slab, at, :] = (
                    field[GAIN + m, slab, at, :]
                    + on_res * field[RES + m, slab, at, :]
                    - on_img * field[IMG + m, slab, at, :]
                )
            for ref in (lower, upper):
                ref[H_RES + m + 1, rows, :] = (
                    ref[H_GAIN + m, rows, :]
                    + on_res * ref[H_RES + m, rows, :]
                    - on_img * ref[H_IMG + m, rows, :]
                )
            return carry

        loop(win, tile, body)

    def coarse_residual():
        def body(b, carry):
            at = pl.ds(PAD + b, tile)
            for slab in range(2):
                field[RES + 3, slab, at, :] = (
                    field[RES, slab, at, :] + field[GAIN, slab, at, :] + field[GAIN + 1, slab, at, :]
                )
            return carry

        loop(win, tile, body)

    def coarse_halo():
        def body(b, carry):
            rows = pl.ds(b, tile)
            for ref in (lower, upper):
                ref[H_RES + 3, rows, :] = (
                    ref[H_RES, rows, :] + ref[H_GAIN, rows, :] + ref[H_GAIN + 1, rows, :]
                )
            return carry

        loop(win, tile, body)

    mailed = (GAIN, GAIN + 1, IMG + 1, IMG + 2, RES + 3)

    def mail_copy(k):
        return remote(
            field.at[mailed[k], other, pl.ds(PAD + own, half)], mail.at[k],
            mail_s.at[k], mail_r.at[k], t, partner,
        )

    def mail_send(k):
        mail_copy(k).start()
        later(mail.at[k], mail_s.at[k])

    def coarse_send(k, which=(0, 1), cond=True):
        for slab, space in [((h, s), (other, partner))[w] for w in which]:
            copy = remote(
                field.at[(RES + 3, IMG + 3)[k - 1], slab, pl.ds(PAD + own, half)],
                kept.at[k, pl.ds(mine, half)], kept_s.at[k], kept_r.at[k], t + 1, space,
            )
            pl.when(jnp.logical_and(has_next, cond))(copy.start)

    def kept_copy(k):
        if k == 0:
            src, dst = nodes_in.at[0, 2, 0], kept.at[0]
        else:
            src, dst = marks.at[k - 3], marks.at[k - 1]
        return remote(src, dst, kept_s.at[k], kept_r.at[k], t + 1, s)

    def marks_send(k, update):
        for row in range(2):
            marks[k - 3, row : row + 1, :] = jnp.broadcast_to(update[row], (1, 128))
        pl.when(has_next)(kept_copy(k).start)

    def marks_of(k):
        arrived(marks.at[k - 1], kept_r.at[k])
        return marks[k - 1, 0:1, 0:1], marks[k - 1, 1:2, 0:1]

    def ahead_send(e):
        copy = remote(
            field.at[(RES + 2, IMG + 2)[e], h, pl.ds(PAD + own, half)], ahead.at[e],
            kept_s.at[5], kept_r.at[5], t + 1, s,
        )
        pl.when(has_next)(copy.start)

    def finish(m, scalars, slab, ref, lo, rows):
        on_res, on_img = scalars
        node = NODE + min(m, 2)

        def body(b, carry):
            at = pl.ds(PAD + own + b, small)
            ref[pl.ds(b, small), :] = (
                field[node, slab, at, :]
                + on_res * field[RES + m, slab, at, :]
                - on_img * field[IMG + m, slab, at, :]
            )
            return carry

        loop(rows, small, body, 0, lo)

    def residuals(b, carry):
        images = [plain_heat(NODE + j, H_NODE + j, b, tile)[1] for j in range(3)]
        at = pl.ds(PAD + b, tile)
        for slab in range(2):
            nodes = [field[NODE + j, slab, at, :] for j in range(3)]
            for row, f in enumerate((RES, GAIN, GAIN + 1)):
                value = nodes[row - 1] - nodes[row] if row else -nodes[0]
                for j in range(3):
                    value = value + (STEP * sweep_weight(row, j)) * images[j][slab]
                field[f, slab, at, :] = value
        return carry

    spans = []
    for c, (lo, rows) in enumerate(bounds):
        begin = lo - tile if c else 0
        end = lo + rows - (tile if c < chunks - 1 else 0)
        spans.append((begin, end - begin))

    def begin_rows(c):
        halo_wait(H_NODE, c, *bounds[c], fields=3)
        lo, rows = spans[c]
        loop(rows, tile, coefficients, 0, lo)
        loop(rows, tile, residuals, 0, lo)

    def add_start(b, carry):
        at = pl.ds(PAD + b, tile)
        for slab in range(2):
            field[RES, slab, at, :] = field[RES, slab, at, :] + field[START, slab, at, :]
        return carry

    def begin_res(c):
        swap_wait(4, c)
        lo, rows = spans[c]
        loop(rows, tile, add_start, 0, lo)
        halo_send(RES, H_RES, c, lo, rows)

    def pass_kappa(q):
        swap_wait(0, q)
        kin_start(0, q)
        first_hop(0, q, other)

    each_part(pass_kappa)
    for c in range(chunks):
        for k in range(1, 4):
            swap_wait(k, c)
            first_hop(k, c, other)
        if c == 0:
            each_part(lambda q: halo_wait(H_KAPPA, 0, *parts[q]))
            pl.when(has_lower)(lambda: each_part(lambda q: kin_start(1, q)))
            pl.when(has_upper)(lambda: each_part(lambda q: kin_start(2, q)))
        if c == min(1, chunks - 1):
            kin_wait(0)
            pl.when(has_lower)(lambda: kin_wait(1))
            pl.when(has_upper)(lambda: kin_wait(2))
        if c > 0:
            begin_rows(c - 1)
    for c in range(chunks):
        if c == chunks - 1:
            begin_rows(c)
        begin_res(c)
    mail_send(0)
    mail_send(1)
    theirs = pl.multiple_of(other * half, 8)
    beside = pl.multiple_of(PAD * other, 8)

    def half_of(m, at):
        return fine_out.at[0, m, 0, pl.ds(at, half)]

    def finish_start(update):
        finish(0, update, other, result, 0, half)
        remote(result, half_of(0, mine), out_s.at[0], out_r.at[0], t, partner).start()
        later(result, out_s.at[0])
        finish(0, update, h, half_of(0, mine), 0, half)

    def finish_second(update):
        finish(1, update, h, half_of(1, mine), 0, half)
        arrived(half_of(0, theirs), out_r.at[0])
        for k in range(3):
            mail_copy(k).wait_recv()

        def body(b, carry):
            rows, at = pl.ds(b, small), pl.ds(beside + b, small)
            there = pl.ds(theirs + b, small)
            residual = fine_out[0, 0, 0, there, :] - outgoing[1, at, :] + mail[0, rows, :]
            step = update[0] * residual - update[1] * mail[2, rows, :]
            fine_out[0, 1, 0, there, :] = outgoing[2, at, :] + step
            mail[1, rows, :] = mail[1, rows, :] + step
            return carry

        loop(half, small, body)

    def finish_third(update, lo, rows):
        def body(b, carry):
            at = pl.ds(b, small)
            fine_out[0, 2, 0, pl.ds(theirs + b, small), :] = (
                outgoing[3, pl.ds(beside + b, small), :]
                + update[0] * mail[1, at, :]
                - update[1] * mail[3, at, :]
            )
            return carry

        loop(rows, small, body, 0, lo)

    def finish_coarse():
        on_res, on_img = marks_of(3)

        def body(b, carry):
            at = pl.ds(b, small)
            coarse_out[0, 0, at, :] = (
                kept[0, at, :] + on_res * kept[1, at, :] - on_img * kept[2, at, :]
            )
            return carry

        loop(ny, small, body)

    @pl.when(jnp.logical_not(has_prev))
    def _():
        pltpu.make_async_copy(start_in.at[0, 0], start_out.at[0, 0], copy_s.at[0]).start()
        pltpu.make_async_copy(start_in.at[0, 0], coarse_out.at[0, 0], copy_s.at[1]).start()

    def gain_send(m, chunk_range):
        for c in chunk_range:
            if c < chunks:
                halo_send(GAIN + m, H_GAIN + m, c, *spans[c])

    def gain_wait(m):
        halo_wait(H_GAIN + m, 0, 0, win)

    gain_send(0, range(0, 2))
    pl.when(has_next)(kept_copy(0).start)
    halo_wait(H_RES, 0, 0, win)
    here = product(0)
    gain_send(0, range(2, 4))
    cross(0, here, local(0))
    gain_send(0, range(4, chunks))
    img_send(0, 1)
    gain_send(1, range(0, 2))
    coarse_residual()
    coarse_send(1, (0,))
    pl.when(has_next)(mail_copy(4).start)
    later(mail.at[4], mail_s.at[4], has_next)
    update = factors(0)
    gain_wait(0)
    img_wait(0, 1)
    advance(0, update)
    here = product(1)
    mail_send(2)
    gain_send(1, range(2, 4))
    cross(1, here, local(1))

    @pl.when(has_next)
    def _():
        mail_copy(4).wait_recv()
        remote(
            mail.at[4], kept.at[1, pl.ds(theirs, half)], kept_s.at[1], kept_r.at[1], t + 1, s
        ).start()

    finish_start(update)
    gain_send(1, range(4, chunks))
    img_send(1, 1)
    gain_wait(1)
    coarse_halo()
    here_coarse = product(3)
    coarse_send(2, (0,))
    coarse_send(2, (1,), early)
    update = factors(1)
    img_wait(1, 1)
    advance(1, update)
    ahead_send(0)
    here = product(2)
    ahead_send(1)
    mail_send(3)
    cross(3, here_coarse, local(3))
    cross(2, here, local(2))
    coarse_send(2, (1,), jnp.logical_not(early))
    finish_second(update)

    def finish_next():
        on_res, on_img = marks_of(4)
        arrived(ahead, kept_r.at[5])

        def body(b, carry):
            at, rows = pl.ds(mine + b, small), pl.ds(b, small)
            start_out[0, 0, at, :] = (
                kept[0, at, :] + on_res * ahead[0, rows, :] - on_img * ahead[1, rows, :]
            )
            return carry

        loop(half, small, body)

    marks_send(3, factors(3))
    mail_copy(3).wait_recv()
    update = factors(2)
    marks_send(4, update)
    pieces = 2 if half % (2 * small) == 0 else 1
    piece = half // pieces
    for c in range(pieces):
        at = theirs + c * piece
        finish_third(update, c * piece, piece)
        copy = remote(
            fine_out.at[0, 2, 0, pl.ds(at, piece)], start_out.at[0, 0, pl.ds(at, piece)],
            end_s.at[0], end_r.at[0], t + 1, s,
        )
        pl.when(has_next)(copy.start)
    finish(2, update, h, half_of(2, mine), 0, half)

    @pl.when(jnp.logical_not(has_prev))
    def _():
        pltpu.make_async_copy(start_in.at[0, 0], start_out.at[0, 0], copy_s.at[0]).wait()
        pltpu.make_async_copy(start_in.at[0, 0], coarse_out.at[0, 0], copy_s.at[1]).wait()

    @pl.when(has_prev)
    def _():
        for k in range(3):
            arrived(kept.at[k], kept_r.at[k])
        finish_coarse()
        finish_next()
        arrived(start_out.at[0, 0, pl.ds(theirs, half)], end_r.at[0])

    each_part(lambda q: sent(outgoing.at[0, pl.ds(*parts[q])], swap_s.at[0]))
    for side, cond in ((0, has_lower), (1, has_upper)):

        @pl.when(cond)
        def _(side=side):
            each_part(
                lambda q: sent(
                    field.at[KAPPA, side, pl.ds(PAD + parts[q][0], parts[q][1])],
                    halo_s.at[side, 0],
                )
            )

    kin_sent(0)
    pl.when(has_lower)(lambda: kin_sent(1))
    pl.when(has_upper)(lambda: kin_sent(2))
    halo_later(NODE, 1, 0, win, 3)
    halo_later(RES, 2, 0, win)
    halo_later(GAIN, 3, 0, win, 2)
    halo_later(IMG, 4, 0, win, 2)
    for side in range(2):
        halo_later(IMG + 2, 5, *rows_of(2, 0)[side], 2, (side,))
    for k in range(3):
        later(kept.at[k], kept_s.at[k], has_next)
    for k in range(2):
        later(marks.at[k], kept_s.at[3 + k], has_next)
    later(ahead, kept_s.at[5], has_next)
    later(fine_out.at[0, 2, 0, pl.ds(theirs, half)], end_s.at[0], has_next)
    later(sums.at[pl.ds(0, 4), pl.ds(0, slabs - 1)], sum_s.at[0])
    for ref, sem, cond in pending:
        if cond is None:
            sent(ref, sem)
        else:
            pl.when(cond)(lambda ref=ref, sem=sem: sent(ref, sem))


def store(fine, begin, coarse, fine_out, start_out, coarse_out, sem):
    pairs = [(begin.at[0, 0], start_out.at[0, 0]), (coarse.at[0, 0], coarse_out.at[0, 0])]
    pairs += [(fine.at[0, m, 0], fine_out.at[0, m, 0]) for m in range(fine.shape[1])]
    copies = []
    for k, (src, dst) in enumerate(pairs):
        rows = src.shape[0] // 2
        for j in range(2):
            at = pl.ds(j * rows, rows)
            copies.append(pltpu.make_async_copy(src.at[at], dst.at[at], sem.at[2 * k + j]))
    for copy in copies:
        copy.start()
    for copy in copies:
        copy.wait()


def solution(mesh):
    slices, slabs = mesh.shape["tm"], mesh.shape["space"]

    def on_device(start_value, old_nodes, diffusivity):
        ny, nz = start_value.shape[2:]
        half = ny // 2
        win = half + PAD
        chunks = len(chunk_bounds(win, tile_of(win, 24)))
        vmem = lambda *shape: pltpu.VMEM(shape, jnp.float32)
        dma = lambda *shape: pltpu.SemaphoreType.DMA(shape)

        def body(*refs):
            kernel(slices, slabs, ny, nz, *refs)

        nodes, ends = pltpu.VMEM(old_nodes.shape, jnp.float32), pltpu.VMEM(start_value.shape, jnp.float32)
        results = pl.pallas_call(
            body,
            out_shape=(nodes, ends, ends),
            in_specs=[pl.BlockSpec(memory_space=pltpu.HBM)] * 3,
            out_specs=(pl.BlockSpec(memory_space=pltpu.VMEM),) * 3,
            scratch_shapes=[
                vmem(FIELDS, 2, win + 2 * PAD, nz),
                vmem(HALOS, win, nz),
                vmem(HALOS, win, nz),
                vmem(4, 2, win, nz),
                vmem(3, win, nz),
                vmem(5, win, nz),
                vmem(half, nz),
                vmem(5, half, nz),
                vmem(3, ny, nz),
                vmem(2, half, nz),
                vmem(4, 8, 128),
                vmem(4, slabs, 4, 128),
                dma(2), dma(1 + 4 * chunks), dma(2), dma(3), dma(3), dma(5), dma(5), dma(6), dma(6),
                dma(2, 6), dma(2, 10 + chunks), dma(1), dma(4),
                dma(1), dma(1), dma(1), dma(1), dma(2),
            ],
            compiler_params=pltpu.CompilerParams(
                collective_id=0, has_side_effects=True, vmem_limit_bytes=61 * 1024 * 1024
            ),
            name="pfasst",
        )(start_value, old_nodes, diffusivity)
        return pl.pallas_call(
            store,
            out_shape=tuple(jax.ShapeDtypeStruct(r.shape, jnp.float32) for r in results),
            in_specs=[pl.BlockSpec(memory_space=pltpu.VMEM)] * 3,
            out_specs=(pl.BlockSpec(memory_space=pltpu.HBM),) * 3,
            scratch_shapes=[dma(4 + 2 * old_nodes.shape[1])],
            compiler_params=pltpu.CompilerParams(vmem_limit_bytes=1024 * 1024),
            name="store",
        )(*results)

    in_specs = (
        P("tm", "space", None, None),
        P("tm", None, "space", None, None),
        P("space", None, None),
    )
    out_specs = (
        P("tm", None, "space", None, None),
        P("tm", "space", None, None),
        P("tm", "space", None, None),
    )
    return jax.shard_map(
        on_device, mesh=mesh, in_specs=in_specs, out_specs=out_specs, check_vma=False
    )
```

```python
import math

import jax
import jax.numpy as jnp
from jax import lax
from jax.experimental import pallas as pl
from jax.experimental.pallas import tpu as pltpu
from jax.sharding import PartitionSpec as P

STEP = 2.0
ROOT_SIX = math.sqrt(6.0)
NODE_TIMES = [(4.0 - ROOT_SIX) / 10.0, (4.0 + ROOT_SIX) / 10.0, 1.0]
COLLOC = [
    [
        (88.0 - 7.0 * ROOT_SIX) / 360.0,
        (296.0 - 169.0 * ROOT_SIX) / 1800.0,
        (-2.0 + 3.0 * ROOT_SIX) / 225.0,
    ],
    [
        (296.0 + 169.0 * ROOT_SIX) / 1800.0,
        (88.0 + 7.0 * ROOT_SIX) / 360.0,
        (-2.0 - 3.0 * ROOT_SIX) / 225.0,
    ],
    [(16.0 - ROOT_SIX) / 36.0, (16.0 + ROOT_SIX) / 36.0, 1.0 / 9.0],
]
MESH = pl.DeviceIdType.MESH
PAD = 8
UNROLL = 16
SHARES = (1, 1)

KAPPA, NODE, START, RES, IMG, GAIN = 0, 1, 4, 5, 9, 13
FIELDS = 15
H_KAPPA, H_NODE, H_RES, H_IMG, H_GAIN = 0, 1, 4, 8, 12
HALOS = 14


def sweep_weight(row, column):
    below = COLLOC[row - 1][column] if row > 0 else 0.0
    return COLLOC[row][column] - below


def node_width(row):
    below = NODE_TIMES[row - 1] if row > 0 else 0.0
    return NODE_TIMES[row] - below


WIDTHS = [STEP * node_width(0), STEP * node_width(1), STEP * node_width(2), STEP]


def chunk_bounds(rows, tile):
    tiles = rows // tile
    parts = min(4, tiles)
    counts = [tiles // parts + (c < tiles % parts) for c in range(parts)]
    if counts[-1] > 1:
        counts[-1] -= 1
        counts[1 if parts > 2 else 0] += 1
    cuts = [tile * sum(counts[:c]) for c in range(parts + 1)]
    return [(cuts[c], cuts[c + 1] - cuts[c]) for c in range(parts)]


def tile_of(rows, most):
    best = 8
    for size in range(8, most + 1, 8):
        if rows % size == 0:
            best = size
    return best


def kernel(
    slices, slabs, ny, nz,
    start_in, nodes_in, kappa_in,
    fine_out, start_out, coarse_out,
    field, lower, upper, faces, across, outgoing, result, mail, kept, ahead, marks, sums,
    swap_s, swap_r, own_s, kin_s, kin_r, mail_s, mail_r, kept_s, kept_r, halo_s, halo_r, sum_s, sum_r, out_s, out_r, end_s, end_r, copy_s,
):
    f32 = jnp.float32
    t = lax.axis_index("tm")
    s = lax.axis_index("space")
    h = lax.rem(s, 2)
    p = lax.div(s, 2)
    pairs = slabs // 2
    half = ny // 2
    win = half + PAD
    other = 1 - h
    partner = s + 1 - 2 * h
    team = next(n for n in (4, 2, 1) if slices % n == 0)
    rank = lax.rem(t, team)
    early = lax.rem(t, 2) == 1
    first_row = pl.multiple_of(h * (half - PAD), 8)
    partner_row = pl.multiple_of(other * (half - PAD), 8)
    own = pl.multiple_of(PAD * h, 8)
    mine = pl.multiple_of(h * half, 8)
    has_next = t < slices - 1
    has_prev = t > 0
    has_lower = p > 0
    has_upper = p < pairs - 1
    pending = []

    def later(ref, sem, cond=None):
        pending.append((ref, sem, cond))

    def remote(src, dst, send, recv, tm, space):
        return pltpu.make_async_remote_copy(
            src_ref=src, dst_ref=dst, send_sem=send, recv_sem=recv,
            device_id=(tm, space), device_id_type=MESH,
        )

    barrier = pltpu.get_barrier_semaphore()

    def greet(d, carry):
        pl.semaphore_signal(
            barrier, inc=1, device_id=(t, lax.rem(s + d, slabs)), device_id_type=MESH
        )
        return carry

    lax.fori_loop(1, slabs, greet, 0)
    for cond, tm in ((has_next, t + 1), (has_prev, t - 1)):

        @pl.when(cond)
        def _(tm=tm):
            for space in (s, partner):
                pl.semaphore_signal(barrier, inc=1, device_id=(tm, space), device_id_type=MESH)

    far = [jnp.abs(rank - q) > 1 for q in range(team)]
    for q in range(team):

        @pl.when(far[q])
        def _(q=q):
            pl.semaphore_signal(
                barrier, inc=1, device_id=(t - rank + q, s), device_id_type=MESH
            )

    sources = [kappa_in.at[0]] + [nodes_in.at[0, j, 0] for j in range(3)] + [start_in.at[0, 0]]
    for k, source in enumerate(sources):
        pltpu.make_async_copy(
            source.at[pl.ds(first_row, win)], field.at[k, h, pl.ds(PAD, win)], own_s.at[0]
        ).start()
        pltpu.make_async_copy(
            source.at[pl.ds(partner_row, win)], outgoing.at[k], own_s.at[1]
        ).start()

    zeros = jnp.zeros((PAD, nz), f32)
    for k in range(FIELDS):
        for slab in range(2):
            field[k, slab, 0:PAD, :] = zeros
            field[k, slab, win + PAD : win + 2 * PAD, :] = zeros

    def clear(ref):
        def body(i, carry):
            for k in range(HALOS):
                ref[k, pl.ds(pl.multiple_of(i * 8, 8), 8), :] = zeros
            return carry

        lax.fori_loop(0, win // 8, body, 0)

    @pl.when(jnp.logical_not(has_lower))
    def _():
        clear(lower)

    @pl.when(jnp.logical_not(has_upper))
    def _():
        clear(upper)

    pl.semaphore_wait(
        barrier,
        slabs - 1 + 2 * has_next.astype(jnp.int32) + 2 * has_prev.astype(jnp.int32)
        + sum(f.astype(jnp.int32) for f in far),
    )

    tile = tile_of(win, 24)
    bounds = chunk_bounds(win, tile)
    chunks = len(bounds)

    weights = [SHARES[q % 2] for q in range(team)]
    cuts = [8 * (win // 8 * sum(weights[:q]) // sum(weights)) for q in range(team)] + [win]
    parts = [(cuts[q], cuts[q + 1] - cuts[q]) for q in range(team)]

    def bounds_of(k, c):
        return bounds[c] if k else parts[c]

    def each_part(body):
        for q in range(team):
            if parts[q][1]:
                pl.when(rank == q)(lambda q=q: body(q))

    def arrived(ref, sem):
        remote(ref, ref, sum_s.at[0], sem, t, partner).wait_recv()

    def sent(ref, sem):
        remote(ref, ref, sem, sum_r.at[0], t, partner).wait_send()

    def swap_sem(k, c):
        return swap_r.at[1 + (k - 1) * chunks + c if k else 0]

    def swap_start(k, c):
        lo, rows = bounds_of(k, c)
        remote(
            outgoing.at[k, pl.ds(lo, rows)], field.at[k, h, pl.ds(PAD + lo, rows)],
            swap_s.at[min(k, 1)], swap_sem(k, c), t, partner,
        ).start()

    def swap_wait(k, c):
        lo, rows = bounds_of(k, c)
        arrived(field.at[k, other, pl.ds(PAD + lo, rows)], swap_sem(k, c))

    def kin_ref(e, lo, rows):
        if e == 0:
            return field.at[KAPPA, other, pl.ds(PAD + lo, rows)]
        return (lower, upper)[e - 1].at[H_KAPPA, pl.ds(lo, rows)]

    def kin_start(e, q):
        ref = kin_ref(e, *parts[q])
        for peer in range(team):
            if peer != q:
                remote(ref, ref, kin_s.at[e], kin_r.at[e], t - q + peer, s).start()

    def kin_wait(e):
        for q in range(team):
            rows = win - parts[q][1]
            if rows:
                pl.when(rank == q)(lambda rows=rows: arrived(kin_ref(e, 0, rows), kin_r.at[e]))

    def kin_sent(e):
        if team > 1:
            each_part(
                lambda q: sent(field.at[pl.ds(0, team - 1), 0, pl.ds(0, parts[q][1])], kin_s.at[e])
            )

    pltpu.make_async_copy(outgoing, outgoing, own_s.at[1]).wait()
    each_part(lambda q: swap_start(0, q))
    for c in range(chunks):
        for k in range(1, 4):
            swap_start(k, c)
    for c in range(chunks):
        swap_start(4, c)
    later(outgoing.at[pl.ds(1, 4)], swap_s.at[1])

    def halo_sems(k, c, side):
        if k == H_KAPPA:
            slots = 0, 0
        elif k < H_RES:
            slots = 1, 1 + c
        elif k == H_RES:
            slots = 1, 1 + chunks
        elif k >= H_GAIN:
            slots = 1, 2 + chunks + k - H_GAIN
        else:
            m = k - H_IMG
            slots = 1 + m // 2, 4 + chunks + (2 * m + c if m < 2 else 2 + m)
        return halo_s.at[side, slots[0]], halo_r.at[side, slots[1]]

    def down(f, k, c, lo, rows):
        return remote(
            field.at[f, 0, pl.ds(PAD + lo, rows)], upper.at[k, pl.ds(lo, rows)],
            *halo_sems(k, c, 0), t, s - 2,
        )

    def up(f, k, c, lo, rows):
        return remote(
            field.at[f, 1, pl.ds(PAD + lo, rows)], lower.at[k, pl.ds(lo, rows)],
            *halo_sems(k, c, 1), t, s + 2,
        )

    def first_hop(k, c, which):
        @pl.when(jnp.logical_and(which == 0, has_lower))
        def _():
            down(k, k, c, *bounds_of(k, c)).start()

        @pl.when(jnp.logical_and(which == 1, has_upper))
        def _():
            up(k, k, c, *bounds_of(k, c)).start()

    own_rows = field.at[pl.ds(0, 5), h, pl.ds(PAD, win)]
    pltpu.make_async_copy(own_rows, own_rows, own_s.at[0]).wait()
    each_part(lambda q: first_hop(0, q, h))
    for c in range(chunks):
        for k in range(1, 4):
            first_hop(k, c, h)

    def halo_wait(k, c, lo, rows, sides=(0, 1), fields=None):
        which = k if fields is None else pl.ds(k, fields)
        for side, ref, cond in ((0, upper, has_upper), (1, lower, has_lower)):
            if side in sides:

                @pl.when(cond)
                def _(side=side, ref=ref):
                    arrived(ref.at[which, pl.ds(lo, rows)], halo_sems(k, c, side)[1])

    def halo_later(f, slot, lo, rows, fields=None, sides=(0, 1)):
        which = f if fields is None else pl.ds(f, fields)
        for side in sides:
            ref = field.at[which, side, pl.ds(PAD + lo, rows)]
            later(ref, halo_s.at[side, slot], (has_lower, has_upper)[side])

    lane = lax.broadcasted_iota(jnp.int32, (tile, nz), 1)

    def loop(rows, size, body, init=0, offset=0):
        def step(i, carry):
            return body(pl.multiple_of(offset + i * size, 8), carry)

        count = rows // size
        return lax.fori_loop(0, count, step, init, unroll=max(u for u in range(1, UNROLL + 1) if count % u == 0))

    def coefficients(b, carry):
        windows = [field[KAPPA, slab, pl.ds(b, tile + 2 * PAD), :] for slab in range(2)]
        centre = [w[PAD : PAD + tile] for w in windows]
        before = 0.5 * (centre[0] + lower[H_KAPPA, pl.ds(b, tile), :])
        between = 0.5 * (centre[0] + centre[1])
        after = 0.5 * (centre[1] + upper[H_KAPPA, pl.ds(b, tile), :])
        across[0, pl.ds(b, tile), :] = before
        across[1, pl.ds(b, tile), :] = between
        across[2, pl.ds(b, tile), :] = after
        ends = [before + between, between + after]
        for slab in range(2):
            w, k = windows[slab], centre[slab]
            above = 0.5 * (k + w[PAD - 1 : PAD - 1 + tile])
            below = 0.5 * (k + w[PAD + 1 : PAD + 1 + tile])
            right = jnp.where(lane == nz - 1, 0.0, pltpu.roll(k, nz - 1, axis=1))
            left = jnp.where(lane == 0, 0.0, pltpu.roll(k, 1, axis=1))
            right_face = 0.5 * (k + right)
            left_face = 0.5 * (k + left)
            faces[0, slab, pl.ds(b, tile), :] = above
            faces[1, slab, pl.ds(b, tile), :] = below
            faces[2, slab, pl.ds(b, tile), :] = jnp.where(lane == nz - 1, 0.0, right_face)
            faces[3, slab, pl.ds(b, tile), :] = ends[slab] + above + below + right_face + left_face
        return carry

    def heat(windows, outer, b, size):
        centre = [w[PAD : PAD + size] for w in windows]
        between = across[1, pl.ds(b, size), :]
        images = []
        for slab in range(2):
            w, v = windows[slab], centre[slab]
            fz = faces[2, slab, pl.ds(b, size), :]
            value = between * centre[1 - slab]
            if outer[slab] is not None:
                value = value + outer[slab]
            value = value + faces[0, slab, pl.ds(b, size), :] * w[PAD - 1 : PAD - 1 + size]
            value = value + faces[1, slab, pl.ds(b, size), :] * w[PAD + 1 : PAD + 1 + size]
            value = value + fz * pltpu.roll(v, nz - 1, axis=1) + pltpu.roll(fz * v, 1, axis=1)
            images.append(value - faces[3, slab, pl.ds(b, size), :] * v)
        return centre, images

    def plain_heat(f, k, b, size):
        windows = [field[f, slab, pl.ds(b, size + 2 * PAD), :] for slab in range(2)]
        outer = (
            across[0, pl.ds(b, size), :] * lower[k, pl.ds(b, size), :],
            across[2, pl.ds(b, size), :] * upper[k, pl.ds(b, size), :],
        )
        return heat(windows, outer, b, size)

    def folded(value):
        return jnp.sum(value.reshape(-1, 8, nz), axis=0)

    def each_slab(body):
        if slabs <= 16:
            for d in range(1, slabs):
                body(d)
        else:

            def step(d, carry):
                body(d)
                return carry

            lax.fori_loop(1, slabs, step, 0)

    def sum_copy(m, d):
        return remote(
            sums.at[m, s], sums.at[m, s], sum_s.at[0], sum_r.at[m], t, lax.rem(s + d, slabs),
        )

    def sum_start(m, parts):
        for row, part in enumerate(parts):
            flat = jnp.sum(part, axis=0, keepdims=True)
            line = flat[:, 0:128]
            for at in range(128, nz, 128):
                line = line + flat[:, at : at + 128]
            sums[m, s, row : row + 1, :] = line
        each_slab(lambda d: sum_copy(m, d).start())

    def sum_wait(m):
        arrived(sums.at[m, pl.ds(0, slabs - 1)], sum_r.at[m])
        total = jnp.sum(sums[m], axis=0)
        total = jnp.sum(total, axis=1, keepdims=True)
        return [total[row : row + 1, :] for row in range(4)]

    def halo_send(f, k, c, lo, rows):
        pl.when(has_lower)(down(f, k, c, lo, rows).start)
        pl.when(has_upper)(up(f, k, c, lo, rows).start)

    quarter = half // 2
    set_up = own
    set_down = pl.multiple_of(own + quarter, 8)
    pieces_of = (
        ((quarter, quarter + PAD), (0, quarter + PAD)),
        ((0, quarter), (quarter + PAD, quarter)),
    )

    def rows_of(m, piece):
        if m < 2:
            return pieces_of[piece]
        return (set_down, quarter), (set_up, quarter)

    def img_send(m, piece):
        (lo_d, rows_d), (lo_u, rows_u) = rows_of(m, piece)
        pl.when(has_lower)(down(IMG + m, H_IMG + m, piece, lo_d, rows_d).start)
        pl.when(has_upper)(up(IMG + m, H_IMG + m, piece, lo_u, rows_u).start)

    def img_wait(m, piece):
        for side in range(2):
            halo_wait(H_IMG + m, piece, *rows_of(m, piece)[side], (side,))

    nothing = jnp.zeros((8, nz), f32)

    def product(m):
        def body(b, carry):
            centre, images = plain_heat(RES + m, H_RES + m, b, tile)
            row = lax.broadcasted_iota(jnp.int32, (tile, nz), 0) + b
            inside = jnp.logical_and(row >= own, row < own + half)
            norm, along = carry
            for slab in range(2):
                v = centre[slab]
                w = -WIDTHS[m] * images[slab]
                field[IMG + m, slab, pl.ds(PAD + b, tile), :] = w
                masked = jnp.where(inside, v, 0.0)
                norm = norm + folded(masked * v)
                along = along + folded(masked * w)
            return norm, along

        sums_here = loop(win, tile, body, (nothing, nothing))
        img_send(m, 0)
        return sums_here

    small = tile_of(quarter, 32)

    def local(m):
        def body(b, carry):
            windows = [field[IMG + m, slab, pl.ds(b, small + 2 * PAD), :] for slab in range(2)]
            centre, images = heat(windows, (None, None), b, small)
            norm, along = carry
            for slab in range(2):
                v = centre[slab]
                norm = norm + folded(v * v)
                along = along + folded(v * images[slab])
            return norm, along

        return loop(half, small, body, (nothing, nothing), own)

    def cross(m, sums_here, sums_local):
        img_wait(m, 0)

        def body_of(side):
            ref = lower if side == 0 else upper

            def body(b, carry):
                rows = pl.ds(b, small)
                edge = across[2 * side, rows, :] * ref[H_IMG + m, rows, :]
                return carry + folded(edge * field[IMG + m, side, pl.ds(PAD + b, small), :])

            return body

        outer = loop(quarter, small, body_of(0), nothing, set_up)
        outer = loop(quarter, small, body_of(1), outer, set_down)
        norm, along = sums_local
        sum_start(m, sums_here + (norm, -WIDTHS[m] * (along + 2.0 * outer)))

    def factors(m):
        rr, rw, ww, wbw = sum_wait(m)
        step_size = rr / (rr + rw)
        mean = rw / rr
        square = step_size * step_size
        norm_next = square * jnp.maximum(ww - mean * rw, 0.0)
        along = square * jnp.maximum(mean * mean * rw - 2.0 * mean * ww + wbw, 0.0)
        momentum = norm_next / rr
        below = norm_next * (1.0 + momentum)
        curve = jnp.maximum(norm_next + along - momentum * norm_next / step_size, below)
        step_next = norm_next / jnp.maximum(curve, 1e-37)
        on_image = step_size * step_next
        return step_size + step_next * (1.0 + momentum) - on_image, on_image

    def advance(m, scalars):
        on_res, on_img = scalars

        def body(b, carry):
            at = pl.ds(PAD + b, tile)
            rows = pl.ds(b, tile)
            for slab in range(2):
                field[RES + m + 1, slab, at, :] = (
                    field[GAIN + m, slab, at, :]
                    + on_res * field[RES + m, slab, at, :]
                    - on_img * field[IMG + m, slab, at, :]
                )
            for ref in (lower, upper):
                ref[H_RES + m + 1, rows, :] = (
                    ref[H_GAIN + m, rows, :]
                    + on_res * ref[H_RES + m, rows, :]
                    - on_img * ref[H_IMG + m, rows, :]
                )
            return carry

        loop(win, tile, body)

    def coarse_residual():
        def body(b, carry):
            at = pl.ds(PAD + b, tile)
            for slab in range(2):
                field[RES + 3, slab, at, :] = (
                    field[RES, slab, at, :] + field[GAIN, slab, at, :] + field[GAIN + 1, slab, at, :]
                )
            return carry

        loop(win, tile, body)

    def coarse_halo():
        def body(b, carry):
            rows = pl.ds(b, tile)
            for ref in (lower, upper):
                ref[H_RES + 3, rows, :] = (
                    ref[H_RES, rows, :] + ref[H_GAIN, rows, :] + ref[H_GAIN + 1, rows, :]
                )
            return carry

        loop(win, tile, body)

    mailed = (GAIN, GAIN + 1, IMG + 1, IMG + 2, RES + 3)

    def mail_copy(k):
        return remote(
            field.at[mailed[k], other, pl.ds(PAD + own, half)], mail.at[k],
            mail_s.at[k // 4], mail_r.at[k], t, partner,
        )

    def mail_send(k):
        mail_copy(k).start()

    def coarse_send(k, which=(0, 1), cond=True):
        for slab, space in [((h, s), (other, partner))[w] for w in which]:
            copy = remote(
                field.at[(RES + 3, IMG + 3)[k - 1], slab, pl.ds(PAD + own, half)],
                kept.at[k, pl.ds(mine, half)], kept_s.at[k], kept_r.at[k], t + 1, space,
            )
            pl.when(jnp.logical_and(has_next, cond))(copy.start)

    def kept_copy(k):
        if k == 0:
            src, dst = nodes_in.at[0, 2, 0], kept.at[0]
        else:
            src, dst = marks.at[k - 3], marks.at[k - 1]
        return remote(src, dst, kept_s.at[k], kept_r.at[k], t + 1, s)

    def marks_send(k, update):
        for row in range(2):
            marks[k - 3, row : row + 1, :] = jnp.broadcast_to(update[row], (1, 128))
        pl.when(has_next)(kept_copy(k).start)

    def marks_of(k):
        arrived(marks.at[k - 1], kept_r.at[k])
        return marks[k - 1, 0:1, 0:1], marks[k - 1, 1:2, 0:1]

    def ahead_send(e):
        copy = remote(
            field.at[(RES + 2, IMG + 2)[e], h, pl.ds(PAD + own, half)], ahead.at[e],
            kept_s.at[5], kept_r.at[5], t + 1, s,
        )
        pl.when(has_next)(copy.start)

    def finish(m, scalars, slab, ref, lo, rows):
        on_res, on_img = scalars
        node = NODE + min(m, 2)

        def body(b, carry):
            at = pl.ds(PAD + own + b, small)
            ref[pl.ds(b, small), :] = (
                field[node, slab, at, :]
                + on_res * field[RES + m, slab, at, :]
                - on_img * field[IMG + m, slab, at, :]
            )
            return carry

        loop(rows, small, body, 0, lo)

    def residuals(b, carry):
        images = [plain_heat(NODE + j, H_NODE + j, b, tile)[1] for j in range(3)]
        at = pl.ds(PAD + b, tile)
        for slab in range(2):
            nodes = [field[NODE + j, slab, at, :] for j in range(3)]
            for row, f in enumerate((RES, GAIN, GAIN + 1)):
                value = nodes[row - 1] - nodes[row] if row else -nodes[0]
                for j in range(3):
                    value = value + (STEP * sweep_weight(row, j)) * images[j][slab]
                field[f, slab, at, :] = value
        return carry

    spans = []
    for c, (lo, rows) in enumerate(bounds):
        begin = lo - tile if c else 0
        end = lo + rows - (tile if c < chunks - 1 else 0)
        spans.append((begin, end - begin))

    def begin_rows(c):
        halo_wait(H_NODE, c, *bounds[c], fields=3)
        lo, rows = spans[c]
        loop(rows, tile, coefficients, 0, lo)
        loop(rows, tile, residuals, 0, lo)

    def add_start(b, carry):
        at = pl.ds(PAD + b, tile)
        for slab in range(2):
            field[RES, slab, at, :] = field[RES, slab, at, :] + field[START, slab, at, :]
        return carry

    def begin_res(c):
        swap_wait(4, c)
        lo, rows = spans[c]
        loop(rows, tile, add_start, 0, lo)
        halo_send(RES, H_RES, c, lo, rows)

    def pass_kappa(q):
        swap_wait(0, q)
        kin_start(0, q)
        first_hop(0, q, other)

    each_part(pass_kappa)
    for c in range(chunks):
        for k in range(1, 4):
            swap_wait(k, c)
            first_hop(k, c, other)
        if c == 0:
            each_part(lambda q: halo_wait(H_KAPPA, 0, *parts[q]))
            pl.when(has_lower)(lambda: each_part(lambda q: kin_start(1, q)))
            pl.when(has_upper)(lambda: each_part(lambda q: kin_start(2, q)))
        if c == min(1, chunks - 1):
            kin_wait(0)
            pl.when(has_lower)(lambda: kin_wait(1))
            pl.when(has_upper)(lambda: kin_wait(2))
        if c > 0:
            begin_rows(c - 1)
    for c in range(chunks):
        if c == chunks - 1:
            begin_rows(c)
        begin_res(c)
    mail_send(0)
    mail_send(1)
    theirs = pl.multiple_of(other * half, 8)
    beside = pl.multiple_of(PAD * other, 8)

    def half_of(m, at):
        return fine_out.at[0, m, 0, pl.ds(at, half)]

    def finish_start(update):
        finish(0, update, other, result, 0, half)
        remote(result, half_of(0, mine), out_s.at[0], out_r.at[0], t, partner).start()
        later(result, out_s.at[0])
        finish(0, update, h, half_of(0, mine), 0, half)

    def finish_second(update):
        finish(1, update, h, half_of(1, mine), 0, half)
        arrived(half_of(0, theirs), out_r.at[0])
        for k in range(3):
            mail_copy(k).wait_recv()

        def body(b, carry):
            rows, at = pl.ds(b, small), pl.ds(beside + b, small)
            there = pl.ds(theirs + b, small)
            residual = fine_out[0, 0, 0, there, :] - outgoing[1, at, :] + mail[0, rows, :]
            step = update[0] * residual - update[1] * mail[2, rows, :]
            fine_out[0, 1, 0, there, :] = outgoing[2, at, :] + step
            mail[1, rows, :] = mail[1, rows, :] + step
            return carry

        loop(half, small, body)

    def finish_third(update, lo, rows):
        def body(b, carry):
            at = pl.ds(b, small)
            fine_out[0, 2, 0, pl.ds(theirs + b, small), :] = (
                outgoing[3, pl.ds(beside + b, small), :]
                + update[0] * mail[1, at, :]
                - update[1] * mail[3, at, :]
            )
            return carry

        loop(rows, small, body, 0, lo)

    def finish_coarse():
        on_res, on_img = marks_of(3)

        def body(b, carry):
            at = pl.ds(b, small)
            coarse_out[0, 0, at, :] = (
                kept[0, at, :] + on_res * kept[1, at, :] - on_img * kept[2, at, :]
            )
            return carry

        loop(ny, small, body)

    @pl.when(jnp.logical_not(has_prev))
    def _():
        pltpu.make_async_copy(start_in.at[0, 0], start_out.at[0, 0], copy_s.at[0]).start()
        pltpu.make_async_copy(start_in.at[0, 0], coarse_out.at[0, 0], copy_s.at[1]).start()

    def gain_send(m, chunk_range):
        for c in chunk_range:
            if c < chunks:
                halo_send(GAIN + m, H_GAIN + m, c, *spans[c])

    def gain_wait(m):
        halo_wait(H_GAIN + m, 0, 0, win)

    gain_send(0, range(0, 2))
    pl.when(has_next)(kept_copy(0).start)
    halo_wait(H_RES, 0, 0, win)
    here = product(0)
    gain_send(0, range(2, 4))
    cross(0, here, local(0))
    gain_send(0, range(4, chunks))
    img_send(0, 1)
    gain_send(1, range(0, 2))
    coarse_residual()
    coarse_send(1, (0,))
    pl.when(has_next)(mail_copy(4).start)
    later(mail.at[4], mail_s.at[1], has_next)
    later(mail.at[pl.ds(0, 4)], mail_s.at[0])
    update = factors(0)
    gain_wait(0)
    img_wait(0, 1)
    advance(0, update)
    here = product(1)
    mail_send(2)
    gain_send(1, range(2, 4))
    cross(1, here, local(1))

    @pl.when(has_next)
    def _():
        mail_copy(4).wait_recv()
        remote(
            mail.at[4], kept.at[1, pl.ds(theirs, half)], kept_s.at[1], kept_r.at[1], t + 1, s
        ).start()

    finish_start(update)
    gain_send(1, range(4, chunks))
    img_send(1, 1)
    gain_wait(1)
    coarse_halo()
    here_coarse = product(3)
    coarse_send(2, (0,))
    coarse_send(2, (1,), early)
    update = factors(1)
    img_wait(1, 1)
    advance(1, update)
    ahead_send(0)
    here = product(2)
    ahead_send(1)
    mail_send(3)
    cross(3, here_coarse, local(3))
    cross(2, here, local(2))
    coarse_send(2, (1,), jnp.logical_not(early))
    finish_second(update)

    def finish_next():
        on_res, on_img = marks_of(4)
        arrived(ahead, kept_r.at[5])

        def body(b, carry):
            at, rows = pl.ds(mine + b, small), pl.ds(b, small)
            start_out[0, 0, at, :] = (
                kept[0, at, :] + on_res * ahead[0, rows, :] - on_img * ahead[1, rows, :]
            )
            return carry

        loop(half, small, body)

    marks_send(3, factors(3))
    mail_copy(3).wait_recv()
    update = factors(2)
    marks_send(4, update)
    pieces = 2 if half % (2 * small) == 0 else 1
    piece = half // pieces
    for c in range(pieces):
        at = theirs + c * piece
        finish_third(update, c * piece, piece)
        copy = remote(
            fine_out.at[0, 2, 0, pl.ds(at, piece)], start_out.at[0, 0, pl.ds(at, piece)],
            end_s.at[0], end_r.at[0], t + 1, s,
        )
        pl.when(has_next)(copy.start)
    finish(2, update, h, half_of(2, mine), 0, half)

    @pl.when(jnp.logical_not(has_prev))
    def _():
        pltpu.make_async_copy(start_in.at[0, 0], start_out.at[0, 0], copy_s.at[0]).wait()
        pltpu.make_async_copy(start_in.at[0, 0], coarse_out.at[0, 0], copy_s.at[1]).wait()

    @pl.when(has_prev)
    def _():
        for k in range(3):
            arrived(kept.at[k], kept_r.at[k])
        finish_coarse()
        finish_next()
        arrived(start_out.at[0, 0, pl.ds(theirs, half)], end_r.at[0])

    each_part(lambda q: sent(outgoing.at[0, pl.ds(*parts[q])], swap_s.at[0]))
    for side, cond in ((0, has_lower), (1, has_upper)):

        @pl.when(cond)
        def _(side=side):
            each_part(
                lambda q: sent(
                    field.at[KAPPA, side, pl.ds(PAD + parts[q][0], parts[q][1])],
                    halo_s.at[side, 0],
                )
            )

    kin_sent(0)
    pl.when(has_lower)(lambda: kin_sent(1))
    pl.when(has_upper)(lambda: kin_sent(2))
    halo_later(0, 1, 0, win, 8)
    for side in range(2):
        halo_later(IMG + 2, 2, *rows_of(2, 0)[side], 2, (side,))
    for k in range(3):
        later(kept.at[k], kept_s.at[k], has_next)
    for k in range(2):
        later(marks.at[k], kept_s.at[3 + k], has_next)
    later(ahead, kept_s.at[5], has_next)
    later(fine_out.at[0, 2, 0, pl.ds(theirs, half)], end_s.at[0], has_next)
    later(sums.at[pl.ds(0, 4), pl.ds(0, slabs - 1)], sum_s.at[0])
    for ref, sem, cond in pending:
        if cond is None:
            sent(ref, sem)
        else:
            pl.when(cond)(lambda ref=ref, sem=sem: sent(ref, sem))


def store(fine, begin, coarse, fine_out, start_out, coarse_out, sem):
    pairs = [(begin.at[0, 0], start_out.at[0, 0]), (coarse.at[0, 0], coarse_out.at[0, 0])]
    pairs += [(fine.at[0, m, 0], fine_out.at[0, m, 0]) for m in range(fine.shape[1])]
    copies = []
    for k, (src, dst) in enumerate(pairs):
        rows = src.shape[0] // 2
        for j in range(2):
            at = pl.ds(j * rows, rows)
            copies.append(pltpu.make_async_copy(src.at[at], dst.at[at], sem.at[2 * k + j]))
    for copy in copies:
        copy.start()
    for copy in copies:
        copy.wait()


def solution(mesh):
    slices, slabs = mesh.shape["tm"], mesh.shape["space"]

    def on_device(start_value, old_nodes, diffusivity):
        ny, nz = start_value.shape[2:]
        half = ny // 2
        win = half + PAD
        chunks = len(chunk_bounds(win, tile_of(win, 24)))
        vmem = lambda *shape: pltpu.VMEM(shape, jnp.float32)
        dma = lambda *shape: pltpu.SemaphoreType.DMA(shape)

        def body(*refs):
            kernel(slices, slabs, ny, nz, *refs)

        nodes, ends = pltpu.VMEM(old_nodes.shape, jnp.float32), pltpu.VMEM(start_value.shape, jnp.float32)
        results = pl.pallas_call(
            body,
            out_shape=(nodes, ends, ends),
            in_specs=[pl.BlockSpec(memory_space=pltpu.HBM)] * 3,
            out_specs=(pl.BlockSpec(memory_space=pltpu.VMEM),) * 3,
            scratch_shapes=[
                vmem(FIELDS, 2, win + 2 * PAD, nz),
                vmem(HALOS, win, nz),
                vmem(HALOS, win, nz),
                vmem(4, 2, win, nz),
                vmem(3, win, nz),
                vmem(5, win, nz),
                vmem(half, nz),
                vmem(5, half, nz),
                vmem(3, ny, nz),
                vmem(2, half, nz),
                vmem(4, 8, 128),
                vmem(4, slabs, 4, 128),
                dma(2), dma(1 + 4 * chunks), dma(2), dma(3), dma(3), dma(2), dma(5), dma(6), dma(6),
                dma(2, 3), dma(2, 10 + chunks), dma(1), dma(4),
                dma(1), dma(1), dma(1), dma(1), dma(2),
            ],
            compiler_params=pltpu.CompilerParams(
                collective_id=0, has_side_effects=True, vmem_limit_bytes=61 * 1024 * 1024
            ),
            name="pfasst",
        )(start_value, old_nodes, diffusivity)
        return pl.pallas_call(
            store,
            out_shape=tuple(jax.ShapeDtypeStruct(r.shape, jnp.float32) for r in results),
            in_specs=[pl.BlockSpec(memory_space=pltpu.VMEM)] * 3,
            out_specs=(pl.BlockSpec(memory_space=pltpu.HBM),) * 3,
            scratch_shapes=[dma(4 + 2 * old_nodes.shape[1])],
            compiler_params=pltpu.CompilerParams(vmem_limit_bytes=1024 * 1024),
            name="store",
        )(*results)

    in_specs = (
        P("tm", "space", None, None),
        P("tm", None, "space", None, None),
        P("space", None, None),
    )
    out_specs = (
        P("tm", None, "space", None, None),
        P("tm", "space", None, None),
        P("tm", "space", None, None),
    )
    return jax.shard_map(
        on_device, mesh=mesh, in_specs=in_specs, out_specs=out_specs, check_vma=False
    )
```
